32 devices in a mesh: dp: 2 (over core), section: 4 (over z), mp: 4 (over y, x).
Axes of the slice: x: 2, y: 2, z: 4, core: 2. Of those that a mesh axis runs over, the one named last changes fastest.
Arguments:
- inputs: bfloat16 [48, 512], P(('dp', 'mp')), may hold values from -6 to 6
- tangents: bfloat16 [48, 32, 512], P(('dp', 'mp')), may hold values from -6 to 6
- targets: bfloat16 [48, 1024], P(('dp', 'mp')), may hold values from -24 to 24
- target_jac: bfloat16 [48, 32, 1024], P(('dp', 'mp')), may hold values from -24 to 24
- rank_mask: int32 [48, 32], P(('dp', 'mp')), may hold values from 0 to 1, as said below
- batch_order: int32 [8, 6], P(('dp', 'mp')), may hold values from 0 to 5, each once within a row
- encoder: bfloat16 [512, 2048], replicated, may hold values from -0.25 to 0.25
- layers: bfloat16 [4, 2048, 2048], P('section', 'mp'), may hold values from -0.125 to 0.125
- head_weight: bfloat16 [2048, 1024], replicated, may hold values from -0.125 to 0.125
Outputs:
- grad_layers: float32 [4, 2048, 2048], P('section', ('dp', 'mp'))
- grad_head: float32 [2048, 1024], P(('dp', 'mp'), 'section')
- loss_value: float32 [], replicated
The draws below stay inside these ranges and needn't reach their ends.
Inputs may be any that keep to these rules, and one draw needn't show every extreme that they name: `rank_mask`: each sample's ones are its first 1 to 32 directions. `batch_order`: each row is an ordering of 0 .. 5.
All inputs are finite; a program needn't handle non-finite values.
Results may differ from the reference program's by a relative error of at most 0.035.
Values may be sent and summed in bfloat16 or wider, within the bound.
No kernel may reach another device: no remote copies, remote signals or barrier semaphores. Data moves between devices by JAX's collectives and lax.ppermute only.
A program may use at most 128 MiB of HBM per device.

```python
import jax
import jax.numpy as jnp
from jax import lax

D = 2048
DIN = 512
DOUT = 1024
RANK = 32
MB = 6
S_DEV = 1
SAMP_DEV = 6
GROUP_ROWS = 8
SAMPLES = 48
LAYERS = 4
N_DP = 2
N_MP = 4


def draw_rank_mask(key, part):
    jitter_key = jax.random.fold_in(key, 12)
    device_rows = jnp.arange(GROUP_ROWS, dtype=jnp.int32)[:, None]
    model_index = device_rows % N_MP
    base_rank = 1 + (RANK - 1) * model_index // max(N_MP - 1, 1)
    jitter = jax.random.randint(jitter_key, (GROUP_ROWS, SAMP_DEV), -1, 2)
    active = jnp.clip(base_rank + jitter, 1, RANK)
    last_row = jnp.arange(SAMP_DEV, dtype=jnp.int32)[None, :] == 0
    active = jnp.where((model_index == N_MP - 1) & last_row, RANK, active).reshape(SAMPLES, 1)
    return (jnp.arange(RANK, dtype=jnp.int32)[None, :] < active).astype(jnp.int32)


def row_scales(key):
    scale_key = jax.random.fold_in(key, 21)
    device_rows = jnp.arange(GROUP_ROWS, dtype=jnp.float32) / max(GROUP_ROWS - 1, 1)
    wobble = jax.random.uniform(scale_key, (GROUP_ROWS,), jnp.float32, -0.1, 0.1)
    low_end = jnp.log(0.3)
    high_end = jnp.log(3.9)
    return jnp.exp(low_end + (high_end - low_end) * device_rows + wobble)


def draw_targets(key, part):
    value_key = jax.random.fold_in(key, 22)
    scales = row_scales(key)[:, None, None]
    values = jnp.clip(jax.random.normal(value_key, (GROUP_ROWS, SAMP_DEV, DOUT), jnp.float32), -6.0, 6.0)
    return jnp.clip(scales * values, -24.0, 24.0).reshape(SAMPLES, DOUT).astype(jnp.bfloat16)


def draw_target_jac(key, part):
    value_key = jax.random.fold_in(key, 23)
    scales = row_scales(key)[:, None, None, None]
    shape = (GROUP_ROWS, SAMP_DEV, RANK, DOUT)
    values = jnp.clip(jax.random.normal(value_key, shape, jnp.float32), -6.0, 6.0)
    return jnp.clip(scales * values, -24.0, 24.0).reshape(SAMPLES, RANK, DOUT).astype(jnp.bfloat16)


def steps_of(own_key, extent, cuts, least, top_value):
    level, own = 1.0, jax.random.fold_in(own_key, 6)
    for axis_at, blocks in cuts:
        draws = jnp.exp(jax.random.uniform(jax.random.fold_in(own, axis_at), (blocks,), jnp.float32, least / len(cuts), top_value / len(cuts)))
        level = level * jnp.repeat(draws, extent[axis_at] // blocks).reshape([-1 if axis == axis_at else 1 for axis in range(len(extent))])
    return level


def normal_values(rng, shape, spread, limit, pieces=(), held_as=jnp.bfloat16):
    result = jax.random.normal(rng, shape, jnp.float32) * spread
    if len(pieces) > 0:
        result = steps_of(rng, shape, pieces, -0.22, 0.18) * result
    return jnp.clip(result, min=-limit, max=limit).astype(held_as)


def setup_inputs(seed: int = 0) -> dict:
    streams_of = jax.random.split(jax.random.key(seed), 10)
    return {
        "inputs": normal_values(streams_of[0], (SAMPLES, DIN), 1.0, 6.0, ((0, 8),)),
        "tangents": normal_values(streams_of[1], (SAMPLES, RANK, DIN), 1.0, 6.0, ((0, 8),)),
        "targets": draw_targets(jax.random.fold_in(streams_of[9], 71), 0),
        "target_jac": draw_target_jac(jax.random.fold_in(streams_of[9], 71), 0),
        "rank_mask": draw_rank_mask(jax.random.fold_in(streams_of[9], 71), 0),
        "batch_order": jax.vmap(lambda own: jax.random.permutation(own, SAMP_DEV))(jax.random.split(streams_of[5], GROUP_ROWS)).reshape((GROUP_ROWS, SAMP_DEV)).astype(jnp.int32),
        "encoder": normal_values(streams_of[6], (DIN, D), DIN ** -0.5, 0.25),
        "layers": normal_values(streams_of[7], (LAYERS, D, D), D ** -0.5, 0.125, ((0, 4), (1, 4))),
        "head_weight": normal_values(streams_of[8], (D, DOUT), D ** -0.5, 0.125),
    }


def forward_layer(row_block, weight):
    model_width = weight.shape[1]
    pre_act = jnp.dot(row_block.reshape(-1, model_width), weight, preferred_element_type=jnp.float32).reshape(row_block.shape)
    tanh_p = jnp.tanh(pre_act[:, 0])
    slope_vals = 1.0 - tanh_p * tanh_p
    primal = row_block[:, 0].astype(jnp.float32) + tanh_p
    tangent = row_block[:, 1:].astype(jnp.float32) + slope_vals[:, None, :] * pre_act[:, 1:]
    return jnp.concatenate([primal[:, None], tangent], axis=1).astype(jnp.bfloat16), pre_act


def backward_layer(row_block, pre_act, grad_rows, weight):
    model_width = weight.shape[1]
    upstream = grad_rows.astype(jnp.float32)
    tanh_p = jnp.tanh(pre_act[:, 0])
    slope_vals = 1.0 - tanh_p * tanh_p
    tangent_part = upstream[:, 1:] * slope_vals[:, None, :]
    slope_grad = jnp.sum(upstream[:, 1:] * pre_act[:, 1:], axis=1)
    primal_part = upstream[:, 0] * slope_vals - 2.0 * slope_grad * tanh_p * slope_vals
    grad_mix = jnp.concatenate([primal_part[:, None], tangent_part], axis=1).astype(jnp.bfloat16)
    back_rows = jnp.dot(grad_mix.reshape(-1, model_width), weight.T, preferred_element_type=jnp.float32).reshape(upstream.shape)
    return grad_mix, (upstream + back_rows).astype(jnp.bfloat16)


def block_sum(left, right):
    blocks = (left.reshape(N_DP * N_MP, -1, left.shape[-1]), right.reshape(N_DP * N_MP, -1, right.shape[-1]))

    def add_block(running, block_pair):
        partial_value = jnp.dot(block_pair[0].T, block_pair[1], preferred_element_type=jnp.float32)
        rounded = lax.optimization_barrier(partial_value.astype(jnp.bfloat16))
        return running + rounded.astype(jnp.float32), None

    running, _ = lax.scan(add_block, jnp.zeros((left.shape[-1], right.shape[-1]), jnp.float32), blocks)
    return running


def reference(inputs, tangents, targets, target_jac, rank_mask, batch_order, encoder, layers, head_weight):
    row_depth = RANK + 1
    rows_in = jnp.concatenate([inputs[:, None, :], tangents], axis=1)
    hidden = jnp.dot(rows_in.reshape(-1, DIN), encoder, preferred_element_type=jnp.float32).reshape(SAMPLES, row_depth, D).astype(jnp.bfloat16)
    saved_in = []
    saved_pre = []
    for layer_idx in range(LAYERS):
        saved_in.append(hidden)
        hidden, pre_act = forward_layer(hidden, layers[layer_idx])
        saved_pre.append(pre_act)
    outputs = jnp.dot(hidden.reshape(-1, D), head_weight, preferred_element_type=jnp.float32).reshape(SAMPLES, row_depth, DOUT)
    row_weight = jnp.concatenate([jnp.ones((SAMPLES, 1), jnp.float32), rank_mask.astype(jnp.float32)], axis=1)
    wanted = jnp.concatenate([targets[:, None, :], target_jac], axis=1).astype(jnp.float32)
    mismatch = outputs - wanted
    misfit = jnp.sum(row_weight[:, :, None] * mismatch * mismatch, axis=(1, 2))
    sample_index = (jnp.arange(GROUP_ROWS, dtype=jnp.int32)[:, None] * SAMP_DEV + batch_order).reshape(-1)
    batch_id = ((jnp.arange(GROUP_ROWS, dtype=jnp.int32)[:, None] // N_MP) * MB + (jnp.arange(SAMP_DEV, dtype=jnp.int32) // S_DEV)[None, :]).reshape(-1)
    micro_of = jnp.zeros((SAMPLES,), jnp.int32).at[sample_index].set(batch_id.astype(jnp.int32))
    totals = jax.ops.segment_sum(jnp.sum(row_weight, axis=1), micro_of, num_segments=N_DP * MB)
    divisor = totals[micro_of]
    loss_value = jnp.sum(misfit / divisor) / (N_DP * MB * DOUT)
    cot_out = (2.0 * row_weight[:, :, None] * mismatch / divisor[:, None, None]).astype(jnp.bfloat16)
    grad_head = block_sum(hidden, cot_out)
    grad_rows = jnp.dot(cot_out.reshape(-1, DOUT), head_weight.T, preferred_element_type=jnp.float32).reshape(SAMPLES, row_depth, D).astype(jnp.bfloat16)
    layer_grads = [None] * LAYERS
    for layer_idx in reversed(range(LAYERS)):
        grad_mix, grad_rows = backward_layer(saved_in[layer_idx], saved_pre[layer_idx], grad_rows, layers[layer_idx])
        layer_grads[layer_idx] = block_sum(saved_in[layer_idx], grad_mix)
    return jnp.stack(layer_grads), grad_head, loss_value
```

```python
import jax
import jax.numpy as jnp
from jax import lax
from jax.experimental import pallas as pl
from jax.experimental.pallas import tpu as pltpu
from jax.sharding import PartitionSpec as P


F32 = jnp.float32
BF16 = jnp.bfloat16
MB = 6
EXTRA = 16
BLOCKS = 4

ANY = pl.BlockSpec(memory_space=pl.ANY)
SMEM = pl.BlockSpec(memory_space=pltpu.SMEM)
VMEM = pl.BlockSpec(memory_space=pltpu.VMEM)


def round_up(value, unit):
    return -(-value // unit) * unit


def mp_swap(value, flip):
    count = lax.axis_size("mp")
    return lax.ppermute(value, "mp", [(m, m ^ flip) for m in range(count)])


def dp_swap(value):
    count = lax.axis_size("dp")
    return lax.ppermute(value, "dp", [(d, d ^ 1) for d in range(count)])


def mp_pieces(value):
    return [value] + [mp_swap(value, k) for k in range(1, lax.axis_size("mp"))]


def hop(value, source, target):
    return lax.ppermute(value, "section", [(source, target)])


def after(value, *others):
    return lax.optimization_barrier((value,) + others)[0]


def spread(onehot, value):
    high = value.astype(BF16)
    low = (value - high.astype(F32)).astype(BF16)
    return jnp.dot(onehot, high, preferred_element_type=F32) + jnp.dot(
        onehot, low, preferred_element_type=F32
    )


class Weights:
    def __init__(self, layer):
        self.count = lax.axis_size("mp")
        self.block_rows, self.width = layer.shape
        dp_index = lax.axis_index("dp")
        half = self.block_rows // 2
        self.offsets = [dp_index * half, (1 - dp_index) * half]
        self.pieces = [(layer, 0, None, 0)]
        if self.count == 4 and lax.axis_size("dp") == 2:
            part = half // 2
            first = lax.dynamic_slice_in_dim(layer, dp_index * half, part, 0)
            second = lax.dynamic_slice_in_dim(layer, dp_index * half + part, part, 0)
            a1 = mp_swap(first, 1)
            b2 = mp_swap(second, 2)
            b1 = mp_swap(second, 1)
            a2 = mp_swap(first, 2)
            a3 = mp_swap(a1, 2)
            b3 = mp_swap(b2, 1)
            got = [(a1, 1, 0), (b2, 2, part), (b1, 1, part), (a2, 2, 0), (a3, 3, 0), (b3, 3, part)]
            for array, block, base in got:
                self.pieces.append((array, block, 0, base))
                self.pieces.append((dp_swap(array), block, 1, base))
            self.last = a3
        else:
            for block in range(1, self.count):
                self.pieces.append((mp_swap(layer, block), block, None, 0))
            self.last = self.pieces[-1][0]

    def arrays(self):
        return [piece[0] for piece in self.pieces]

    def start(self, ids, refs, buf, sems, by_column):
        for n in range(BLOCKS if by_column else 1):
            for ref, (array, block, which, base) in zip(refs, self.pieces):
                row = block * self.block_rows + base
                if which is not None:
                    row = row + pl.multiple_of(ids[1 + which], self.block_rows // 2)
                dst = buf.at[pl.ds(row, array.shape[0]), :]
                if by_column:
                    col = self.width // BLOCKS
                    ref_n, dst, sem = ref.at[:, n * col : (n + 1) * col], dst.at[:, n * col : (n + 1) * col], n
                else:
                    ref_n, sem = ref, block
                pltpu.make_async_copy(ref_n, dst, sems.at[sem]).start()

    def scratch(self, by_column):
        return [
            pltpu.VMEM((self.count * self.block_rows, self.width), BF16),
            pltpu.SemaphoreType.DMA((BLOCKS if by_column else self.count,)),
        ]


def finish(view, sem):
    pltpu.make_async_copy(view, view, sem).wait()


def fwd_stage(level, weights, ids, rows, onehot, slope):
    height, width = rows.shape
    prims = onehot.shape[1]
    leads = slope is None
    pieces = len(weights.pieces)
    kb = weights.block_rows
    nb = width // BLOCKS

    def body(ids_ref, rows_ref, onehot_ref, *rest):
        if not leads:
            slope_ref, *rest = rest
        w_refs, rest = rest[:pieces], rest[pieces:]
        if leads:
            next_ref, pre_ref, tanh_ref, buf, sems, turned = rest
        else:
            next_ref, pre_ref, buf, sems, turned = rest

        @pl.when(ids_ref[0] == level)
        def _():
            weights.start(ids_ref, w_refs, buf, sems, True)
            for k in range(weights.count):
                col = pl.multiple_of(ids_ref[3 + k] * kb, kb)
                turned[:, k * kb : (k + 1) * kb] = rows_ref[:, pl.ds(col, kb)]

            def block(n, carry):
                cols = pl.ds(pl.multiple_of(n * nb, nb), nb)
                view = buf.at[:, cols]
                finish(view, sems.at[n])
                acc = jnp.dot(turned[...], view[...], preferred_element_type=F32)
                old = rows_ref[:, cols].astype(F32)
                pre_ref[:, cols] = acc.astype(BF16)
                if leads:
                    tanh_p = jnp.tanh(acc[:prims])
                    tanh_ref[:, cols] = tanh_p
                    factor = spread(onehot_ref[...], 1.0 - tanh_p * tanh_p)
                    new = jnp.concatenate(
                        [old[:prims] + tanh_p, old[prims:] + factor * acc[prims:]], axis=0
                    )
                else:
                    tanh_p = slope_ref[:, cols]
                    new = old + spread(onehot_ref[...], 1.0 - tanh_p * tanh_p) * acc
                next_ref[:, cols] = new.astype(BF16)
                return carry

            lax.fori_loop(0, BLOCKS, block, 0)

    outs = [jax.ShapeDtypeStruct((height, width), BF16)] * 2
    if leads:
        outs.append(jax.ShapeDtypeStruct((prims, width), F32))
    args = [ids, rows, onehot] + ([] if leads else [slope]) + weights.arrays()
    specs = [SMEM, VMEM, VMEM] + ([] if leads else [VMEM]) + [ANY] * pieces
    return pl.pallas_call(
        body,
        out_shape=outs,
        in_specs=specs,
        out_specs=[VMEM] * len(outs),
        scratch_shapes=weights.scratch(True) + [pltpu.VMEM((height, width), BF16)],
        cost_estimate=pl.CostEstimate(flops=2 * height * width * width * 4, bytes_accessed=2 * width * width, transcendentals=0),
        compiler_params=pltpu.CompilerParams(vmem_limit_bytes=40 * 2**20),
        name=f"fwd{level}",
    )(*args)


def bwd_stage(level, weights, ids, cot, pre, tanh_p, onehot, onehot_t, total, leads):
    height, width = cot.shape
    prims = tanh_p.shape[0]
    deep = level > 0
    pieces = len(weights.pieces) if deep else 0
    kb = weights.block_rows
    nb = width // BLOCKS

    def body(ids_ref, cot_ref, pre_ref, tanh_ref, onehot_ref, onehot_t_ref, *rest):
        if total is not None:
            total_ref, *rest = rest
        w_refs, rest = rest[:pieces], rest[pieces:]
        if deep:
            mix_ref, side_ref, new_ref, buf, sems = rest
        else:
            mix_ref, side_ref = rest

        @pl.when(ids_ref[0] == level)
        def _():
            if deep:
                weights.start(ids_ref, w_refs, buf, sems, False)
            skip = prims if leads else 0

            def block(n, carry):
                cols = pl.ds(pl.multiple_of(n * nb, nb), nb)
                up = cot_ref[:, cols].astype(F32)
                tanh = tanh_ref[:, cols]
                slope = 1.0 - tanh * tanh
                up_t = up[skip:]
                mix_t = up_t * spread(onehot_ref[...], slope)
                total_here = spread(onehot_t_ref[...], up_t * pre_ref[:, cols].astype(F32)[skip:])
                if total is not None:
                    total_here = total_here + total_ref[:, cols]
                if leads:
                    mix_p = up[:prims] * slope - 2.0 * total_here * tanh * slope
                    mix_ref[:, cols] = jnp.concatenate([mix_p, mix_t], axis=0).astype(BF16)
                else:
                    mix_ref[:, cols] = mix_t.astype(BF16)
                side_ref[:, cols] = total_here
                return carry

            lax.fori_loop(0, BLOCKS, block, 0)
            if deep:

                def back_block(k, carry):
                    view = buf.at[pl.ds(pl.multiple_of(k * kb, kb), kb), :]
                    finish(view, sems.at[k])
                    cols = pl.ds(pl.multiple_of(ids_ref[3 + k] * kb, kb), kb)
                    back = lax.dot_general(
                        mix_ref[...], view[...], (((1,), (1,)), ((), ())), preferred_element_type=F32
                    )
                    new_ref[:, cols] = (cot_ref[:, cols].astype(F32) + back).astype(BF16)
                    return carry

                lax.fori_loop(0, weights.count, back_block, 0)

    rows_shape = jax.ShapeDtypeStruct((height, width), BF16)
    outs = [rows_shape, jax.ShapeDtypeStruct((prims, width), F32)] + ([rows_shape] if deep else [])
    sums = [] if total is None else [total]
    return pl.pallas_call(
        body,
        out_shape=outs,
        in_specs=[SMEM] + [VMEM] * (5 + len(sums)) + [ANY] * pieces,
        out_specs=[VMEM] * len(outs),
        scratch_shapes=weights.scratch(False) if deep else [],
        cost_estimate=pl.CostEstimate(flops=2 * height * width * width * 4, bytes_accessed=2 * width * width, transcendentals=0),
        compiler_params=pltpu.CompilerParams(vmem_limit_bytes=40 * 2**20),
        name=f"bwd{level}",
    )(ids, cot, pre, tanh_p, onehot, onehot_t, *sums, *(weights.arrays() if deep else []))


def pick_rows(ids, index, pieces, level, matrix=None):
    height = index.shape[0]
    piece_rows, width = pieces[0].shape
    out_width = width if matrix is None else matrix.shape[1]

    def body(ids_ref, index_ref, *rest):
        piece_refs, rest = rest[: len(pieces)], rest[len(pieces) :]
        out_ref = rest[-1]

        @pl.when(ids_ref[0] == level)
        def _():
            index_here = index_ref[...]
            acc = jnp.zeros((height, width), F32)
            for k, piece_ref in enumerate(piece_refs):
                place = lax.broadcasted_iota(jnp.int32, (height, piece_rows), 1) + k * piece_rows
                onehot = jnp.where(place == index_here, 1.0, 0.0).astype(BF16)
                acc = acc + jnp.dot(onehot, piece_ref[...], preferred_element_type=F32)
            rows = acc.astype(BF16)
            if matrix is not None:
                rows = jnp.dot(rows, rest[0][...], preferred_element_type=F32).astype(BF16)
            out_ref[...] = rows

    extra = [] if matrix is None else [matrix]
    return pl.pallas_call(
        body,
        out_shape=jax.ShapeDtypeStruct((height, out_width), BF16),
        in_specs=[SMEM] + [VMEM] * (1 + len(pieces) + len(extra)),
        out_specs=VMEM,
        compiler_params=pltpu.CompilerParams(vmem_limit_bytes=40 * 2**20),
        name="pick",
    )(ids, index, *pieces, *extra)


def head_stage(level, ids, rows, wanted, share, head_weight):
    height, width = rows.shape
    out_width = head_weight.shape[1]

    def body(ids_ref, rows_ref, wanted_ref, share_ref, head_ref, cot_ref, new_ref):
        @pl.when(ids_ref[0] == level)
        def _():
            nb = out_width // BLOCKS

            def block(n, loss):
                cols = pl.ds(pl.multiple_of(n * nb, nb), nb)
                outputs = jnp.dot(rows_ref[...], head_ref[:, cols], preferred_element_type=F32)
                mismatch = outputs - wanted_ref[:, cols].astype(F32)
                scaled = share_ref[...] * mismatch
                cot_ref[:height, cols] = (2.0 * scaled).astype(BF16)
                return loss + jnp.sum(scaled * mismatch, axis=1, keepdims=True)

            loss = lax.fori_loop(0, BLOCKS, block, jnp.zeros((height, 1), F32))
            loss = jnp.sum(loss, axis=0, keepdims=True)
            line = lax.broadcasted_iota(jnp.int32, (EXTRA, out_width), 0)
            high = loss.astype(BF16).astype(F32)
            tail = jnp.where(line == 0, high, jnp.where(line == 1, loss - high, 0.0))
            cot_ref[height:, :] = tail.astype(BF16)
            kb = width // BLOCKS

            def back_block(k, carry):
                cols = pl.ds(pl.multiple_of(k * kb, kb), kb)
                new_ref[:, cols] = lax.dot_general(
                    cot_ref[:height, :], head_ref[cols, :], (((1,), (1,)), ((), ())), preferred_element_type=F32
                ).astype(BF16)
                return carry

            lax.fori_loop(0, BLOCKS, back_block, 0)

    return pl.pallas_call(
        body,
        out_shape=[
            jax.ShapeDtypeStruct((height + EXTRA, out_width), BF16),
            jax.ShapeDtypeStruct((height, width), BF16),
        ],
        in_specs=[SMEM] + [VMEM] * 4,
        out_specs=[VMEM] * 2,
        cost_estimate=pl.CostEstimate(flops=2 * height * width * width * 4, bytes_accessed=2 * width * out_width, transcendentals=0),
        compiler_params=pltpu.CompilerParams(vmem_limit_bytes=40 * 2**20),
        name="head",
    )(ids, rows, wanted, share, head_weight)


def local(
    inputs, tangents, targets, target_jac, rank_mask, batch_order, encoder, layers, head_weight
):
    samp_dev, rank = rank_mask.shape
    in_width = inputs.shape[1]
    width = layers.shape[2]
    out_width = head_weight.shape[1]
    n_dp = lax.axis_size("dp")
    n_mp = lax.axis_size("mp")
    n_sec = lax.axis_size("section")
    last = n_sec - 1
    dp_index = lax.axis_index("dp")
    sec = lax.axis_index("section")
    mp_index = lax.axis_index("mp")
    prims = n_mp * samp_dev
    blk = width // (n_dp * n_mp)

    own_rank = jnp.sum(rank_mask, axis=1)
    slot_line = jnp.arange(samp_dev, dtype=jnp.int32)
    own_slot = jnp.sum(
        jnp.where(batch_order[0][None, :] == slot_line[:, None], slot_line[None, :], 0), axis=1
    ) // (samp_dev // MB)
    own_meta = jnp.stack([own_rank, own_slot]).astype(jnp.int32)
    meta_pieces = jnp.stack(mp_pieces(own_meta))
    order_line = jnp.arange(n_mp, dtype=jnp.int32)
    swap = ((order_line[:, None] ^ mp_index) == order_line[None, :]).astype(jnp.int32)
    meta = jnp.sum(swap[:, :, None, None] * meta_pieces[None], axis=1)
    ranks = meta[:, 0].reshape(prims)
    slots = meta[:, 1].reshape(prims)
    sample_line = jnp.arange(prims, dtype=jnp.int32)
    ends = jnp.sum(jnp.where(sample_line[None, :] <= sample_line[:, None], ranks[None, :], 0), axis=1)
    active = jnp.sum(ranks)
    counts = jnp.sum(jnp.where(slots[None, :] == slots[:, None], ranks[None, :] + 1, 0), axis=1)
    inverse = 1.0 / counts.astype(F32)
    other_active = dp_swap(active.reshape(1, 1)).reshape(()) if n_dp > 1 else active
    most_active = jnp.maximum(active, other_active)

    piece_rows = round_up(samp_dev * (rank + 1), 16)
    pad = piece_rows - samp_dev * (rank + 1)

    def join(flat, deep):
        wide = deep.shape[-1]
        return jnp.concatenate([deep.reshape(-1, wide), flat, jnp.zeros((pad, wide), flat.dtype)], axis=0)

    row_pieces = mp_pieces(join(inputs, tangents))
    weights = Weights(layers[0])
    goal = after(join(targets, target_jac), weights.last)
    goal_pieces = mp_pieces(goal)
    ids = jnp.stack(
        [sec] + weights.offsets + [mp_index ^ k for k in range(n_mp)]
    ).astype(jnp.int32)

    def run(chunks, height):
        slots_here = chunks * height - prims
        place = mp_index * slots_here + jnp.arange(slots_here, dtype=jnp.int32)
        passed = ends[None, :] <= place[:, None]
        sample = jnp.sum(passed.astype(jnp.int32), axis=1)
        column = place - jnp.sum(jnp.where(passed, ranks[None, :], 0), axis=1)
        present = place < active
        belongs = (sample[:, None] == sample_line[None, :]) & present[:, None]
        source = ((sample // samp_dev) ^ mp_index) * piece_rows + (sample % samp_dev) * rank + column
        source = jnp.where(present, source, -1)
        source_p = ((sample_line // samp_dev) ^ mp_index) * piece_rows + samp_dev * rank + sample_line % samp_dev
        share = jnp.sum(jnp.where(belongs, inverse[None, :], 0.0), axis=1)
        share_p = jnp.where(sample_line // samp_dev == mp_index, inverse, 0.0)
        index = jnp.concatenate([source_p, source])[:, None]
        shares = jnp.concatenate([share_p, share])[:, None]
        onehot = belongs.astype(BF16)
        first = height - prims
        cuts = [(0, first)] + [(first + c * height, first + (c + 1) * height) for c in range(chunks - 1)]
        onehots = [onehot[a:b] for a, b in cuts]
        onehots_t = [onehot[a:b].T for a, b in cuts]

        start = pick_rows(ids, index, row_pieces, 0, encoder)
        wanted = pick_rows(ids, index, goal_pieces, last)
        cut = lambda array, c: array[c * height : (c + 1) * height]

        rows = [cut(start, c) for c in range(chunks)]
        entered = [[] for _ in range(chunks)]
        pres = [[] for _ in range(chunks)]
        tanhs = []
        for level in range(n_sec):
            for c in range(chunks):
                entered[c].append(rows[c])
                got = fwd_stage(level, weights, ids, rows[c], onehots[c], None if c == 0 else tanhs[level])
                pres[c].append(got[1])
                if c == 0:
                    tanhs.append(got[2])
                rows[c] = got[0] if level == last else hop(got[0], level, level + 1)

        heads = [head_stage(last, ids, rows[c], cut(wanted, c), cut(shares, c), head_weight) for c in range(chunks)]
        backward_order = list(range(1, chunks)) + [0]
        cots = [heads[c][1] for c in range(chunks)]
        mixes = [None] * chunks
        for level in range(last, -1, -1):
            total = None
            for c in backward_order:
                got = bwd_stage(
                    level, weights, ids, cots[c], pres[c][level], tanhs[level],
                    onehots[c], onehots_t[c], total, c == 0,
                )
                total = got[1]
                mixes[c] = got[0] if mixes[c] is None else jnp.where(sec == level, got[0], mixes[c])
                if level > 0:
                    cots[c] = hop(got[2], level, level - 1)

        def exchange_columns(array):
            blocks = array.reshape(array.shape[0], n_dp, n_mp, blk)

            def block_pair(k):
                part = lax.dynamic_slice_in_dim(blocks, mp_index ^ k, 1, 2)
                return part.reshape(array.shape[0], n_dp * blk)

            got = jnp.concatenate(
                [block_pair(0)] + [mp_swap(block_pair(k), k) for k in range(1, n_mp)], axis=0
            )
            mine = lax.dynamic_slice_in_dim(got, dp_index * blk, blk, 1)
            if n_dp == 1:
                return mine
            theirs = lax.dynamic_slice_in_dim(got, (1 - dp_index) * blk, blk, 1)
            return jnp.concatenate([mine, dp_swap(theirs)], axis=0)

        def gather_rows(array):
            got = jnp.concatenate(mp_pieces(array), axis=0)
            return got if n_dp == 1 else jnp.concatenate([got, dp_swap(got)], axis=0)

        hidden = []
        for c in range(chunks):
            mine = entered[c][0]
            for level in range(1, n_sec):
                mine = jnp.where(sec == level, entered[c][level], mine)
            hidden.append(mine)
        zero_rows = jnp.zeros((EXTRA, width), BF16)
        final = jnp.concatenate([x for c in range(chunks) for x in (rows[c], zero_rows)], axis=0)
        final_blocks = exchange_columns(final)
        cot_all = gather_rows(jnp.concatenate([heads[c][0] for c in range(chunks)], axis=0))
        contract = (((0,), (0,)), ((), ()))
        grad_head = lax.dot_general(final_blocks, cot_all, contract, preferred_element_type=F32)
        tails = cot_all.reshape(-1, height + EXTRA, out_width)[:, height : height + 2, :1]
        loss = jnp.sum(tails.astype(F32)) / (n_dp * MB * out_width)
        loss_high = lax.reduce_precision(loss, 8, 7)
        cols = out_width // n_sec
        line = lax.broadcasted_iota(jnp.int32, (EXTRA, cols), 0)
        loss_rows = jnp.where(line == 0, loss_high, jnp.where(line == 1, loss - loss_high, 0.0))

        def head_block(j):
            return jnp.concatenate([grad_head[:, j * cols : (j + 1) * cols], loss_rows], axis=0).astype(BF16)

        arrived = jnp.zeros((blk + EXTRA, cols), F32)
        for j in range(last):
            arrived = arrived + hop(head_block(j), last, j).astype(F32)
        arrived = jnp.where(sec == last, head_block(last).astype(F32), arrived)
        grad_head_mine = arrived[:blk]
        loss_mine = arrived[blk, 0] + arrived[blk + 1, 0]

        grad = None
        if n_dp * n_mp > 8:
            joined = jnp.concatenate(hidden, axis=0)
            part = lax.dot_general(joined, jnp.concatenate(mixes, axis=0), contract, preferred_element_type=F32)
            grad = lax.psum_scatter(part.astype(BF16), ("dp", "mp"), scatter_dimension=0, tiled=True)
            return grad.astype(F32)[None], grad_head_mine, loss_mine
        hidden_blocks = [exchange_columns(hidden[c]) for c in range(chunks)]
        for c in backward_order:
            part = lax.dot_general(
                hidden_blocks[c], gather_rows(mixes[c]), contract, preferred_element_type=F32
            )
            grad = part if grad is None else grad + part
        return grad[None], grad_head_mine, loss_mine

    def plain():
        depth = rank + 1
        total_rows = samp_dev * depth
        layer_full = jnp.zeros((width, width), BF16)
        kb = weights.block_rows
        for array, block, which, base in weights.pieces:
            row = (mp_index ^ block) * kb + base
            row = row if which is None else row + weights.offsets[which]
            layer_full = lax.dynamic_update_slice_in_dim(layer_full, array, row, 0)
        rows_in = jnp.concatenate([inputs[:, None, :], tangents], axis=1).reshape(total_rows, in_width)
        start = jnp.dot(rows_in, encoder, preferred_element_type=F32).astype(BF16)
        chain = [(j, j + 1) for j in range(last)]

        def pre_of(rows):
            pre = jnp.dot(rows, layer_full, preferred_element_type=F32).reshape(samp_dev, depth, width)
            tanh_p = jnp.tanh(pre[:, 0])
            return pre, tanh_p, 1.0 - tanh_p * tanh_p

        def forward(level, state):
            rows, mine, final = state
            mine = jnp.where(level == sec, rows, mine)
            pre, tanh_p, slope = pre_of(rows)
            change = jnp.concatenate([tanh_p[:, None], slope[:, None] * pre[:, 1:]], axis=1)
            new = (rows.astype(F32) + change.reshape(total_rows, width)).astype(BF16)
            return lax.ppermute(new, "section", chain), mine, new

        _, mine, final = lax.fori_loop(0, n_sec, forward, (start, start, start))
        own = lax.dynamic_slice_in_dim(inverse, mp_index * samp_dev, samp_dev, 0)
        row_weight = jnp.concatenate([jnp.ones((samp_dev, 1), F32), rank_mask.astype(F32)], axis=1)
        share = (row_weight * own[:, None]).reshape(total_rows, 1)
        outputs = jnp.dot(final, head_weight, preferred_element_type=F32)
        wanted = jnp.concatenate([targets[:, None, :], target_jac], axis=1).reshape(total_rows, out_width)
        mismatch = outputs - wanted.astype(F32)
        loss = jnp.sum(share * mismatch * mismatch)
        cot_out = (2.0 * share * mismatch).astype(BF16)
        cot = lax.dot_general(cot_out, head_weight, (((1,), (1,)), ((), ())), preferred_element_type=F32)
        pre, tanh_p, slope = pre_of(mine)

        def backward(step, state):
            cot, mix_mine = state
            up = cot.astype(F32).reshape(samp_dev, depth, width)
            side = jnp.sum(up[:, 1:] * pre[:, 1:], axis=1)
            lead = up[:, 0] * slope - 2.0 * side * tanh_p * slope
            mix = jnp.concatenate([lead[:, None], up[:, 1:] * slope[:, None]], axis=1)
            mix = mix.astype(BF16).reshape(total_rows, width)
            mix_mine = jnp.where(step == last - sec, mix, mix_mine)
            back = lax.dot_general(mix, layer_full, (((1,), (1,)), ((), ())), preferred_element_type=F32)
            new = (up.reshape(total_rows, width) + back).astype(BF16)
            return lax.ppermute(new, "section", [(j + 1, j) for j in range(last)]), mix_mine

        _, mix = lax.fori_loop(0, n_sec, backward, (cot.astype(BF16), mine))

        def scatter(left, right):
            part = lax.dot_general(left, right, (((0,), (0,)), ((), ())), preferred_element_type=F32)
            part = part.astype(BF16).reshape(n_dp, n_mp, blk, right.shape[1])
            mine_part = jnp.zeros((n_dp, blk, right.shape[1]), F32)
            for k in range(n_mp):
                piece = lax.dynamic_index_in_dim(part, mp_index ^ k, 1, False)
                mine_part = mine_part + (piece if k == 0 else mp_swap(piece, k)).astype(F32)
            kept = lax.dynamic_index_in_dim(mine_part, dp_index, 0, False)
            if n_dp > 1:
                sent = lax.dynamic_index_in_dim(mine_part, 1 - dp_index, 0, False)
                kept = kept + dp_swap(sent.astype(BF16)).astype(F32)
            return kept

        grad = scatter(mine, mix)
        head = scatter(final, cot_out)
        cols = out_width // n_sec
        loss_group = sum(mp_pieces(loss.reshape(1, 1)))
        if n_dp > 1:
            loss_group = loss_group + dp_swap(loss_group)
        head_mine = jnp.where(sec == last, head[:, last * cols :], 0.0)
        loss_mine = jnp.where(sec == last, loss_group, 0.0)
        for j in range(last):
            head_mine = head_mine + hop(head[:, j * cols : (j + 1) * cols].astype(BF16), last, j).astype(F32)
            loss_mine = loss_mine + hop(loss_group, last, j)
        return grad[None], head_mine, loss_mine.reshape(()) / (n_dp * MB * out_width)

    usual = samp_dev * (rank // 2 + 1)
    height = max(round_up(-(-(prims + usual) // 2), 16), round_up(prims + 8, 16))
    fast = run(2, height)
    room = n_mp * (2 * height - prims)
    if room >= n_mp * samp_dev * rank:
        return fast
    return lax.cond(most_active <= room, lambda: fast, plain)


def solution(mesh):
    in_specs = (
        P(("dp", "mp"), None),
        P(("dp", "mp"), None, None),
        P(("dp", "mp"), None),
        P(("dp", "mp"), None, None),
        P(("dp", "mp"), None),
        P(("dp", "mp"), None),
        P(),
        P("section", "mp", None),
        P(),
    )
    out_specs = (P("section", ("dp", "mp"), None), P(("dp", "mp"), "section"), P())
    return jax.shard_map(local, mesh=mesh, in_specs=in_specs, out_specs=out_specs, check_vma=False)
```

```python
import jax
import jax.numpy as jnp
from jax import lax
from jax.experimental import pallas as pl
from jax.experimental.pallas import tpu as pltpu
from jax.sharding import PartitionSpec as P


F32 = jnp.float32
BF16 = jnp.bfloat16
MB = 6
EXTRA = 16
BLOCKS = 4

ANY = pl.BlockSpec(memory_space=pl.ANY)
SMEM = pl.BlockSpec(memory_space=pltpu.SMEM)
VMEM = pl.BlockSpec(memory_space=pltpu.VMEM)


def round_up(value, unit):
    return -(-value // unit) * unit


def mp_swap(value, flip):
    count = lax.axis_size("mp")
    return lax.ppermute(value, "mp", [(m, m ^ flip) for m in range(count)])


def dp_swap(value):
    count = lax.axis_size("dp")
    return lax.ppermute(value, "dp", [(d, d ^ 1) for d in range(count)])


def mp_pieces(value):
    return [value] + [mp_swap(value, k) for k in range(1, lax.axis_size("mp"))]


def hop(value, source, target):
    return lax.ppermute(value, "section", [(source, target)])


def plane_pieces(value, section):
    count = lax.axis_size("mp")
    base = section * count
    swaps = [[(base + m, base + (m ^ k)) for m in range(count)] for k in range(1, count)]
    return [value] + [lax.ppermute(value, ("section", "mp"), pairs) for pairs in swaps]


def after(value, *others):
    return lax.optimization_barrier((value,) + others)[0]


def params():
    return pltpu.CompilerParams(vmem_limit_bytes=40 * 2**20)


def run_copies(copies):
    for copy in copies:
        copy.start()
    for copy in copies:
        copy.wait()


def spread(onehot, value):
    high = value.astype(BF16)
    low = (value - high.astype(F32)).astype(BF16)
    return jnp.dot(onehot, high, preferred_element_type=F32) + jnp.dot(
        onehot, low, preferred_element_type=F32
    )


class Weights:
    def __init__(self, layer):
        self.count = lax.axis_size("mp")
        self.block_rows, self.width = layer.shape
        dp_index = lax.axis_index("dp")
        half = self.block_rows // 2
        self.offsets = [dp_index * half, (1 - dp_index) * half]
        self.pieces = [(layer, 0, None, 0)]
        if self.count == 4 and lax.axis_size("dp") == 2:
            part = half // 2
            first = lax.dynamic_slice_in_dim(layer, dp_index * half, part, 0)
            second = lax.dynamic_slice_in_dim(layer, dp_index * half + part, part, 0)
            a1 = mp_swap(first, 1)
            b2 = mp_swap(second, 2)
            b1 = mp_swap(second, 1)
            a2 = mp_swap(first, 2)
            a3 = mp_swap(a1, 2)
            b3 = mp_swap(b2, 1)
            got = [(a1, 1, 0), (b2, 2, part), (b1, 1, part), (a2, 2, 0), (a3, 3, 0), (b3, 3, part)]
            for array, block, base in got:
                self.pieces.append((array, block, 0, base))
                self.pieces.append((dp_swap(array), block, 1, base))
            self.last = a3
        else:
            for block in range(1, self.count):
                self.pieces.append((mp_swap(layer, block), block, None, 0))
            self.last = self.pieces[-1][0]

    def arrays(self):
        return [piece[0] for piece in self.pieces]

    def start(self, ids, refs, buf, sems, by_column):
        for n in range(BLOCKS if by_column else 1):
            for ref, (array, block, which, base) in zip(refs, self.pieces):
                row = block * self.block_rows + base
                if which is not None:
                    row = row + pl.multiple_of(ids[1 + which], self.block_rows // 2)
                dst = buf.at[pl.ds(row, array.shape[0]), :]
                if by_column:
                    col = self.width // BLOCKS
                    ref_n, dst, sem = ref.at[:, n * col : (n + 1) * col], dst.at[:, n * col : (n + 1) * col], n
                else:
                    ref_n, sem = ref, block
                pltpu.make_async_copy(ref_n, dst, sems.at[sem]).start()

    def scratch(self, by_column):
        return [
            pltpu.VMEM((self.count * self.block_rows, self.width), BF16),
            pltpu.SemaphoreType.DMA((BLOCKS if by_column else self.count,)),
        ]


def finish(view, sem):
    pltpu.make_async_copy(view, view, sem).wait()


def fwd_stage(level, weights, ids, rows, onehot, slope, kept):
    height, width = rows.shape
    prims = onehot.shape[1]
    leads = slope is None
    pieces = len(weights.pieces)
    kb = weights.block_rows
    nb = width // BLOCKS

    def body(ids_ref, rows_ref, onehot_ref, *rest):
        if not leads:
            slope_ref, *rest = rest
        w_refs, rest = rest[:pieces], rest[pieces + (kept is not None) :]
        next_ref, pre_ref, kept_ref, *rest = rest
        if leads:
            tanh_ref, *rest = rest
        buf, sems, turned, kept_sem = rest

        @pl.when(ids_ref[0] == level)
        def _():
            weights.start(ids_ref, w_refs, buf, sems, True)
            keep = pltpu.make_async_copy(rows_ref, kept_ref, kept_sem)
            keep.start()
            for k in range(weights.count):
                col = pl.multiple_of(ids_ref[3 + k] * kb, kb)
                turned[:, k * kb : (k + 1) * kb] = rows_ref[:, pl.ds(col, kb)]

            def block(n, carry):
                cols = pl.ds(pl.multiple_of(n * nb, nb), nb)
                view = buf.at[:, cols]
                finish(view, sems.at[n])
                acc = jnp.dot(turned[...], view[...], preferred_element_type=F32)
                old = rows_ref[:, cols].astype(F32)
                pre_ref[:, cols] = acc.astype(BF16)
                if leads:
                    tanh_p = jnp.tanh(acc[:prims])
                    tanh_ref[:, cols] = tanh_p
                    factor = spread(onehot_ref[...], 1.0 - tanh_p * tanh_p)
                    new = jnp.concatenate(
                        [old[:prims] + tanh_p, old[prims:] + factor * acc[prims:]], axis=0
                    )
                else:
                    tanh_p = slope_ref[:, cols]
                    new = old + spread(onehot_ref[...], 1.0 - tanh_p * tanh_p) * acc
                next_ref[:, cols] = new.astype(BF16)
                return carry

            lax.fori_loop(0, BLOCKS, block, 0)
            keep.wait()

    outs = [jax.ShapeDtypeStruct((height, width), BF16)] * 3
    if leads:
        outs.append(jax.ShapeDtypeStruct((prims, width), F32))
    args = [ids, rows, onehot] + ([] if leads else [slope]) + weights.arrays()
    specs = [SMEM, VMEM, VMEM] + ([] if leads else [VMEM]) + [ANY] * pieces
    alias = {}
    if kept is not None:
        alias = {len(args): 2}
        args.append(kept)
        specs.append(ANY)
    return pl.pallas_call(
        body,
        out_shape=outs,
        in_specs=specs,
        out_specs=[VMEM, VMEM, ANY] + [VMEM] * (len(outs) - 3),
        input_output_aliases=alias,
        scratch_shapes=weights.scratch(True) + [pltpu.VMEM((height, width), BF16), pltpu.SemaphoreType.DMA],
        cost_estimate=pl.CostEstimate(flops=2 * height * width * width * 4, bytes_accessed=2 * width * width, transcendentals=0),
        compiler_params=params(),
        name=f"fwd{level}",
    )(*args)


def bwd_stage(level, weights, ids, cot, pre, tanh_p, onehot, onehot_t, total, leads, kept):
    height, width = cot.shape
    prims = tanh_p.shape[0]
    deep = level > 0
    pieces = len(weights.pieces) if deep else 0
    kb = weights.block_rows
    nb = width // BLOCKS

    def body(ids_ref, cot_ref, pre_ref, tanh_ref, onehot_ref, onehot_t_ref, *rest):
        if total is not None:
            total_ref, *rest = rest
        w_refs, rest = rest[:pieces], rest[pieces + (kept is not None) :]
        kept_ref, side_ref, *rest = rest
        if deep:
            new_ref, mix_ref, kept_sem, buf, sems = rest
        else:
            mix_ref, kept_sem = rest

        @pl.when(ids_ref[0] == level)
        def _():
            if deep:
                weights.start(ids_ref, w_refs, buf, sems, False)
            skip = prims if leads else 0

            def block(n, carry):
                cols = pl.ds(pl.multiple_of(n * nb, nb), nb)
                up = cot_ref[:, cols].astype(F32)
                tanh = tanh_ref[:, cols]
                slope = 1.0 - tanh * tanh
                up_t = up[skip:]
                mix_t = up_t * spread(onehot_ref[...], slope)
                total_here = spread(onehot_t_ref[...], up_t * pre_ref[:, cols].astype(F32)[skip:])
                if total is not None:
                    total_here = total_here + total_ref[:, cols]
                if leads:
                    mix_p = up[:prims] * slope - 2.0 * total_here * tanh * slope
                    mix_ref[:, cols] = jnp.concatenate([mix_p, mix_t], axis=0).astype(BF16)
                else:
                    mix_ref[:, cols] = mix_t.astype(BF16)
                side_ref[:, cols] = total_here
                return carry

            lax.fori_loop(0, BLOCKS, block, 0)
            keep = pltpu.make_async_copy(mix_ref, kept_ref, kept_sem)
            keep.start()
            if deep:

                def back_block(k, carry):
                    view = buf.at[pl.ds(pl.multiple_of(k * kb, kb), kb), :]
                    finish(view, sems.at[k])
                    cols = pl.ds(pl.multiple_of(ids_ref[3 + k] * kb, kb), kb)
                    back = lax.dot_general(
                        mix_ref[...], view[...], (((1,), (1,)), ((), ())), preferred_element_type=F32
                    )
                    new_ref[:, cols] = (cot_ref[:, cols].astype(F32) + back).astype(BF16)
                    return carry

                lax.fori_loop(0, weights.count, back_block, 0)
            keep.wait()

    rows_shape = jax.ShapeDtypeStruct((height, width), BF16)
    outs = [rows_shape, jax.ShapeDtypeStruct((prims, width), F32)] + ([rows_shape] if deep else [])
    args = [ids, cot, pre, tanh_p, onehot, onehot_t] + ([] if total is None else [total])
    specs = [SMEM] + [VMEM] * (len(args) - 1) + [ANY] * pieces
    args += weights.arrays() if deep else []
    alias = {}
    if kept is not None:
        alias = {len(args): 0}
        args.append(kept)
        specs.append(ANY)
    return pl.pallas_call(
        body,
        out_shape=outs,
        in_specs=specs,
        out_specs=[ANY] + [VMEM] * (len(outs) - 1),
        input_output_aliases=alias,
        scratch_shapes=[pltpu.VMEM((height, width), BF16), pltpu.SemaphoreType.DMA]
        + (weights.scratch(False) if deep else []),
        cost_estimate=pl.CostEstimate(flops=2 * height * width * width * 4, bytes_accessed=2 * width * width, transcendentals=0),
        compiler_params=params(),
        name=f"bwd{level}",
    )(*args)


def pick_rows(ids, index, pieces, level):
    height = index.shape[0]
    piece_rows, width = pieces[0].shape

    def body(ids_ref, index_ref, *rest):
        out_ref = rest[-1]

        @pl.when(ids_ref[0] == level)
        def _():
            index_here = index_ref[...]
            acc = jnp.zeros((height, width), F32)
            for k, piece_ref in enumerate(rest[:-1]):
                place = lax.broadcasted_iota(jnp.int32, (height, piece_rows), 1) + k * piece_rows
                onehot = jnp.where(place == index_here, 1.0, 0.0).astype(BF16)
                acc = acc + jnp.dot(onehot, piece_ref[...], preferred_element_type=F32)
            out_ref[...] = acc.astype(BF16)

    return pl.pallas_call(
        body,
        out_shape=jax.ShapeDtypeStruct((height, width), BF16),
        in_specs=[SMEM] + [VMEM] * (1 + len(pieces)),
        out_specs=VMEM,
        compiler_params=params(),
        name="pick",
    )(ids, index, *pieces)


def lift_rows(ids, rows, encoder, chunks):
    height = rows.shape[0] // chunks
    width = encoder.shape[1]

    def body(ids_ref, rows_ref, encoder_ref, *outs):
        @pl.when(ids_ref[0] == 0)
        def _():
            for c, out in enumerate(outs):
                part = rows_ref[c * height : (c + 1) * height, :]
                out[...] = jnp.dot(part, encoder_ref[...], preferred_element_type=F32).astype(BF16)

    return pl.pallas_call(
        body,
        out_shape=[jax.ShapeDtypeStruct((height, width), BF16)] * chunks,
        in_specs=[SMEM, VMEM, VMEM],
        out_specs=[VMEM] * chunks,
        compiler_params=params(),
        name="lift",
    )(ids, rows, encoder)


def pack_columns(ids, chunks, tails, level, n_dp, n_mp, blk):
    count = len(chunks)
    height, width = chunks[0].shape
    tail_rows, tail_width = tails[0].shape if tails else (height, 0)
    core = n_dp * blk

    def body(ids_ref, *refs):
        chunk_refs, rest = refs[:count], refs[count:]
        tail_refs, outs = rest[: len(tails)], rest[len(tails) :]

        def fill():
            for k, out in enumerate(outs):
                for c, chunk_ref in enumerate(chunk_refs):
                    first = c * tail_rows
                    for d in range(n_dp):
                        col = pl.multiple_of((ids_ref[3 + k] + d * n_mp) * blk, blk)
                        out[first : first + height, d * blk : (d + 1) * blk] = chunk_ref[:, pl.ds(col, blk)]
                    if tails:
                        out[first + height : first + tail_rows, :core] = jnp.zeros((EXTRA, core), BF16)
                        out[first : first + tail_rows, core:] = tail_refs[c][...]

        if level is None:
            fill()
        else:
            pl.when(ids_ref[0] == level)(fill)

    shape = jax.ShapeDtypeStruct((count * tail_rows, core + tail_width), BF16)
    return pl.pallas_call(
        body,
        out_shape=[shape] * n_mp,
        in_specs=[SMEM] + [VMEM] * (count + len(tails)),
        out_specs=[VMEM] * n_mp,
        compiler_params=params(),
        name="pack",
    )(ids, *chunks, *tails)


def both_groups(pieces):
    return pieces + ([dp_swap(piece) for piece in pieces] if lax.axis_size("dp") > 1 else [])


def head_gradient(ids, pieces, level, blk, n_sec, height):
    rows_each, wide = pieces[0].shape
    core = 2 * blk
    out_width = wide - core
    cols = out_width // n_sec
    many = len(pieces)

    def body(ids_ref, *refs):
        piece_refs, outs = refs[:many], refs[many : many + n_sec]
        left, right, sems = refs[many + n_sec :]

        @pl.when(ids_ref[0] == level)
        def _():
            mine = pl.multiple_of(ids_ref[1] // ids_ref[7] * blk, blk)
            copies = []
            for i, ref in enumerate(piece_refs):
                rows = pl.ds(i * rows_each, rows_each)
                copies.append(pltpu.make_async_copy(ref.at[:, pl.ds(mine, blk)], left.at[rows], sems.at[0, i]))
                copies.append(pltpu.make_async_copy(ref.at[:, core:], right.at[rows], sems.at[1, i]))
            run_copies(copies)
            loss = jnp.zeros((1, 128), F32)
            for first in range(height, many * rows_each, height + EXTRA):
                loss = loss + right[first : first + 1, :128].astype(F32) + right[first + 1 : first + 2, :128].astype(F32)
            high = loss[:, :1].astype(BF16).astype(F32)
            line = lax.broadcasted_iota(jnp.int32, (EXTRA, cols), 0)
            tail = jnp.where(line == 0, high, jnp.where(line == 1, loss[:, :1] - high, 0.0)).astype(BF16)
            for j, out in enumerate(outs):
                out[:blk, :] = lax.dot_general(
                    left[...], right[:, j * cols : (j + 1) * cols], (((0,), (0,)), ((), ())),
                    preferred_element_type=F32,
                ).astype(BF16)
                out[blk:, :] = tail

    return pl.pallas_call(
        body,
        out_shape=[jax.ShapeDtypeStruct((blk + EXTRA, cols), BF16)] * n_sec,
        in_specs=[SMEM] + [ANY] * many,
        out_specs=[VMEM] * n_sec,
        scratch_shapes=[
            pltpu.VMEM((many * rows_each, blk), BF16),
            pltpu.VMEM((many * rows_each, out_width), BF16),
            pltpu.SemaphoreType.DMA((2, many)),
        ],
        compiler_params=params(),
        name="grad_head",
    )(ids, *pieces)


def layer_gradient(ids, blocks, chunk, mixes, blk, height, before):
    many = len(mixes)
    width = mixes[0].shape[1]
    nb = width // BLOCKS

    def body(ids_ref, *refs):
        block_refs, mix_refs = refs[:many], refs[many : 2 * many]
        rest = refs[2 * many :]
        if before is not None:
            before_ref, *rest = rest
        out, left, right, turned, sems = rest
        mine = pl.multiple_of(ids_ref[1] // ids_ref[7] * blk, blk)
        top = chunk * height
        copies = []
        for i in range(many):
            rows = pl.ds(i * height, height)
            src = block_refs[i].at[top : top + height, pl.ds(mine, blk)]
            copies.append(pltpu.make_async_copy(src, left.at[rows], sems.at[0, i]))
            copies.append(pltpu.make_async_copy(mix_refs[i], right.at[rows], sems.at[1, i]))
        run_copies(copies)
        turned[...] = left[...].astype(F32).T.astype(BF16)

        def block(n, carry):
            cols = pl.ds(pl.multiple_of(n * nb, nb), nb)
            part = jnp.dot(turned[...], right[:, cols], preferred_element_type=F32)
            if before is not None:
                part = part + before_ref[:, cols]
            out[:, cols] = part
            return carry

        lax.fori_loop(0, BLOCKS, block, 0)

    return pl.pallas_call(
        body,
        out_shape=jax.ShapeDtypeStruct((blk, width), F32),
        in_specs=[SMEM] + [ANY] * (2 * many) + ([] if before is None else [VMEM]),
        out_specs=VMEM,
        scratch_shapes=[
            pltpu.VMEM((many * height, blk), BF16),
            pltpu.VMEM((many * height, width), BF16),
            pltpu.VMEM((blk, many * height), BF16),
            pltpu.SemaphoreType.DMA((2, many)),
        ],
        compiler_params=params(),
        name="grad_layer",
    )(ids, *blocks, *mixes, *([] if before is None else [before]))


def head_stage(level, ids, rows, wanted, share, head_weight):
    height, width = rows.shape
    out_width = head_weight.shape[1]

    def body(ids_ref, rows_ref, wanted_ref, share_ref, head_ref, cot_ref, new_ref):
        @pl.when(ids_ref[0] == level)
        def _():
            nb = out_width // BLOCKS

            def block(n, loss):
                cols = pl.ds(pl.multiple_of(n * nb, nb), nb)
                outputs = jnp.dot(rows_ref[...], head_ref[:, cols], preferred_element_type=F32)
                mismatch = outputs - wanted_ref[:, cols].astype(F32)
                scaled = share_ref[...] * mismatch
                cot_ref[:height, cols] = (2.0 * scaled).astype(BF16)
                return loss + jnp.sum(scaled * mismatch, axis=1, keepdims=True)

            loss = lax.fori_loop(0, BLOCKS, block, jnp.zeros((height, 1), F32))
            loss = jnp.sum(loss, axis=0, keepdims=True)
            line = lax.broadcasted_iota(jnp.int32, (EXTRA, out_width), 0)
            high = loss.astype(BF16).astype(F32)
            tail = jnp.where(line == 0, high, jnp.where(line == 1, loss - high, 0.0))
            cot_ref[height:, :] = tail.astype(BF16)
            kb = width // BLOCKS

            def back_block(k, carry):
                cols = pl.ds(pl.multiple_of(k * kb, kb), kb)
                new_ref[:, cols] = lax.dot_general(
                    cot_ref[:height, :], head_ref[cols, :], (((1,), (1,)), ((), ())), preferred_element_type=F32
                ).astype(BF16)
                return carry

            lax.fori_loop(0, BLOCKS, back_block, 0)

    return pl.pallas_call(
        body,
        out_shape=[
            jax.ShapeDtypeStruct((height + EXTRA, out_width), BF16),
            jax.ShapeDtypeStruct((height, width), BF16),
        ],
        in_specs=[SMEM] + [VMEM] * 4,
        out_specs=[VMEM] * 2,
        cost_estimate=pl.CostEstimate(flops=2 * height * width * width * 4, bytes_accessed=2 * width * out_width, transcendentals=0),
        compiler_params=params(),
        name="head",
    )(ids, rows, wanted, share, head_weight)


def local(
    inputs, tangents, targets, target_jac, rank_mask, batch_order, encoder, layers, head_weight
):
    samp_dev, rank = rank_mask.shape
    in_width = inputs.shape[1]
    width = layers.shape[2]
    out_width = head_weight.shape[1]
    n_dp = lax.axis_size("dp")
    n_mp = lax.axis_size("mp")
    n_sec = lax.axis_size("section")
    last = n_sec - 1
    dp_index = lax.axis_index("dp")
    sec = lax.axis_index("section")
    mp_index = lax.axis_index("mp")
    prims = n_mp * samp_dev
    blk = width // (n_dp * n_mp)

    weights = Weights(layers[0])
    helper = 1 if n_sec > 1 else 0

    piece_rows = round_up(samp_dev * (rank + 1), 16)
    pad = piece_rows - samp_dev * (rank + 1)

    def join(flat, deep):
        wide = deep.shape[-1]
        return jnp.concatenate([deep.reshape(-1, wide), flat, jnp.zeros((pad, wide), flat.dtype)], axis=0)

    row_pieces = plane_pieces(join(inputs, tangents), helper)

    own_rank = jnp.sum(rank_mask, axis=1)
    slot_line = jnp.arange(samp_dev, dtype=jnp.int32)
    own_slot = jnp.sum(
        jnp.where(batch_order[0][None, :] == slot_line[:, None], slot_line[None, :], 0), axis=1
    ) // (samp_dev // MB)
    own_meta = jnp.stack([own_rank, own_slot]).astype(jnp.int32)
    meta_pieces = jnp.stack(mp_pieces(own_meta))
    order_line = jnp.arange(n_mp, dtype=jnp.int32)
    swap = ((order_line[:, None] ^ mp_index) == order_line[None, :]).astype(jnp.int32)
    meta = jnp.sum(swap[:, :, None, None] * meta_pieces[None], axis=1)
    ranks = meta[:, 0].reshape(prims)
    slots = meta[:, 1].reshape(prims)
    sample_line = jnp.arange(prims, dtype=jnp.int32)
    ends = jnp.sum(jnp.where(sample_line[None, :] <= sample_line[:, None], ranks[None, :], 0), axis=1)
    active = jnp.sum(ranks)
    counts = jnp.sum(jnp.where(slots[None, :] == slots[:, None], ranks[None, :] + 1, 0), axis=1)
    inverse = 1.0 / counts.astype(F32)

    kb = width // n_mp
    ids = jnp.stack(
        [sec] + weights.offsets + [mp_index ^ k for k in range(n_mp)] + [jnp.int32(kb // 2)] * (n_mp == 4)
    ).astype(jnp.int32)
    chunks = 2
    usual = samp_dev * (rank // 2 + 1)
    height = max(round_up(-(-(prims + usual) // chunks), 16), round_up(prims + 8, 16))
    slots_here = chunks * height - prims

    place = mp_index * slots_here + jnp.arange(slots_here, dtype=jnp.int32)
    passed = ends[None, :] <= place[:, None]
    sample = jnp.sum(passed.astype(jnp.int32), axis=1)
    column = place - jnp.sum(jnp.where(passed, ranks[None, :], 0), axis=1)
    present = place < active
    belongs = (sample[:, None] == sample_line[None, :]) & present[:, None]
    source = ((sample // samp_dev) ^ mp_index) * piece_rows + (sample % samp_dev) * rank + column
    source = jnp.where(present, source, -1)
    source_p = ((sample_line // samp_dev) ^ mp_index) * piece_rows + samp_dev * rank + sample_line % samp_dev
    share = jnp.sum(jnp.where(belongs, inverse[None, :], 0.0), axis=1)
    share_p = jnp.where(sample_line // samp_dev == mp_index, inverse, 0.0)
    index = jnp.concatenate([source_p, source])[:, None]
    shares = jnp.concatenate([share_p, share])[:, None]
    onehot = belongs.astype(BF16)
    first = height - prims
    onehots = [onehot[:first], onehot[first:]]
    onehots_t = [part.T for part in onehots]
    share_of = [shares[:height], shares[height:]]

    packed = pick_rows(ids, index, row_pieces, helper)
    if helper != 0:
        packed = hop(packed, helper, 0)
    rows = list(lift_rows(ids, packed, encoder, chunks))
    other_active = dp_swap(active.reshape(1, 1)).reshape(()) if n_dp > 1 else active
    most_active = jnp.maximum(active, other_active)

    token = ids
    entered = [None] * chunks
    pres = [[None] * n_sec for _ in range(chunks)]
    tanhs = [None] * n_sec
    heads = [None] * chunks
    goal_pieces = None
    for level in range(n_sec):
        for c in range(chunks):
            got = fwd_stage(
                level, weights, token, rows[c], onehots[c], None if c == 0 else tanhs[level], entered[c]
            )
            token = after(ids, got[0])
            entered[c], pres[c][level] = got[2], got[1]
            if c == 0:
                tanhs[level] = got[3]
            rows[c] = got[0] if level == last else hop(got[0], level, level + 1)
            if level == last:
                heads[c] = head_stage(
                    last, token, rows[c], wanted[c * height : (c + 1) * height], share_of[c], head_weight
                )
                token = after(ids, heads[c][1])
        if goal_pieces is None:
            goal_pieces = plane_pieces(after(join(targets, target_jac), token), last)
        if level == max(last - 1, 0):
            wanted = pick_rows(token, index, goal_pieces, last)
            token = after(ids, wanted)

    small = n_dp * n_mp <= 8 and blk % 128 == 0
    cots = [heads[c][1] for c in range(chunks)]
    mixes = [None] * chunks
    backward_order = list(range(1, chunks)) + [0]
    hidden_pieces = head_pieces = None
    arrived = []
    for level in range(last, -1, -1):
        total = None
        for c in backward_order:
            got = bwd_stage(
                level, weights, token, cots[c], pres[c][level], tanhs[level],
                onehots[c], onehots_t[c], total, c == 0, mixes[c],
            )
            mixes[c], total = got[0], got[1]
            token = after(ids, got[1])
            if level > 0:
                cots[c] = hop(got[2], level, level - 1)
        if not small:
            continue
        if level == last:
            sends = pack_columns(token, rows, [h[0] for h in heads], last, n_dp, n_mp, blk)
            head_sends = sends
            token = after(ids, sends[0])
            base = last * n_mp
            head_pieces = [sends[0]] + [
                lax.ppermute(sends[k], ("section", "mp"), [(base + m, base + (m ^ k)) for m in range(n_mp)])
                for k in range(1, n_mp)
            ]
        elif level == last - 1:
            sends = pack_columns(token, entered, [], None, n_dp, n_mp, blk)
            token = after(ids, sends[0])
            hidden_pieces = [sends[0]] + [mp_swap(sends[k], k) for k in range(1, n_mp)]
            head_pieces = both_groups([after(piece, token) for piece in head_pieces])
        elif level == last - 2:
            blocks = head_gradient(token, head_pieces, last, blk, n_sec, height)
            token = after(ids, blocks[0])
            arrived = [hop(blocks[j], last, j) for j in range(last)]
            hidden_pieces = both_groups([after(piece, token) for piece in hidden_pieces])

    cols = out_width // n_sec
    if small:
        head_ext = blocks[last].astype(F32)
        for j in range(last):
            head_ext = jnp.where(sec == j, arrived[j].astype(F32), head_ext)
        head_mine = head_ext[:blk]
        loss_mine = (head_ext[blk, 0] + head_ext[blk + 1, 0]) / (n_dp * MB * out_width)
        grad = None
        for c in backward_order:
            mix_pieces = both_groups([mixes[c]] + [mp_swap(mixes[c], k) for k in range(1, n_mp)])
            grad = layer_gradient(token, hidden_pieces, c, mix_pieces, blk, height, grad)
    else:
        contract = (((0,), (0,)), ((), ()))
        joined = jnp.concatenate(entered, axis=0)
        part = lax.dot_general(joined, jnp.concatenate(mixes, axis=0), contract, preferred_element_type=F32)
        grad = lax.psum_scatter(part.astype(BF16), ("dp", "mp"), scatter_dimension=0, tiled=True).astype(F32)
        cot_out = jnp.concatenate([h[0][:height] for h in heads], axis=0)
        part = lax.dot_general(jnp.concatenate(rows, axis=0), cot_out, contract, preferred_element_type=F32)
        head = lax.psum_scatter(part.astype(BF16), ("dp", "mp"), scatter_dimension=0, tiled=True)
        loss = sum(jnp.sum(h[0][height : height + 2, 0].astype(F32)) for h in heads)
        loss = jnp.where(sec == last, lax.psum(loss, ("dp", "mp")), 0.0).reshape(1, 1)
        head_mine = jnp.where(sec == last, head[:, last * cols :], jnp.zeros((blk, cols), BF16))
        loss_mine = loss
        for j in range(last):
            head_mine = head_mine + hop(head[:, j * cols : (j + 1) * cols], last, j)
            loss_mine = loss_mine + hop(loss, last, j)
        head_mine = head_mine.astype(F32)
        loss_mine = loss_mine.reshape(()) / (n_dp * MB * out_width)
    fast = (grad[None], head_mine, loss_mine)

    def plain():
        depth = rank + 1
        total_rows = samp_dev * depth
        layer_full = jnp.zeros((width, width), BF16)
        kb = weights.block_rows
        for array, block, which, base in weights.pieces:
            row = (mp_index ^ block) * kb + base
            row = row if which is None else row + weights.offsets[which]
            layer_full = lax.dynamic_update_slice_in_dim(layer_full, array, row, 0)
        rows_in = jnp.concatenate([inputs[:, None, :], tangents], axis=1).reshape(total_rows, in_width)
        start = jnp.dot(rows_in, encoder, preferred_element_type=F32).astype(BF16)
        chain = [(j, j + 1) for j in range(last)]

        def pre_of(rows):
            pre = jnp.dot(rows, layer_full, preferred_element_type=F32).reshape(samp_dev, depth, width)
            tanh_p = jnp.tanh(pre[:, 0])
            return pre, tanh_p, 1.0 - tanh_p * tanh_p

        def forward(level, state):
            rows, mine, final = state
            mine = jnp.where(level == sec, rows, mine)
            pre, tanh_p, slope = pre_of(rows)
            change = jnp.concatenate([tanh_p[:, None], slope[:, None] * pre[:, 1:]], axis=1)
            new = (rows.astype(F32) + change.reshape(total_rows, width)).astype(BF16)
            return lax.ppermute(new, "section", chain), mine, new

        _, mine, final = lax.fori_loop(0, n_sec, forward, (start, start, start))
        own = lax.dynamic_slice_in_dim(inverse, mp_index * samp_dev, samp_dev, 0)
        row_weight = jnp.concatenate([jnp.ones((samp_dev, 1), F32), rank_mask.astype(F32)], axis=1)
        share = (row_weight * own[:, None]).reshape(total_rows, 1)
        outputs = jnp.dot(final, head_weight, preferred_element_type=F32)
        wanted = jnp.concatenate([targets[:, None, :], target_jac], axis=1).reshape(total_rows, out_width)
        mismatch = outputs - wanted.astype(F32)
        loss = jnp.sum(share * mismatch * mismatch)
        cot_out = (2.0 * share * mismatch).astype(BF16)
        cot = lax.dot_general(cot_out, head_weight, (((1,), (1,)), ((), ())), preferred_element_type=F32)
        pre, tanh_p, slope = pre_of(mine)

        def backward(step, state):
            cot, mix_mine = state
            up = cot.astype(F32).reshape(samp_dev, depth, width)
            side = jnp.sum(up[:, 1:] * pre[:, 1:], axis=1)
            lead = up[:, 0] * slope - 2.0 * side * tanh_p * slope
            mix = jnp.concatenate([lead[:, None], up[:, 1:] * slope[:, None]], axis=1)
            mix = mix.astype(BF16).reshape(total_rows, width)
            mix_mine = jnp.where(step == last - sec, mix, mix_mine)
            back = lax.dot_general(mix, layer_full, (((1,), (1,)), ((), ())), preferred_element_type=F32)
            new = (up.reshape(total_rows, width) + back).astype(BF16)
            return lax.ppermute(new, "section", [(j + 1, j) for j in range(last)]), mix_mine

        _, mix = lax.fori_loop(0, n_sec, backward, (cot.astype(BF16), mine))

        def scatter(left, right):
            part = lax.dot_general(left, right, (((0,), (0,)), ((), ())), preferred_element_type=F32)
            part = part.astype(BF16).reshape(n_dp, n_mp, blk, right.shape[1])
            mine_part = jnp.zeros((n_dp, blk, right.shape[1]), F32)
            for k in range(n_mp):
                piece = lax.dynamic_index_in_dim(part, mp_index ^ k, 1, False)
                mine_part = mine_part + (piece if k == 0 else mp_swap(piece, k)).astype(F32)
            kept = lax.dynamic_index_in_dim(mine_part, dp_index, 0, False)
            if n_dp > 1:
                sent = lax.dynamic_index_in_dim(mine_part, 1 - dp_index, 0, False)
                kept = kept + dp_swap(sent.astype(BF16)).astype(F32)
            return kept

        grad = scatter(mine, mix)
        head = scatter(final, cot_out)
        cols = out_width // n_sec
        loss_group = sum(mp_pieces(loss.reshape(1, 1)))
        if n_dp > 1:
            loss_group = loss_group + dp_swap(loss_group)
        head_mine = jnp.where(sec == last, head[:, last * cols :], 0.0)
        loss_mine = jnp.where(sec == last, loss_group, 0.0)
        for j in range(last):
            head_mine = head_mine + hop(head[:, j * cols : (j + 1) * cols].astype(BF16), last, j).astype(F32)
            loss_mine = loss_mine + hop(loss_group, last, j)
        return grad[None], head_mine, loss_mine.reshape(()) / (n_dp * MB * out_width)

    room = n_mp * slots_here
    if room >= n_mp * samp_dev * rank:
        return fast
    return lax.while_loop(
        lambda state: state[0] > room, lambda state: (jnp.int32(0), *plain()), (most_active, *fast)
    )[1:]


def solution(mesh):
    in_specs = (
        P(("dp", "mp"), None),
        P(("dp", "mp"), None, None),
        P(("dp", "mp"), None),
        P(("dp", "mp"), None, None),
        P(("dp", "mp"), None),
        P(("dp", "mp"), None),
        P(),
        P("section", "mp", None),
        P(),
    )
    out_specs = (P("section", ("dp", "mp"), None), P(("dp", "mp"), "section"), P())
    return jax.shard_map(local, mesh=mesh, in_specs=in_specs, out_specs=out_specs, check_vma=False)
```

```python
import jax
import jax.numpy as jnp
from jax import lax
from jax.experimental import pallas as pl
from jax.experimental.pallas import tpu as pltpu
from jax.sharding import PartitionSpec as P


F32 = jnp.float32
BF16 = jnp.bfloat16
MB = 6
EXTRA = 16
BLOCKS = 4

ANY = pl.BlockSpec(memory_space=pl.ANY)
SMEM = pl.BlockSpec(memory_space=pltpu.SMEM)
VMEM = pl.BlockSpec(memory_space=pltpu.VMEM)


def round_up(value, unit):
    return -(-value // unit) * unit


def mp_swap(value, flip):
    count = lax.axis_size("mp")
    return lax.ppermute(value, "mp", [(m, m ^ flip) for m in range(count)])


def dp_swap(value):
    count = lax.axis_size("dp")
    return lax.ppermute(value, "dp", [(d, d ^ 1) for d in range(count)])


def mp_pieces(value):
    return [value] + [mp_swap(value, k) for k in range(1, lax.axis_size("mp"))]


def hop(value, source, target):
    return lax.ppermute(value, "section", [(source, target)])


def plane_pieces(value, section):
    count = lax.axis_size("mp")
    base = section * count
    swaps = [[(base + m, base + (m ^ k)) for m in range(count)] for k in range(1, count)]
    return [value] + [lax.ppermute(value, ("section", "mp"), pairs) for pairs in swaps]


def params():
    return pltpu.CompilerParams(vmem_limit_bytes=24 * 2**20)


def call(body, args, specs, deps=(), **options):
    reads, waits = len(args), len(deps)

    def inner(*refs):
        body(*refs[:reads], *refs[reads + waits :])

    return pl.pallas_call(
        inner, in_specs=list(specs) + [ANY] * waits, compiler_params=params(), **options
    )(*args, *deps)


def run_copies(copies):
    for copy in copies:
        copy.start()
    for copy in copies:
        copy.wait()


def spread(onehot, value):
    high = value.astype(BF16)
    low = (value - high.astype(F32)).astype(BF16)
    return jnp.dot(onehot, high, preferred_element_type=F32) + jnp.dot(
        onehot, low, preferred_element_type=F32
    )


class Weights:
    def __init__(self, layer):
        self.count = lax.axis_size("mp")
        self.block_rows, self.width = layer.shape
        dp_index = lax.axis_index("dp")
        half = self.block_rows // 2
        self.offsets = [dp_index * half, (1 - dp_index) * half]
        self.pieces = [(layer, 0, None, 0)]
        self.colored = self.count == 4 and lax.axis_size("dp") == 2
        self.part = part = half // 2
        if self.colored:
            self.first = lax.dynamic_slice_in_dim(layer, dp_index * half, part, 0)
            self.second = lax.dynamic_slice_in_dim(layer, dp_index * half + part, part, 0)
            self.b1 = self.swap(self.second, 1)
            self.a2 = self.swap(self.first, 2)
            self.a1 = self.swap(self.first, 1)
            self.b2 = self.swap(self.second, 2)
            self.a3 = self.swap(self.a1, 2)
            self.b3 = self.swap(self.b2, 1)
            got = [(self.a1, 1, 0), (self.b2, 2, part), (self.b1, 1, part), (self.a2, 2, 0), (self.a3, 3, 0), (self.b3, 3, part)]
            for array, block, base in got:
                self.pieces.append((array, block, 0, base))
                self.pieces.append((dp_swap(array), block, 1, base))
        else:
            for block in range(1, self.count):
                self.pieces.append((mp_swap(layer, block), block, None, 0))

    def swap(self, array, flip):
        return mp_swap(array, flip)

    def assemble(self, ids):
        many = len(self.pieces)

        def body(ids_ref, *refs):
            out, sems = refs[many:]
            copies = []
            for i, (array, block, which, base) in enumerate(self.pieces):
                row = pl.multiple_of(ids_ref[3 + block] * self.block_rows, self.block_rows) + base
                if which is not None:
                    row = row + pl.multiple_of(ids_ref[1 + which], self.block_rows // 2)
                copies.append(
                    pltpu.make_async_copy(refs[i], out.at[pl.ds(row, array.shape[0]), :], sems.at[i])
                )
            run_copies(copies)

        return pl.pallas_call(
            body,
            out_shape=jax.ShapeDtypeStruct((self.count * self.block_rows, self.width), BF16),
            in_specs=[SMEM] + [ANY] * many,
            out_specs=VMEM,
            scratch_shapes=[pltpu.SemaphoreType.DMA((many,))],
            compiler_params=params(),
            name="assemble",
        )(ids, *[piece[0] for piece in self.pieces])


def fwd_stage(deps, level, ids, layer, rows, onehot, slope, kept):
    height, width = rows.shape
    prims = onehot.shape[1]
    leads = slope is None
    nb = width // BLOCKS

    def body(ids_ref, layer_ref, rows_ref, onehot_ref, *rest):
        if not leads:
            slope_ref, *rest = rest
        next_ref, pre_ref, kept_ref, *rest = rest[(kept is not None) :]
        if leads:
            tanh_ref, *rest = rest
        (kept_sem,) = rest

        @pl.when(ids_ref[0] == level)
        def _():
            keep = pltpu.make_async_copy(rows_ref, kept_ref, kept_sem)
            keep.start()

            def block(n, carry):
                cols = pl.ds(pl.multiple_of(n * nb, nb), nb)
                acc = jnp.dot(rows_ref[...], layer_ref[:, cols], preferred_element_type=F32)
                old = rows_ref[:, cols].astype(F32)
                pre_ref[:, cols] = acc.astype(BF16)
                if leads:
                    tanh_p = jnp.tanh(acc[:prims])
                    tanh_ref[:, cols] = tanh_p
                    factor = spread(onehot_ref[...], 1.0 - tanh_p * tanh_p)
                    new = jnp.concatenate(
                        [old[:prims] + tanh_p, old[prims:] + factor * acc[prims:]], axis=0
                    )
                else:
                    tanh_p = slope_ref[:, cols]
                    new = old + spread(onehot_ref[...], 1.0 - tanh_p * tanh_p) * acc
                next_ref[:, cols] = new.astype(BF16)
                return carry

            lax.fori_loop(0, BLOCKS, block, 0)
            keep.wait()

    outs = [jax.ShapeDtypeStruct((height, width), BF16)] * 3
    if leads:
        outs.append(jax.ShapeDtypeStruct((prims, width), F32))
    args = [ids, layer, rows, onehot] + ([] if leads else [slope])
    specs = [SMEM] + [VMEM] * (len(args) - 1)
    alias = {}
    if kept is not None:
        alias = {len(args): 2}
        args.append(kept)
        specs.append(ANY)
    return call(
        body,
        args,
        specs,
        deps,
        out_shape=outs,
        out_specs=[VMEM, VMEM, ANY] + [VMEM] * (len(outs) - 3),
        input_output_aliases=alias,
        scratch_shapes=[pltpu.SemaphoreType.DMA],
        cost_estimate=pl.CostEstimate(flops=2 * height * width * width * 4, bytes_accessed=2 * width * width, transcendentals=0),
        name=f"fwd{level}",
    )


def bwd_stage(deps, level, ids, layer, cot, pre, tanh_p, onehot, onehot_t, total, leads, kept):
    height, width = cot.shape
    prims = tanh_p.shape[0]
    deep = level > 0
    nb = width // BLOCKS

    def body(ids_ref, cot_ref, pre_ref, tanh_ref, onehot_ref, onehot_t_ref, *rest):
        if total is not None:
            total_ref, *rest = rest
        if deep:
            layer_ref, *rest = rest
        kept_ref, side_ref, *rest = rest[(kept is not None) :]
        if deep:
            new_ref, *rest = rest
        mix_ref, kept_sem = rest

        @pl.when(ids_ref[0] == level)
        def _():
            skip = prims if leads else 0

            def block(n, carry):
                cols = pl.ds(pl.multiple_of(n * nb, nb), nb)
                up = cot_ref[:, cols].astype(F32)
                tanh = tanh_ref[:, cols]
                slope = 1.0 - tanh * tanh
                up_t = up[skip:]
                mix_t = up_t * spread(onehot_ref[...], slope)
                total_here = spread(onehot_t_ref[...], up_t * pre_ref[:, cols].astype(F32)[skip:])
                if total is not None:
                    total_here = total_here + total_ref[:, cols]
                if leads:
                    mix_p = up[:prims] * slope - 2.0 * total_here * tanh * slope
                    mix_ref[:, cols] = jnp.concatenate([mix_p, mix_t], axis=0).astype(BF16)
                else:
                    mix_ref[:, cols] = mix_t.astype(BF16)
                side_ref[:, cols] = total_here
                return carry

            lax.fori_loop(0, BLOCKS, block, 0)
            keep = pltpu.make_async_copy(mix_ref, kept_ref, kept_sem)
            keep.start()
            if deep:

                def back_block(n, carry):
                    cols = pl.ds(pl.multiple_of(n * nb, nb), nb)
                    back = lax.dot_general(
                        mix_ref[...], layer_ref[cols, :], (((1,), (1,)), ((), ())), preferred_element_type=F32
                    )
                    new_ref[:, cols] = (cot_ref[:, cols].astype(F32) + back).astype(BF16)
                    return carry

                lax.fori_loop(0, BLOCKS, back_block, 0)
            keep.wait()

    rows_shape = jax.ShapeDtypeStruct((height, width), BF16)
    outs = [rows_shape, jax.ShapeDtypeStruct((prims, width), F32)] + ([rows_shape] if deep else [])
    args = [ids, cot, pre, tanh_p, onehot, onehot_t] + ([] if total is None else [total])
    args += [layer] if deep else []
    specs = [SMEM] + [VMEM] * (len(args) - 1)
    alias = {}
    if kept is not None:
        alias = {len(args): 0}
        args.append(kept)
        specs.append(ANY)
    return call(
        body,
        args,
        specs,
        deps,
        out_shape=outs,
        out_specs=[ANY] + [VMEM] * (len(outs) - 1),
        input_output_aliases=alias,
        scratch_shapes=[pltpu.VMEM((height, width), BF16), pltpu.SemaphoreType.DMA],
        cost_estimate=pl.CostEstimate(flops=2 * height * width * width * 4, bytes_accessed=2 * width * width, transcendentals=0),
        name=f"bwd{level}",
    )


def pick_rows(deps, ids, index, pieces, level):
    height = index.shape[0]
    piece_rows, width = pieces[0].shape

    def body(ids_ref, index_ref, *rest):
        out_ref = rest[-1]

        @pl.when(ids_ref[0] == level)
        def _():
            index_here = index_ref[...]
            acc = jnp.zeros((height, width), F32)
            for k, piece_ref in enumerate(rest[:-1]):
                place = lax.broadcasted_iota(jnp.int32, (height, piece_rows), 1) + k * piece_rows
                onehot = jnp.where(place == index_here, 1.0, 0.0).astype(BF16)
                acc = acc + jnp.dot(onehot, piece_ref[...], preferred_element_type=F32)
            out_ref[...] = acc.astype(BF16)

    return call(
        body,
        [ids, index, *pieces],
        [SMEM] + [VMEM] * (1 + len(pieces)),
        deps,
        out_shape=jax.ShapeDtypeStruct((height, width), BF16),
        out_specs=VMEM,
        name="pick",
    )


def lift_rows(ids, rows, encoder, chunks):
    height = rows.shape[0] // chunks
    width = encoder.shape[1]

    def body(ids_ref, rows_ref, encoder_ref, *outs):
        @pl.when(ids_ref[0] == 0)
        def _():
            for c, out in enumerate(outs):
                part = rows_ref[c * height : (c + 1) * height, :]
                out[...] = jnp.dot(part, encoder_ref[...], preferred_element_type=F32).astype(BF16)

    return pl.pallas_call(
        body,
        out_shape=[jax.ShapeDtypeStruct((height, width), BF16)] * chunks,
        in_specs=[SMEM, VMEM, VMEM],
        out_specs=[VMEM] * chunks,
        compiler_params=params(),
        name="lift",
    )(ids, rows, encoder)


def pack_columns(deps, ids, chunks, tails, level, n_dp, n_mp, blk):
    count = len(chunks)
    height, _ = chunks[0].shape
    tail_rows, tail_width = tails[0].shape if tails else (height, 0)
    core = n_dp * blk

    def body(ids_ref, *refs):
        chunk_refs, rest = refs[:count], refs[count:]
        tail_refs, outs = rest[: len(tails)], rest[len(tails) :]

        def fill():
            for k, out in enumerate(outs):
                for c, chunk_ref in enumerate(chunk_refs):
                    first = c * tail_rows
                    for d in range(n_dp):
                        col = pl.multiple_of((ids_ref[3 + k] + d * n_mp) * blk, blk)
                        out[first : first + height, d * blk : (d + 1) * blk] = chunk_ref[:, pl.ds(col, blk)]
                    if tails:
                        out[first + height : first + tail_rows, :core] = jnp.zeros((EXTRA, core), BF16)
                        out[first : first + tail_rows, core:] = tail_refs[c][...]

        if level is None:
            fill()
        else:
            pl.when(ids_ref[0] == level)(fill)

    shape = jax.ShapeDtypeStruct((count * tail_rows, core + tail_width), BF16)
    return call(
        body,
        [ids, *chunks, *tails],
        [SMEM] + [VMEM] * (count + len(tails)),
        deps,
        out_shape=[shape] * n_mp,
        out_specs=[VMEM] * n_mp,
        name="pack",
    )


def both_groups(pieces):
    return pieces + ([dp_swap(piece) for piece in pieces] if lax.axis_size("dp") > 1 else [])


def loss_rows(loss, cols):
    high = loss.astype(BF16).astype(F32)
    line = lax.broadcasted_iota(jnp.int32, (EXTRA, cols), 0)
    return jnp.where(line == 0, high, jnp.where(line == 1, loss - high, 0.0))


def head_partial(deps, ids, pieces, level, blk, height):
    rows_each, wide = pieces[0].shape
    core = 2 * blk
    out_width = wide - core
    many = len(pieces)

    def body(ids_ref, *refs):
        piece_refs, (mine_ref, send_ref, left, right, sems) = refs[:many], refs[many:]

        @pl.when(ids_ref[0] == level)
        def _():
            here = pl.multiple_of(ids_ref[1] // ids_ref[7] * blk, blk)
            there = pl.multiple_of(blk - here, blk)
            copies = []
            for i, ref in enumerate(piece_refs):
                rows = pl.ds(i * rows_each, rows_each)
                copies.append(pltpu.make_async_copy(ref.at[:, pl.ds(here, blk)], left.at[rows, :blk], sems.at[0, i]))
                copies.append(pltpu.make_async_copy(ref.at[:, pl.ds(there, blk)], left.at[rows, blk:], sems.at[1, i]))
                copies.append(pltpu.make_async_copy(ref.at[:, core:], right.at[rows], sems.at[2, i]))
            run_copies(copies)
            loss = jnp.zeros((1, 128), F32)
            for first in range(height, many * rows_each, height + EXTRA):
                loss = loss + right[first : first + 1, :128].astype(F32) + right[first + 1 : first + 2, :128].astype(F32)
            tail = loss_rows(loss[:, :1], out_width)
            part = lax.dot_general(left[...], right[...], (((0,), (0,)), ((), ())), preferred_element_type=F32)
            mine_ref[:blk, :] = part[:blk]
            mine_ref[blk:, :] = tail
            send_ref[:blk, :] = part[blk:].astype(BF16)
            send_ref[blk:, :] = tail.astype(BF16)

    shape = (blk + EXTRA, out_width)
    return call(
        body,
        [ids, *pieces],
        [SMEM] + [ANY] * many,
        deps,
        out_shape=[jax.ShapeDtypeStruct(shape, F32), jax.ShapeDtypeStruct(shape, BF16)],
        out_specs=[VMEM] * 2,
        scratch_shapes=[
            pltpu.VMEM((many * rows_each, core), BF16),
            pltpu.VMEM((many * rows_each, out_width), BF16),
            pltpu.SemaphoreType.DMA((3, many)),
        ],
        name="head_partial",
    )


def head_gradient(deps, ids, mine, other, level, blk, n_sec):
    cols = mine.shape[1] // n_sec

    def body(ids_ref, mine_ref, other_ref, *outs):
        @pl.when(ids_ref[0] == level)
        def _():
            tails = mine_ref[blk:, :1] + other_ref[blk:, :128].astype(F32)[:, :1]
            tail = loss_rows(tails[0:1] + tails[1:2], cols).astype(BF16)
            for j, out in enumerate(outs):
                span = slice(j * cols, (j + 1) * cols)
                out[:blk, :] = (mine_ref[:blk, span] + other_ref[:blk, span].astype(F32)).astype(BF16)
                out[blk:, :] = tail

    return call(
        body,
        [ids, mine, other],
        [SMEM, VMEM, VMEM],
        deps,
        out_shape=[jax.ShapeDtypeStruct((blk + EXTRA, cols), BF16)] * n_sec,
        out_specs=[VMEM] * n_sec,
        name="grad_head",
    )


def layer_gradient(deps, ids, blocks, chunk, mixes, blk, height, before):
    many = len(mixes)
    width = mixes[0].shape[1]
    nb = width // BLOCKS

    def body(ids_ref, *refs):
        block_refs, mix_refs = refs[:many], refs[many : 2 * many]
        rest = refs[2 * many :]
        if before is not None:
            before_ref, *rest = rest
        out, left, right, turned, sems = rest
        mine = pl.multiple_of(ids_ref[1] // ids_ref[7] * blk, blk)
        top = chunk * height
        copies = []
        for i in range(many):
            rows = pl.ds(i * height, height)
            src = block_refs[i].at[top : top + height, pl.ds(mine, blk)]
            copies.append(pltpu.make_async_copy(src, left.at[rows], sems.at[0, i]))
            copies.append(pltpu.make_async_copy(mix_refs[i], right.at[rows], sems.at[1, i]))
        run_copies(copies)
        turned[...] = left[...].astype(F32).T.astype(BF16)

        def block(n, carry):
            cols = pl.ds(pl.multiple_of(n * nb, nb), nb)
            part = jnp.dot(turned[...], right[:, cols], preferred_element_type=F32)
            if before is not None:
                part = part + before_ref[:, cols]
            out[:, cols] = part
            return carry

        lax.fori_loop(0, BLOCKS, block, 0)

    return call(
        body,
        [ids, *blocks, *mixes, *([] if before is None else [before])],
        [SMEM] + [ANY] * (2 * many) + ([] if before is None else [VMEM]),
        deps,
        out_shape=jax.ShapeDtypeStruct((blk, width), F32),
        out_specs=VMEM,
        scratch_shapes=[
            pltpu.VMEM((many * height, blk), BF16),
            pltpu.VMEM((many * height, width), BF16),
            pltpu.VMEM((blk, many * height), BF16),
            pltpu.SemaphoreType.DMA((2, many)),
        ],
        name="grad_layer",
    )


def join_rows(deps, flat, deep, rows_out):
    count, rank, width = deep.shape

    def body(flat_ref, deep_ref, out, sem):
        copies = [
            pltpu.make_async_copy(deep_ref.at[i], out.at[i * rank : (i + 1) * rank], sem.at[i])
            for i in range(count)
        ]
        for copy in copies:
            copy.start()
        spare = jnp.zeros((rows_out - count * (rank + 1), width), F32)
        out[count * rank :, :] = jnp.concatenate([flat_ref[...].astype(F32), spare], axis=0).astype(BF16)
        for copy in copies:
            copy.wait()

    return call(
        body,
        [flat, deep],
        [VMEM, ANY],
        deps,
        out_shape=jax.ShapeDtypeStruct((rows_out, width), BF16),
        out_specs=VMEM,
        scratch_shapes=[pltpu.SemaphoreType.DMA((count,))],
        name="join",
    )


def head_stage(deps, level, ids, rows, wanted, share, head_weight):
    height, width = rows.shape
    out_width = head_weight.shape[1]

    def body(ids_ref, rows_ref, wanted_ref, share_ref, head_ref, cot_ref, new_ref):
        @pl.when(ids_ref[0] == level)
        def _():
            nb = out_width // BLOCKS

            def block(n, loss):
                cols = pl.ds(pl.multiple_of(n * nb, nb), nb)
                outputs = jnp.dot(rows_ref[...], head_ref[:, cols], preferred_element_type=F32)
                mismatch = outputs - wanted_ref[:, cols].astype(F32)
                scaled = share_ref[...] * mismatch
                cot_ref[:height, cols] = (2.0 * scaled).astype(BF16)
                return loss + jnp.sum(scaled * mismatch, axis=1, keepdims=True)

            loss = lax.fori_loop(0, BLOCKS, block, jnp.zeros((height, 1), F32))
            loss = jnp.sum(loss, axis=0, keepdims=True)
            line = lax.broadcasted_iota(jnp.int32, (EXTRA, out_width), 0)
            high = loss.astype(BF16).astype(F32)
            tail = jnp.where(line == 0, high, jnp.where(line == 1, loss - high, 0.0))
            cot_ref[height:, :] = tail.astype(BF16)
            kb = width // BLOCKS

            def back_block(k, carry):
                cols = pl.ds(pl.multiple_of(k * kb, kb), kb)
                new_ref[:, cols] = lax.dot_general(
                    cot_ref[:height, :], head_ref[cols, :], (((1,), (1,)), ((), ())), preferred_element_type=F32
                ).astype(BF16)
                return carry

            lax.fori_loop(0, BLOCKS, back_block, 0)

    return call(
        body,
        [ids, rows, wanted, share, head_weight],
        [SMEM] + [VMEM] * 4,
        deps,
        out_shape=[
            jax.ShapeDtypeStruct((height + EXTRA, out_width), BF16),
            jax.ShapeDtypeStruct((height, width), BF16),
        ],
        out_specs=[VMEM] * 2,
        cost_estimate=pl.CostEstimate(flops=2 * height * width * width * 4, bytes_accessed=2 * width * out_width, transcendentals=0),
        name="head",
    )


def local(
    inputs, tangents, targets, target_jac, rank_mask, batch_order, encoder, layers, head_weight
):
    samp_dev, rank = rank_mask.shape
    in_width = inputs.shape[1]
    width = layers.shape[2]
    out_width = head_weight.shape[1]
    n_dp = lax.axis_size("dp")
    n_mp = lax.axis_size("mp")
    n_sec = lax.axis_size("section")
    last = n_sec - 1
    dp_index = lax.axis_index("dp")
    sec = lax.axis_index("section")
    mp_index = lax.axis_index("mp")
    prims = n_mp * samp_dev
    blk = width // (n_dp * n_mp)

    weights = Weights(layers[0])
    helper = 1 if n_sec > 1 else 0

    piece_rows = round_up(samp_dev * (rank + 1), 16)
    joined_rows = join_rows([], inputs, tangents, piece_rows)
    row_pieces = plane_pieces(joined_rows, helper)

    own_rank = jnp.sum(rank_mask, axis=1)
    slot_line = jnp.arange(samp_dev, dtype=jnp.int32)
    own_slot = jnp.sum(
        jnp.where(batch_order[0][None, :] == slot_line[:, None], slot_line[None, :], 0), axis=1
    ) // (samp_dev // MB)
    own_meta = jnp.stack([own_rank, own_slot]).astype(jnp.int32)
    meta_pieces = jnp.stack(mp_pieces(own_meta))
    order_line = jnp.arange(n_mp, dtype=jnp.int32)
    swap = ((order_line[:, None] ^ mp_index) == order_line[None, :]).astype(jnp.int32)
    meta = jnp.sum(swap[:, :, None, None] * meta_pieces[None], axis=1)
    ranks = meta[:, 0].reshape(prims)
    slots = meta[:, 1].reshape(prims)
    sample_line = jnp.arange(prims, dtype=jnp.int32)
    ends = jnp.sum(jnp.where(sample_line[None, :] <= sample_line[:, None], ranks[None, :], 0), axis=1)
    active = jnp.sum(ranks)
    counts = jnp.sum(jnp.where(slots[None, :] == slots[:, None], ranks[None, :] + 1, 0), axis=1)
    inverse = 1.0 / counts.astype(F32)

    kb = width // n_mp
    ids = jnp.stack(
        [sec] + weights.offsets + [mp_index ^ k for k in range(n_mp)] + [jnp.int32(kb // 2)] * (n_mp == 4)
    ).astype(jnp.int32)
    chunks = 2
    usual = samp_dev * (rank // 2 + 1)
    height = max(round_up(-(-(prims + usual) // chunks), 16), round_up(prims + 8, 16))
    slots_here = chunks * height - prims

    place = mp_index * slots_here + jnp.arange(slots_here, dtype=jnp.int32)
    passed = ends[None, :] <= place[:, None]
    sample = jnp.sum(passed.astype(jnp.int32), axis=1)
    column = place - jnp.sum(jnp.where(passed, ranks[None, :], 0), axis=1)
    present = place < active
    belongs = (sample[:, None] == sample_line[None, :]) & present[:, None]
    source = ((sample // samp_dev) ^ mp_index) * piece_rows + (sample % samp_dev) * rank + column
    source = jnp.where(present, source, -1)
    source_p = ((sample_line // samp_dev) ^ mp_index) * piece_rows + samp_dev * rank + sample_line % samp_dev
    share = jnp.sum(jnp.where(belongs, inverse[None, :], 0.0), axis=1)
    share_p = jnp.where(sample_line // samp_dev == mp_index, inverse, 0.0)
    index = jnp.concatenate([source_p, source])[:, None]
    shares = jnp.concatenate([share_p, share])[:, None]
    onehot = belongs.astype(BF16)
    first = height - prims
    onehots = [onehot[:first], onehot[first:]]
    onehots_t = [part.T for part in onehots]
    share_of = [shares[:height], shares[height:]]

    packed = pick_rows([], ids, index, row_pieces, helper)
    if helper != 0:
        packed = hop(packed, helper, 0)
    rows = list(lift_rows(ids, packed, encoder, chunks))
    layer = weights.assemble(ids)
    other_active = dp_swap(active.reshape(1, 1)).reshape(()) if n_dp > 1 else active
    most_active = jnp.maximum(active, other_active)

    token = []
    entered = [None] * chunks
    pres = [[None] * n_sec for _ in range(chunks)]
    tanhs = [None] * n_sec
    heads = [None] * chunks
    goal_pieces = None
    for level in range(n_sec):
        for c in range(chunks):
            got = fwd_stage(
                token, level, ids, layer, rows[c], onehots[c], None if c == 0 else tanhs[level], entered[c]
            )
            token = [got[0]]
            entered[c], pres[c][level] = got[2], got[1]
            if c == 0:
                tanhs[level] = got[3]
            rows[c] = got[0] if level == last else hop(got[0], level, level + 1)
            if level == last:
                heads[c] = head_stage(
                    token, last, ids, rows[c], wanted[c * height : (c + 1) * height], share_of[c], head_weight
                )
                token = [heads[c][1]]
        if goal_pieces is None:
            goal_pieces = plane_pieces(join_rows(token, targets, target_jac, piece_rows), last)
        if level == max(last - 1, 0):
            wanted = pick_rows([*token, most_active.reshape(1)], ids, index, goal_pieces, last)
            token = [wanted]

    small = n_dp * n_mp <= 8 and blk % 128 == 0
    cots = [heads[c][1] for c in range(chunks)]
    mixes = [None] * chunks
    backward_order = list(range(1, chunks)) + [0]
    hidden_pieces = head_pieces = None
    arrived = []
    for level in range(last, -1, -1):
        total = None
        for c in backward_order:
            got = bwd_stage(
                token, level, ids, layer, cots[c], pres[c][level], tanhs[level],
                onehots[c], onehots_t[c], total, c == 0, mixes[c],
            )
            mixes[c], total = got[0], got[1]
            token = [got[1]]
            if level > 0:
                cots[c] = hop(got[2], level, level - 1)
        if not small:
            continue
        if level == last:
            sends = pack_columns(token, ids, rows, [h[0] for h in heads], last, n_dp, n_mp, blk)
            token = [sends[0]]
            base = last * n_mp
            head_pieces = [sends[0]] + [
                lax.ppermute(sends[k], ("section", "mp"), [(base + m, base + (m ^ k)) for m in range(n_mp)])
                for k in range(1, n_mp)
            ]
        elif level == last - 1:
            sends = pack_columns(token, ids, entered, [], None, n_dp, n_mp, blk)
            token = [sends[0]]
            hidden_pieces = [sends[0]] + [mp_swap(sends[k], k) for k in range(1, n_mp)]
            mine, send = head_partial(token, ids, head_pieces, last, blk, height)
            token = [send]
            other = dp_swap(send)
        elif level == last - 2:
            blocks = head_gradient(token, ids, mine, other, last, blk, n_sec)
            token = [blocks[0]]
            arrived = [hop(blocks[j], last, j) for j in range(last)]
            hidden_pieces = both_groups(hidden_pieces)
            token = [blocks[0], *hidden_pieces]

    cols = out_width // n_sec
    if small:
        head_ext = blocks[last].astype(F32)
        for j in range(last):
            head_ext = jnp.where(sec == j, arrived[j].astype(F32), head_ext)
        head_mine = head_ext[:blk]
        loss_mine = (head_ext[blk, 0] + head_ext[blk + 1, 0]) / (n_dp * MB * out_width)
        grad = None
        for c in backward_order:
            swapped = [mixes[c]] + [mp_swap(mixes[c], k) for k in range(1, n_mp)]
            mix_pieces = both_groups(swapped)
            grad = layer_gradient(token, ids, hidden_pieces, c, mix_pieces, blk, height, grad)
            token = [grad]
    else:
        contract = (((0,), (0,)), ((), ()))
        joined = jnp.concatenate(entered, axis=0)
        part = lax.dot_general(joined, jnp.concatenate(mixes, axis=0), contract, preferred_element_type=F32)
        grad = lax.psum_scatter(part.astype(BF16), ("dp", "mp"), scatter_dimension=0, tiled=True).astype(F32)
        cot_out = jnp.concatenate([h[0][:height] for h in heads], axis=0)
        part = lax.dot_general(jnp.concatenate(rows, axis=0), cot_out, contract, preferred_element_type=F32)
        head = lax.psum_scatter(part.astype(BF16), ("dp", "mp"), scatter_dimension=0, tiled=True)
        loss = sum(jnp.sum(h[0][height : height + 2, 0].astype(F32)) for h in heads)
        loss = jnp.where(sec == last, lax.psum(loss, ("dp", "mp")), 0.0).reshape(1, 1)
        head_mine = jnp.where(sec == last, head[:, last * cols :], jnp.zeros((blk, cols), BF16))
        loss_mine = loss
        for j in range(last):
            head_mine = head_mine + hop(head[:, j * cols : (j + 1) * cols], last, j)
            loss_mine = loss_mine + hop(loss, last, j)
        head_mine = head_mine.astype(F32)
        loss_mine = loss_mine.reshape(()) / (n_dp * MB * out_width)
    fast = (grad[None], head_mine, loss_mine)

    def plain():
        depth = rank + 1
        total_rows = samp_dev * depth
        layer_full = jnp.zeros((width, width), BF16)
        kb = weights.block_rows
        for array, block, which, base in weights.pieces:
            row = (mp_index ^ block) * kb + base
            row = row if which is None else row + weights.offsets[which]
            layer_full = lax.dynamic_update_slice_in_dim(layer_full, array, row, 0)
        rows_in = jnp.concatenate([inputs[:, None, :], tangents], axis=1).reshape(total_rows, in_width)
        start = jnp.dot(rows_in, encoder, preferred_element_type=F32).astype(BF16)
        chain = [(j, (j + 1) % n_sec) for j in range(n_sec)]

        def back_one(value):
            return lax.fori_loop(0, last, lambda _, v: lax.ppermute(v, "section", chain), value)

        def pre_of(rows):
            pre = jnp.dot(rows, layer_full, preferred_element_type=F32).reshape(samp_dev, depth, width)
            tanh_p = jnp.tanh(pre[:, 0])
            return pre, tanh_p, 1.0 - tanh_p * tanh_p

        def forward(level, state):
            rows, mine, _ = state
            mine = jnp.where(level == sec, rows, mine)
            pre, tanh_p, slope = pre_of(rows)
            change = jnp.concatenate([tanh_p[:, None], slope[:, None] * pre[:, 1:]], axis=1)
            new = (rows.astype(F32) + change.reshape(total_rows, width)).astype(BF16)
            return lax.ppermute(new, "section", chain), mine, new

        _, mine, final = lax.fori_loop(0, n_sec, forward, (start, start, start))
        own = lax.dynamic_slice_in_dim(inverse, mp_index * samp_dev, samp_dev, 0)
        row_weight = jnp.concatenate([jnp.ones((samp_dev, 1), F32), rank_mask.astype(F32)], axis=1)
        share = (row_weight * own[:, None]).reshape(total_rows, 1)
        outputs = jnp.dot(final, head_weight, preferred_element_type=F32)
        wanted = jnp.concatenate([targets[:, None, :], target_jac], axis=1).reshape(total_rows, out_width)
        mismatch = outputs - wanted.astype(F32)
        loss = jnp.sum(share * mismatch * mismatch)
        cot_out = (2.0 * share * mismatch).astype(BF16)
        cot = lax.dot_general(cot_out, head_weight, (((1,), (1,)), ((), ())), preferred_element_type=F32)
        pre, tanh_p, slope = pre_of(mine)

        def backward(step, state):
            cot, mix_mine = state
            up = cot.astype(F32).reshape(samp_dev, depth, width)
            side = jnp.sum(up[:, 1:] * pre[:, 1:], axis=1)
            lead = up[:, 0] * slope - 2.0 * side * tanh_p * slope
            mix = jnp.concatenate([lead[:, None], up[:, 1:] * slope[:, None]], axis=1)
            mix = mix.astype(BF16).reshape(total_rows, width)
            mix_mine = jnp.where(step == last - sec, mix, mix_mine)
            back = lax.dot_general(mix, layer_full, (((1,), (1,)), ((), ())), preferred_element_type=F32)
            new = (up.reshape(total_rows, width) + back).astype(BF16)
            return back_one(new), mix_mine

        _, mix = lax.fori_loop(0, n_sec, backward, (cot.astype(BF16), mine))

        def scatter(left, right):
            part = lax.dot_general(left, right, (((0,), (0,)), ((), ())), preferred_element_type=F32)
            part = part.astype(BF16).reshape(n_dp, n_mp, blk, right.shape[1])
            mine_part = jnp.zeros((n_dp, blk, right.shape[1]), F32)
            for k in range(n_mp):
                piece = lax.dynamic_index_in_dim(part, mp_index ^ k, 1, False)
                mine_part = mine_part + (piece if k == 0 else mp_swap(piece, k)).astype(F32)
            kept = lax.dynamic_index_in_dim(mine_part, dp_index, 0, False)
            if n_dp > 1:
                sent = lax.dynamic_index_in_dim(mine_part, 1 - dp_index, 0, False)
                kept = kept + dp_swap(sent.astype(BF16)).astype(F32)
            return kept

        grad = scatter(mine, mix)
        head = scatter(final, cot_out)
        cols = out_width // n_sec
        loss_group = sum(mp_pieces(loss.reshape(1, 1)))
        if n_dp > 1:
            loss_group = loss_group + dp_swap(loss_group)
        head_mine = jnp.where(sec == last, head[:, last * cols :], 0.0)
        loss_mine = jnp.where(sec == last, loss_group, 0.0)
        for j in range(last):
            block = jnp.concatenate([head[:, j * cols : (j + 1) * cols], jnp.broadcast_to(loss_group, (8, cols))])
            block = hop(block, last, j)
            head_mine = head_mine + block[:blk]
            loss_mine = loss_mine + block[blk:, :1][:1]
        return grad[None], head_mine, loss_mine.reshape(()) / (n_dp * MB * out_width)

    room = n_mp * slots_here
    if room >= n_mp * samp_dev * rank:
        return fast
    return lax.while_loop(
        lambda state: state[0] > room, lambda state: (jnp.int32(0), *plain()), (most_active, *fast)
    )[1:]


def solution(mesh):
    in_specs = (
        P(("dp", "mp"), None),
        P(("dp", "mp"), None, None),
        P(("dp", "mp"), None),
        P(("dp", "mp"), None, None),
        P(("dp", "mp"), None),
        P(("dp", "mp"), None),
        P(),
        P("section", "mp", None),
        P(),
    )
    out_specs = (P("section", ("dp", "mp"), None), P(("dp", "mp"), "section"), P())

    return jax.shard_map(local, mesh=mesh, in_specs=in_specs, out_specs=out_specs, check_vma=False)
```

```python
import jax
import jax.numpy as jnp
from jax import lax
from jax.experimental import pallas as pl
from jax.experimental.pallas import tpu as pltpu
from jax.sharding import PartitionSpec as P


F32 = jnp.float32
BF16 = jnp.bfloat16
MB = 6
EXTRA = 16
BLOCKS = 4

ANY = pl.BlockSpec(memory_space=pl.ANY)
SMEM = pl.BlockSpec(memory_space=pltpu.SMEM)
VMEM = pl.BlockSpec(memory_space=pltpu.VMEM)


def round_up(value, unit):
    return -(-value // unit) * unit


def mp_swap(value, flip):
    count = lax.axis_size("mp")
    return lax.ppermute(value, "mp", [(m, m ^ flip) for m in range(count)])


def dp_swap(value):
    count = lax.axis_size("dp")
    return lax.ppermute(value, "dp", [(d, d ^ 1) for d in range(count)])


def mp_pieces(value):
    return [value] + [mp_swap(value, k) for k in range(1, lax.axis_size("mp"))]


def hop(value, source, target):
    return lax.ppermute(value, "section", [(source, target)])


def plane_pieces(value, section):
    count = lax.axis_size("mp")
    base = section * count
    swaps = [[(base + m, base + (m ^ k)) for m in range(count)] for k in range(1, count)]
    return [value] + [lax.ppermute(value, ("section", "mp"), pairs) for pairs in swaps]


def params():
    return pltpu.CompilerParams(vmem_limit_bytes=16 * 2**20)


def call(body, args, specs, deps=(), **options):
    reads, waits = len(args), len(deps)

    def inner(*refs):
        body(*refs[:reads], *refs[reads + waits :])

    return pl.pallas_call(
        inner, in_specs=list(specs) + [ANY] * waits, compiler_params=params(), **options
    )(*args, *deps)


def run_copies(copies):
    for copy in copies:
        copy.start()
    for copy in copies:
        copy.wait()


def spread(onehot, value):
    high = value.astype(BF16)
    low = (value - high.astype(F32)).astype(BF16)
    return jnp.dot(onehot, high, preferred_element_type=F32) + jnp.dot(
        onehot, low, preferred_element_type=F32
    )


class Weights:
    def __init__(self, layer):
        self.count = lax.axis_size("mp")
        self.block_rows, self.width = layer.shape
        dp_index = lax.axis_index("dp")
        half = self.block_rows // 2
        self.offsets = [dp_index * half, (1 - dp_index) * half]
        self.pieces = [(layer, 0, None, 0)]
        self.colored = self.count == 4 and lax.axis_size("dp") == 2
        self.part = part = half // 2
        if self.colored:
            self.first = lax.dynamic_slice_in_dim(layer, dp_index * half, part, 0)
            self.second = lax.dynamic_slice_in_dim(layer, dp_index * half + part, part, 0)
            self.b1 = self.swap(self.second, 1)
            self.a2 = self.swap(self.first, 2)
            self.a1 = self.swap(self.first, 1)
            self.b2 = self.swap(self.second, 2)
            self.a3 = self.swap(self.a1, 2)
            self.b3 = self.swap(self.b2, 1)
            got = [(self.a1, 1, 0), (self.b2, 2, part), (self.b1, 1, part), (self.a2, 2, 0), (self.a3, 3, 0), (self.b3, 3, part)]
            for array, block, base in got:
                self.pieces.append((array, block, 0, base))
                self.pieces.append((dp_swap(array), block, 1, base))
        else:
            for block in range(1, self.count):
                self.pieces.append((mp_swap(layer, block), block, None, 0))

    def swap(self, array, flip):
        return mp_swap(array, flip)

    def assemble(self, ids):
        early = len(self.pieces) - 4 if self.colored else len(self.pieces)
        layer = self.place(ids, None, self.pieces[:early], "assemble")
        return layer if early == len(self.pieces) else self.place(ids, layer, self.pieces[early:], "complete")

    def place(self, ids, layer, pieces, name):
        many = len(pieces)

        def body(ids_ref, *refs):
            out, sems = refs[-2:]
            copies = []
            for i, (array, block, which, base) in enumerate(pieces):
                row = pl.multiple_of(ids_ref[3 + block] * self.block_rows, self.block_rows) + base
                if which is not None:
                    row = row + pl.multiple_of(ids_ref[1 + which], self.block_rows // 2)
                copies.append(
                    pltpu.make_async_copy(refs[i], out.at[pl.ds(row, array.shape[0]), :], sems.at[i])
                )
            run_copies(copies)

        before = [] if layer is None else [layer]
        return call(
            body,
            [ids, *[piece[0] for piece in pieces], *before],
            [SMEM] + [ANY] * many + [VMEM] * len(before),
            out_shape=jax.ShapeDtypeStruct((self.count * self.block_rows, self.width), BF16),
            out_specs=VMEM,
            input_output_aliases={1 + many: 0} if before else {},
            scratch_shapes=[pltpu.SemaphoreType.DMA((many,))],
            name=name,
        )


def fwd_stage(deps, level, ids, layer, rows, onehot, slope, kept):
    height, width = rows.shape
    prims = onehot.shape[1]
    leads = slope is None
    nb = width // BLOCKS

    def body(ids_ref, layer_ref, rows_ref, onehot_ref, *rest):
        if not leads:
            slope_ref, *rest = rest
        next_ref, pre_ref, kept_ref, *rest = rest[(kept is not None) :]
        if leads:
            tanh_ref, *rest = rest
        (kept_sem,) = rest

        @pl.when(ids_ref[0] == level)
        def _():
            keep = pltpu.make_async_copy(rows_ref, kept_ref, kept_sem)
            keep.start()

            def block(n, carry):
                cols = pl.ds(pl.multiple_of(n * nb, nb), nb)
                acc = jnp.dot(rows_ref[...], layer_ref[:, cols], preferred_element_type=F32)
                old = rows_ref[:, cols].astype(F32)
                pre_ref[:, cols] = acc.astype(BF16)
                if leads:
                    tanh_p = jnp.tanh(acc[:prims])
                    tanh_ref[:, cols] = tanh_p
                    factor = spread(onehot_ref[...], 1.0 - tanh_p * tanh_p)
                    new = jnp.concatenate(
                        [old[:prims] + tanh_p, old[prims:] + factor * acc[prims:]], axis=0
                    )
                else:
                    tanh_p = slope_ref[:, cols]
                    new = old + spread(onehot_ref[...], 1.0 - tanh_p * tanh_p) * acc
                next_ref[:, cols] = new.astype(BF16)
                return carry

            lax.fori_loop(0, BLOCKS, block, 0)
            keep.wait()

    outs = [jax.ShapeDtypeStruct((height, width), BF16)] * 3
    if leads:
        outs.append(jax.ShapeDtypeStruct((prims, width), F32))
    args = [ids, layer, rows, onehot] + ([] if leads else [slope])
    specs = [SMEM] + [VMEM] * (len(args) - 1)
    alias = {}
    if kept is not None:
        alias = {len(args): 2}
        args.append(kept)
        specs.append(ANY)
    return call(
        body,
        args,
        specs,
        deps,
        out_shape=outs,
        out_specs=[VMEM, VMEM, ANY] + [VMEM] * (len(outs) - 3),
        input_output_aliases=alias,
        scratch_shapes=[pltpu.SemaphoreType.DMA],
        cost_estimate=pl.CostEstimate(flops=2 * height * width * width * 4, bytes_accessed=2 * width * width, transcendentals=0),
        name=f"fwd{level}",
    )


def bwd_stage(deps, level, ids, layer, cot, pre, tanh_p, onehot, onehot_t, total, leads, kept):
    height, width = cot.shape
    prims = tanh_p.shape[0]
    deep = level > 0
    nb = width // BLOCKS

    def body(ids_ref, cot_ref, pre_ref, tanh_ref, onehot_ref, onehot_t_ref, *rest):
        if total is not None:
            total_ref, *rest = rest
        if deep:
            layer_ref, *rest = rest
        kept_ref, side_ref, *rest = rest[(kept is not None) :]
        if deep:
            new_ref, *rest = rest
        mix_ref, kept_sem = rest

        @pl.when(ids_ref[0] == level)
        def _():
            skip = prims if leads else 0

            def block(n, carry):
                cols = pl.ds(pl.multiple_of(n * nb, nb), nb)
                up = cot_ref[:, cols].astype(F32)
                tanh = tanh_ref[:, cols]
                slope = 1.0 - tanh * tanh
                up_t = up[skip:]
                mix_t = up_t * spread(onehot_ref[...], slope)
                total_here = spread(onehot_t_ref[...], up_t * pre_ref[:, cols].astype(F32)[skip:])
                if total is not None:
                    total_here = total_here + total_ref[:, cols]
                if leads:
                    mix_p = up[:prims] * slope - 2.0 * total_here * tanh * slope
                    mix_ref[:, cols] = jnp.concatenate([mix_p, mix_t], axis=0).astype(BF16)
                else:
                    mix_ref[:, cols] = mix_t.astype(BF16)
                side_ref[:, cols] = total_here
                return carry

            lax.fori_loop(0, BLOCKS, block, 0)
            keep = pltpu.make_async_copy(mix_ref, kept_ref, kept_sem)
            keep.start()
            if deep:

                def back_block(n, carry):
                    cols = pl.ds(pl.multiple_of(n * nb, nb), nb)
                    back = lax.dot_general(
                        mix_ref[...], layer_ref[cols, :], (((1,), (1,)), ((), ())), preferred_element_type=F32
                    )
                    new_ref[:, cols] = (cot_ref[:, cols].astype(F32) + back).astype(BF16)
                    return carry

                lax.fori_loop(0, BLOCKS, back_block, 0)
            keep.wait()

    rows_shape = jax.ShapeDtypeStruct((height, width), BF16)
    outs = [rows_shape, jax.ShapeDtypeStruct((prims, width), F32)] + ([rows_shape] if deep else [])
    args = [ids, cot, pre, tanh_p, onehot, onehot_t] + ([] if total is None else [total])
    args += [layer] if deep else []
    specs = [SMEM] + [VMEM] * (len(args) - 1)
    alias = {}
    if kept is not None:
        alias = {len(args): 0}
        args.append(kept)
        specs.append(ANY)
    return call(
        body,
        args,
        specs,
        deps,
        out_shape=outs,
        out_specs=[ANY] + [VMEM] * (len(outs) - 1),
        input_output_aliases=alias,
        scratch_shapes=[pltpu.VMEM((height, width), BF16), pltpu.SemaphoreType.DMA],
        cost_estimate=pl.CostEstimate(flops=2 * height * width * width * 4, bytes_accessed=2 * width * width, transcendentals=0),
        name=f"bwd{level}",
    )


def pick_rows(deps, ids, index, pieces, level):
    height = index.shape[0]
    piece_rows, width = pieces[0].shape

    def body(ids_ref, index_ref, *rest):
        out_ref = rest[-1]

        @pl.when(ids_ref[0] == level)
        def _():
            index_here = index_ref[...]
            acc = jnp.zeros((height, width), F32)
            for k, piece_ref in enumerate(rest[:-1]):
                place = lax.broadcasted_iota(jnp.int32, (height, piece_rows), 1) + k * piece_rows
                onehot = jnp.where(place == index_here, 1.0, 0.0).astype(BF16)
                acc = acc + jnp.dot(onehot, piece_ref[...], preferred_element_type=F32)
            out_ref[...] = acc.astype(BF16)

    return call(
        body,
        [ids, index, *pieces],
        [SMEM] + [VMEM] * (1 + len(pieces)),
        deps,
        out_shape=jax.ShapeDtypeStruct((height, width), BF16),
        out_specs=VMEM,
        name="pick",
    )


def lift_rows(ids, rows, encoder, chunks):
    height = rows.shape[0] // chunks
    width = encoder.shape[1]

    def body(ids_ref, rows_ref, encoder_ref, *outs):
        @pl.when(ids_ref[0] == 0)
        def _():
            for c, out in enumerate(outs):
                part = rows_ref[c * height : (c + 1) * height, :]
                out[...] = jnp.dot(part, encoder_ref[...], preferred_element_type=F32).astype(BF16)

    return pl.pallas_call(
        body,
        out_shape=[jax.ShapeDtypeStruct((height, width), BF16)] * chunks,
        in_specs=[SMEM, VMEM, VMEM],
        out_specs=[VMEM] * chunks,
        compiler_params=params(),
        name="lift",
    )(ids, rows, encoder)


def pack_columns(deps, ids, chunks, tails, level, n_dp, n_mp, blk):
    count = len(chunks)
    height, _ = chunks[0].shape
    tail_rows, tail_width = tails[0].shape if tails else (height, 0)
    core = n_dp * blk

    def body(ids_ref, *refs):
        chunk_refs, rest = refs[:count], refs[count:]
        tail_refs, outs = rest[: len(tails)], rest[len(tails) :]

        def fill():
            for k, out in enumerate(outs):
                for c, chunk_ref in enumerate(chunk_refs):
                    first = c * tail_rows
                    for d in range(n_dp):
                        col = pl.multiple_of((ids_ref[3 + k] + d * n_mp) * blk, blk)
                        out[first : first + height, d * blk : (d + 1) * blk] = chunk_ref[:, pl.ds(col, blk)]
                    if tails:
                        out[first + height : first + tail_rows, :core] = jnp.zeros((EXTRA, core), BF16)
                        out[first : first + tail_rows, core:] = tail_refs[c][...]

        if level is None:
            fill()
        else:
            pl.when(ids_ref[0] == level)(fill)

    shape = jax.ShapeDtypeStruct((count * tail_rows, core + tail_width), BF16)
    return call(
        body,
        [ids, *chunks, *tails],
        [SMEM] + [VMEM] * (count + len(tails)),
        deps,
        out_shape=[shape] * n_mp,
        out_specs=[VMEM] * n_mp,
        name="pack",
    )


def both_groups(pieces):
    return pieces + ([dp_swap(piece) for piece in pieces] if lax.axis_size("dp") > 1 else [])


def loss_rows(loss, cols):
    high = loss.astype(BF16).astype(F32)
    line = lax.broadcasted_iota(jnp.int32, (EXTRA, cols), 0)
    return jnp.where(line == 0, high, jnp.where(line == 1, loss - high, 0.0))


def head_partial(deps, ids, pieces, level, blk, height):
    rows_each, wide = pieces[0].shape
    core = 2 * blk
    out_width = wide - core
    many = len(pieces)

    def body(ids_ref, *refs):
        piece_refs, (mine_ref, send_ref, left, right, sems) = refs[:many], refs[many:]

        @pl.when(ids_ref[0] == level)
        def _():
            here = pl.multiple_of(ids_ref[1] // ids_ref[7] * blk, blk)
            there = pl.multiple_of(blk - here, blk)
            copies = []
            for i, ref in enumerate(piece_refs):
                rows = pl.ds(i * rows_each, rows_each)
                copies.append(pltpu.make_async_copy(ref.at[:, pl.ds(here, blk)], left.at[rows, :blk], sems.at[0, i]))
                copies.append(pltpu.make_async_copy(ref.at[:, pl.ds(there, blk)], left.at[rows, blk:], sems.at[1, i]))
                copies.append(pltpu.make_async_copy(ref.at[:, core:], right.at[rows], sems.at[2, i]))
            run_copies(copies)
            loss = jnp.zeros((1, 128), F32)
            for first in range(height, many * rows_each, height + EXTRA):
                loss = loss + right[first : first + 1, :128].astype(F32) + right[first + 1 : first + 2, :128].astype(F32)
            tail = loss_rows(loss[:, :1], out_width)
            part = lax.dot_general(left[...], right[...], (((0,), (0,)), ((), ())), preferred_element_type=F32)
            mine_ref[:blk, :] = part[:blk]
            mine_ref[blk:, :] = tail
            send_ref[:blk, :] = part[blk:].astype(BF16)
            send_ref[blk:, :] = tail.astype(BF16)

    shape = (blk + EXTRA, out_width)
    return call(
        body,
        [ids, *pieces],
        [SMEM] + [ANY] * many,
        deps,
        out_shape=[jax.ShapeDtypeStruct(shape, F32), jax.ShapeDtypeStruct(shape, BF16)],
        out_specs=[VMEM] * 2,
        scratch_shapes=[
            pltpu.VMEM((many * rows_each, core), BF16),
            pltpu.VMEM((many * rows_each, out_width), BF16),
            pltpu.SemaphoreType.DMA((3, many)),
        ],
        name="head_partial",
    )


def head_gradient(deps, ids, mine, other, level, blk, n_sec):
    cols = mine.shape[1] // n_sec

    def body(ids_ref, mine_ref, other_ref, *outs):
        @pl.when(ids_ref[0] == level)
        def _():
            tails = mine_ref[blk:, :1] + other_ref[blk:, :128].astype(F32)[:, :1]
            tail = loss_rows(tails[0:1] + tails[1:2], cols).astype(BF16)
            for j, out in enumerate(outs):
                span = slice(j * cols, (j + 1) * cols)
                out[:blk, :] = (mine_ref[:blk, span] + other_ref[:blk, span].astype(F32)).astype(BF16)
                out[blk:, :] = tail

    return call(
        body,
        [ids, mine, other],
        [SMEM, VMEM, VMEM],
        deps,
        out_shape=[jax.ShapeDtypeStruct((blk + EXTRA, cols), BF16)] * n_sec,
        out_specs=[VMEM] * n_sec,
        name="grad_head",
    )


def layer_gradient(deps, ids, blocks, chunk, mixes, blk, height, before):
    many = len(mixes)
    width = mixes[0].shape[1]
    nb = width // BLOCKS
    full = before is None
    tall = 2 * blk if full else blk
    extra = [] if full else before

    def body(ids_ref, *refs):
        block_refs, mix_refs = refs[:many], refs[many : 2 * many]
        rest = refs[2 * many :]
        before_refs, rest = rest[: len(extra)], rest[len(extra) :]
        outs, (left, right, turned, sems) = rest[:-4], rest[-4:]
        here = pl.multiple_of(ids_ref[1] // ids_ref[7] * blk, blk)
        starts = [here, pl.multiple_of(blk - here, blk)] if full else [here]
        top = chunk * height
        copies = []
        for i in range(many):
            rows = pl.ds(i * height, height)
            for j, col in enumerate(starts):
                src = block_refs[i].at[top : top + height, pl.ds(col, blk)]
                copies.append(pltpu.make_async_copy(src, left.at[rows, j * blk : (j + 1) * blk], sems.at[j, i]))
            copies.append(pltpu.make_async_copy(mix_refs[i], right.at[rows], sems.at[2, i]))
        run_copies(copies)
        turned[...] = left[...].astype(F32).T.astype(BF16)

        def block(n, carry):
            cols = pl.ds(pl.multiple_of(n * nb, nb), nb)
            part = jnp.dot(turned[...], right[:, cols], preferred_element_type=F32)
            if full:
                outs[1][:, cols] = part[blk:].astype(BF16)
            for ref in before_refs:
                part = part + ref[:, cols].astype(F32)
            outs[0][:, cols] = part[:blk]
            return carry

        lax.fori_loop(0, BLOCKS, block, 0)

    shape = jax.ShapeDtypeStruct((blk, width), F32)
    return call(
        body,
        [ids, *blocks, *mixes, *extra],
        [SMEM] + [ANY] * (2 * many) + [VMEM] * len(extra),
        deps,
        out_shape=[shape, jax.ShapeDtypeStruct((blk, width), BF16)] if full else shape,
        out_specs=[VMEM] * 2 if full else VMEM,
        scratch_shapes=[
            pltpu.VMEM((many * height, tall), BF16),
            pltpu.VMEM((many * height, width), BF16),
            pltpu.VMEM((tall, many * height), BF16),
            pltpu.SemaphoreType.DMA((3, many)),
        ],
        name="grad_layer",
    )


def join_rows(deps, flat, deep, rows_out):
    count, rank, width = deep.shape

    def body(flat_ref, deep_ref, out, sem):
        copies = [
            pltpu.make_async_copy(deep_ref.at[i], out.at[i * rank : (i + 1) * rank], sem.at[i])
            for i in range(count)
        ]
        for copy in copies:
            copy.start()
        spare = jnp.zeros((rows_out - count * (rank + 1), width), F32)
        out[count * rank :, :] = jnp.concatenate([flat_ref[...].astype(F32), spare], axis=0).astype(BF16)
        for copy in copies:
            copy.wait()

    return call(
        body,
        [flat, deep],
        [VMEM, ANY],
        deps,
        out_shape=jax.ShapeDtypeStruct((rows_out, width), BF16),
        out_specs=VMEM,
        scratch_shapes=[pltpu.SemaphoreType.DMA((count,))],
        name="join",
    )


def head_stage(deps, level, ids, rows, wanted, share, head_weight):
    height, width = rows.shape
    out_width = head_weight.shape[1]

    def body(ids_ref, rows_ref, wanted_ref, share_ref, head_ref, cot_ref, new_ref):
        @pl.when(ids_ref[0] == level)
        def _():
            nb = out_width // BLOCKS

            def block(n, loss):
                cols = pl.ds(pl.multiple_of(n * nb, nb), nb)
                outputs = jnp.dot(rows_ref[...], head_ref[:, cols], preferred_element_type=F32)
                mismatch = outputs - wanted_ref[:, cols].astype(F32)
                scaled = share_ref[...] * mismatch
                cot_ref[:height, cols] = (2.0 * scaled).astype(BF16)
                return loss + jnp.sum(scaled * mismatch, axis=1, keepdims=True)

            loss = lax.fori_loop(0, BLOCKS, block, jnp.zeros((height, 1), F32))
            loss = jnp.sum(loss, axis=0, keepdims=True)
            line = lax.broadcasted_iota(jnp.int32, (EXTRA, out_width), 0)
            high = loss.astype(BF16).astype(F32)
            tail = jnp.where(line == 0, high, jnp.where(line == 1, loss - high, 0.0))
            cot_ref[height:, :] = tail.astype(BF16)
            kb = width // BLOCKS

            def back_block(k, carry):
                cols = pl.ds(pl.multiple_of(k * kb, kb), kb)
                new_ref[:, cols] = lax.dot_general(
                    cot_ref[:height, :], head_ref[cols, :], (((1,), (1,)), ((), ())), preferred_element_type=F32
                ).astype(BF16)
                return carry

            lax.fori_loop(0, BLOCKS, back_block, 0)

    return call(
        body,
        [ids, rows, wanted, share, head_weight],
        [SMEM] + [VMEM] * 4,
        deps,
        out_shape=[
            jax.ShapeDtypeStruct((height + EXTRA, out_width), BF16),
            jax.ShapeDtypeStruct((height, width), BF16),
        ],
        out_specs=[VMEM] * 2,
        cost_estimate=pl.CostEstimate(flops=2 * height * width * width * 4, bytes_accessed=2 * width * out_width, transcendentals=0),
        name="head",
    )


def local(
    inputs, tangents, targets, target_jac, rank_mask, batch_order, encoder, layers, head_weight
):
    samp_dev, rank = rank_mask.shape
    in_width = inputs.shape[1]
    width = layers.shape[2]
    out_width = head_weight.shape[1]
    n_dp = lax.axis_size("dp")
    n_mp = lax.axis_size("mp")
    n_sec = lax.axis_size("section")
    last = n_sec - 1
    dp_index = lax.axis_index("dp")
    sec = lax.axis_index("section")
    mp_index = lax.axis_index("mp")
    prims = n_mp * samp_dev
    blk = width // (n_dp * n_mp)

    weights = Weights(layers[0])
    helper = last

    piece_rows = round_up(samp_dev * (rank + 1), 16)
    joined_rows = join_rows([], inputs, tangents, piece_rows)
    row_pieces = plane_pieces(joined_rows, helper)

    own_rank = jnp.sum(rank_mask, axis=1)
    slot_line = jnp.arange(samp_dev, dtype=jnp.int32)
    own_slot = jnp.sum(
        jnp.where(batch_order[0][None, :] == slot_line[:, None], slot_line[None, :], 0), axis=1
    ) // (samp_dev // MB)
    own_meta = jnp.stack([own_rank, own_slot]).astype(jnp.int32)
    meta_pieces = jnp.stack(mp_pieces(own_meta))
    order_line = jnp.arange(n_mp, dtype=jnp.int32)
    swap = ((order_line[:, None] ^ mp_index) == order_line[None, :]).astype(jnp.int32)
    meta = jnp.sum(swap[:, :, None, None] * meta_pieces[None], axis=1)
    ranks = meta[:, 0].reshape(prims)
    slots = meta[:, 1].reshape(prims)
    sample_line = jnp.arange(prims, dtype=jnp.int32)
    ends = jnp.sum(jnp.where(sample_line[None, :] <= sample_line[:, None], ranks[None, :], 0), axis=1)
    active = jnp.sum(ranks)
    counts = jnp.sum(jnp.where(slots[None, :] == slots[:, None], ranks[None, :] + 1, 0), axis=1)
    inverse = 1.0 / counts.astype(F32)

    kb = width // n_mp
    ids = jnp.stack(
        [sec] + weights.offsets + [mp_index ^ k for k in range(n_mp)] + [jnp.int32(kb // 2)] * (n_mp == 4)
    ).astype(jnp.int32)
    chunks = 2
    usual = samp_dev * (rank // 2 + 1)
    height = max(round_up(-(-(prims + usual) // chunks), 16), round_up(prims + 8, 16))
    slots_here = chunks * height - prims

    place = mp_index * slots_here + jnp.arange(slots_here, dtype=jnp.int32)
    passed = ends[None, :] <= place[:, None]
    sample = jnp.sum(passed.astype(jnp.int32), axis=1)
    column = place - jnp.sum(jnp.where(passed, ranks[None, :], 0), axis=1)
    present = place < active
    belongs = (sample[:, None] == sample_line[None, :]) & present[:, None]
    source = ((sample // samp_dev) ^ mp_index) * piece_rows + (sample % samp_dev) * rank + column
    source = jnp.where(present, source, -1)
    source_p = ((sample_line // samp_dev) ^ mp_index) * piece_rows + samp_dev * rank + sample_line % samp_dev
    share = jnp.sum(jnp.where(belongs, inverse[None, :], 0.0), axis=1)
    share_p = jnp.where(sample_line // samp_dev == mp_index, inverse, 0.0)
    index = jnp.concatenate([source_p, source])[:, None]
    shares = jnp.concatenate([share_p, share])[:, None]
    onehot = belongs.astype(BF16)
    first = height - prims
    onehots = [onehot[:first], onehot[first:]]
    onehots_t = [part.T for part in onehots]
    share_of = [shares[:height], shares[height:]]

    packed = pick_rows([], ids, index, row_pieces, helper)
    if helper != 0:
        packed = hop(packed, helper, 0)
    rows = list(lift_rows(ids, packed, encoder, chunks))
    layer = weights.assemble(ids)
    other_active = dp_swap(active.reshape(1, 1)).reshape(()) if n_dp > 1 else active
    most_active = jnp.maximum(active, other_active)

    token = []
    entered = [None] * chunks
    pres = [[None] * n_sec for _ in range(chunks)]
    tanhs = [None] * n_sec
    heads = [None] * chunks
    goal_pieces = None
    for level in range(n_sec):
        for c in range(chunks):
            got = fwd_stage(
                token, level, ids, layer, rows[c], onehots[c], None if c == 0 else tanhs[level], entered[c]
            )
            token = [got[0]]
            entered[c], pres[c][level] = got[2], got[1]
            if c == 0:
                tanhs[level] = got[3]
            rows[c] = got[0] if level == last else hop(got[0], level, level + 1)
            if level == last:
                heads[c] = head_stage(
                    token, last, ids, rows[c], wanted[c * height : (c + 1) * height], share_of[c], head_weight
                )
                token = [heads[c][1]]
        if goal_pieces is None:
            goal_pieces = plane_pieces(join_rows(token, targets, target_jac, piece_rows), last)
        if level == max(last - 1, 0):
            wanted = pick_rows([*token, most_active.reshape(1)], ids, index, goal_pieces, last)
            token = [wanted]

    small = n_dp * n_mp <= 8 and blk % 128 == 0
    cots = [heads[c][1] for c in range(chunks)]
    mixes = [None] * chunks
    backward_order = list(range(1, chunks)) + [0]
    hidden_pieces = head_pieces = None
    arrived = []
    for level in range(last, -1, -1):
        total = None
        for c in backward_order:
            got = bwd_stage(
                token, level, ids, layer, cots[c], pres[c][level], tanhs[level],
                onehots[c], onehots_t[c], total, c == 0, mixes[c],
            )
            mixes[c], total = got[0], got[1]
            token = [got[1]]
            if level > 0:
                cots[c] = hop(got[2], level, level - 1)
        if not small:
            continue
        if level == last:
            sends = pack_columns(token, ids, rows, [h[0] for h in heads], last, n_dp, n_mp, blk)
            token = [sends[0]]
            base = last * n_mp
            head_pieces = [sends[0]] + [
                lax.ppermute(sends[k], ("section", "mp"), [(base + m, base + (m ^ k)) for m in range(n_mp)])
                for k in range(1, n_mp)
            ]
        elif level == last - 1:
            sends = pack_columns(token, ids, entered, [], None, n_dp, n_mp, blk)
            token = [sends[0]]
            hidden_pieces = [sends[0]] + [mp_swap(sends[k], k) for k in range(1, n_mp)]
        elif level == last - 2:
            hidden_pieces = both_groups(hidden_pieces)
            token = [*token, *hidden_pieces]

    cols = out_width // n_sec
    if small:
        swapped = []
        for c in backward_order:
            swapped.append([mixes[c]] + [mp_swap(mixes[c], k) for k in range(1, n_mp)])
        mine, send = layer_gradient([], ids, hidden_pieces[:n_mp], 1, swapped[0], blk, height, None)
        grad_parts = [mine, dp_swap(send)]
        mine, send = head_partial([], ids, head_pieces, last, blk, height)
        other = dp_swap(send)
        blocks = head_gradient([], ids, mine, other, last, blk, n_sec)
        arrived = [hop(blocks[j], last, j) for j in range(last)]
        head_ext = blocks[last].astype(F32)
        for j in range(last):
            head_ext = jnp.where(sec == j, arrived[j].astype(F32), head_ext)
        head_mine = head_ext[:blk]
        loss_mine = (head_ext[blk, 0] + head_ext[blk + 1, 0]) / (n_dp * MB * out_width)
        grad = layer_gradient([], ids, hidden_pieces, 0, both_groups(swapped[1]), blk, height, grad_parts)
    else:
        contract = (((0,), (0,)), ((), ()))
        joined = jnp.concatenate(entered, axis=0)
        part = lax.dot_general(joined, jnp.concatenate(mixes, axis=0), contract, preferred_element_type=F32)
        grad = lax.psum_scatter(part.astype(BF16), ("dp", "mp"), scatter_dimension=0, tiled=True).astype(F32)
        cot_out = jnp.concatenate([h[0][:height] for h in heads], axis=0)
        part = lax.dot_general(jnp.concatenate(rows, axis=0), cot_out, contract, preferred_element_type=F32)
        head = lax.psum_scatter(part.astype(BF16), ("dp", "mp"), scatter_dimension=0, tiled=True)
        loss = sum(jnp.sum(h[0][height : height + 2, 0].astype(F32)) for h in heads)
        loss = jnp.where(sec == last, lax.psum(loss, ("dp", "mp")), 0.0).reshape(1, 1)
        head_mine = jnp.where(sec == last, head[:, last * cols :], jnp.zeros((blk, cols), BF16))
        loss_mine = loss
        for j in range(last):
            head_mine = head_mine + hop(head[:, j * cols : (j + 1) * cols], last, j)
            loss_mine = loss_mine + hop(loss, last, j)
        head_mine = head_mine.astype(F32)
        loss_mine = loss_mine.reshape(()) / (n_dp * MB * out_width)
    fast = (grad[None], head_mine, loss_mine)

    def plain():
        depth = rank + 1
        total_rows = samp_dev * depth
        layer_full = jnp.zeros((width, width), BF16)
        kb = weights.block_rows
        for array, block, which, base in weights.pieces:
            row = (mp_index ^ block) * kb + base
            row = row if which is None else row + weights.offsets[which]
            layer_full = lax.dynamic_update_slice_in_dim(layer_full, array, row, 0)
        rows_in = jnp.concatenate([inputs[:, None, :], tangents], axis=1).reshape(total_rows, in_width)
        start = jnp.dot(rows_in, encoder, preferred_element_type=F32).astype(BF16)
        chain = [(j, (j + 1) % n_sec) for j in range(n_sec)]

        def back_one(value):
            return lax.fori_loop(0, last, lambda _, v: lax.ppermute(v, "section", chain), value)

        def pre_of(rows):
            pre = jnp.dot(rows, layer_full, preferred_element_type=F32).reshape(samp_dev, depth, width)
            tanh_p = jnp.tanh(pre[:, 0])
            return pre, tanh_p, 1.0 - tanh_p * tanh_p

        def forward(level, state):
            rows, mine, _ = state
            mine = jnp.where(level == sec, rows, mine)
            pre, tanh_p, slope = pre_of(rows)
            change = jnp.concatenate([tanh_p[:, None], slope[:, None] * pre[:, 1:]], axis=1)
            new = (rows.astype(F32) + change.reshape(total_rows, width)).astype(BF16)
            return lax.ppermute(new, "section", chain), mine, new

        _, mine, final = lax.fori_loop(0, n_sec, forward, (start, start, start))
        own = lax.dynamic_slice_in_dim(inverse, mp_index * samp_dev, samp_dev, 0)
        row_weight = jnp.concatenate([jnp.ones((samp_dev, 1), F32), rank_mask.astype(F32)], axis=1)
        share = (row_weight * own[:, None]).reshape(total_rows, 1)
        outputs = jnp.dot(final, head_weight, preferred_element_type=F32)
        wanted = jnp.concatenate([targets[:, None, :], target_jac], axis=1).reshape(total_rows, out_width)
        mismatch = outputs - wanted.astype(F32)
        loss = jnp.sum(share * mismatch * mismatch)
        cot_out = (2.0 * share * mismatch).astype(BF16)
        cot = lax.dot_general(cot_out, head_weight, (((1,), (1,)), ((), ())), preferred_element_type=F32)
        pre, tanh_p, slope = pre_of(mine)

        def backward(step, state):
            cot, mix_mine = state
            up = cot.astype(F32).reshape(samp_dev, depth, width)
            side = jnp.sum(up[:, 1:] * pre[:, 1:], axis=1)
            lead = up[:, 0] * slope - 2.0 * side * tanh_p * slope
            mix = jnp.concatenate([lead[:, None], up[:, 1:] * slope[:, None]], axis=1)
            mix = mix.astype(BF16).reshape(total_rows, width)
            mix_mine = jnp.where(step == last - sec, mix, mix_mine)
            back = lax.dot_general(mix, layer_full, (((1,), (1,)), ((), ())), preferred_element_type=F32)
            new = (up.reshape(total_rows, width) + back).astype(BF16)
            return back_one(new), mix_mine

        _, mix = lax.fori_loop(0, n_sec, backward, (cot.astype(BF16), mine))

        def scatter(left, right):
            part = lax.dot_general(left, right, (((0,), (0,)), ((), ())), preferred_element_type=F32)
            part = part.astype(BF16).reshape(n_dp, n_mp, blk, right.shape[1])
            mine_part = jnp.zeros((n_dp, blk, right.shape[1]), F32)
            for k in range(n_mp):
                piece = lax.dynamic_index_in_dim(part, mp_index ^ k, 1, False)
                mine_part = mine_part + (piece if k == 0 else mp_swap(piece, k)).astype(F32)
            kept = lax.dynamic_index_in_dim(mine_part, dp_index, 0, False)
            if n_dp > 1:
                sent = lax.dynamic_index_in_dim(mine_part, 1 - dp_index, 0, False)
                kept = kept + dp_swap(sent.astype(BF16)).astype(F32)
            return kept

        grad = scatter(mine, mix)
        head = scatter(final, cot_out)
        cols = out_width // n_sec
        loss_group = sum(mp_pieces(loss.reshape(1, 1)))
        if n_dp > 1:
            loss_group = loss_group + dp_swap(loss_group)
        head_mine = jnp.where(sec == last, head[:, last * cols :], 0.0)
        loss_mine = jnp.where(sec == last, loss_group, 0.0)
        for j in range(last):
            block = jnp.concatenate([head[:, j * cols : (j + 1) * cols], jnp.broadcast_to(loss_group, (8, cols))])
            block = hop(block, last, j)
            head_mine = head_mine + block[:blk]
            loss_mine = loss_mine + block[blk:, :1][:1]
        return grad[None], head_mine, loss_mine.reshape(()) / (n_dp * MB * out_width)

    room = n_mp * slots_here
    if room >= n_mp * samp_dev * rank:
        return fast
    return lax.while_loop(
        lambda state: state[0] > room, lambda state: (jnp.int32(0), *plain()), (most_active, *fast)
    )[1:]


def solution(mesh):
    in_specs = (
        P(("dp", "mp"), None),
        P(("dp", "mp"), None, None),
        P(("dp", "mp"), None),
        P(("dp", "mp"), None, None),
        P(("dp", "mp"), None),
        P(("dp", "mp"), None),
        P(),
        P("section", "mp", None),
        P(),
    )
    out_specs = (P("section", ("dp", "mp"), None), P(("dp", "mp"), "section"), P())

    return jax.shard_map(local, mesh=mesh, in_specs=in_specs, out_specs=out_specs, check_vma=False)
```

```python
import jax
import jax.numpy as jnp
from jax import lax
from jax.experimental import pallas as pl
from jax.experimental.pallas import tpu as pltpu
from jax.sharding import PartitionSpec as P


F32 = jnp.float32
BF16 = jnp.bfloat16
MB = 6
EXTRA = 16
BLOCKS = 4

ANY = pl.BlockSpec(memory_space=pl.ANY)
SMEM = pl.BlockSpec(memory_space=pltpu.SMEM)
VMEM = pl.BlockSpec(memory_space=pltpu.VMEM)


def round_up(value, unit):
    return -(-value // unit) * unit


def mp_swap(value, flip):
    count = lax.axis_size("mp")
    return lax.ppermute(value, "mp", [(m, m ^ flip) for m in range(count)])


def dp_swap(value):
    count = lax.axis_size("dp")
    return lax.ppermute(value, "dp", [(d, d ^ 1) for d in range(count)])


def mp_pieces(value):
    return [value] + [mp_swap(value, k) for k in range(1, lax.axis_size("mp"))]


def hop(value, source, target):
    return lax.ppermute(value, "section", [(source, target)])


def plane_pieces(value, section):
    count = lax.axis_size("mp")
    base = section * count
    swaps = [[(base + m, base + (m ^ k)) for m in range(count)] for k in range(1, count)]
    return [value] + [lax.ppermute(value, ("section", "mp"), pairs) for pairs in swaps]


def params():
    return pltpu.CompilerParams(vmem_limit_bytes=16 * 2**20)


def call(body, args, specs, deps=(), **options):
    reads, waits = len(args), len(deps)

    def inner(*refs):
        body(*refs[:reads], *refs[reads + waits :])

    return pl.pallas_call(
        inner, in_specs=list(specs) + [ANY] * waits, compiler_params=params(), **options
    )(*args, *deps)


def run_copies(copies):
    for copy in copies:
        copy.start()
    for copy in copies:
        copy.wait()


def spread(onehot, value):
    high = value.astype(BF16)
    low = (value - high.astype(F32)).astype(BF16)
    return jnp.dot(onehot, high, preferred_element_type=F32) + jnp.dot(
        onehot, low, preferred_element_type=F32
    )


class Weights:
    def __init__(self, layer):
        self.count = lax.axis_size("mp")
        self.block_rows, self.width = layer.shape
        dp_index = lax.axis_index("dp")
        half = self.block_rows // 2
        self.offsets = [dp_index * half, (1 - dp_index) * half]
        self.pieces = [(layer, 0, None, 0)]
        self.colored = self.count == 4 and lax.axis_size("dp") == 2
        self.part = part = half // 2
        if self.colored:
            self.first = lax.dynamic_slice_in_dim(layer, dp_index * half, part, 0)
            self.second = lax.dynamic_slice_in_dim(layer, dp_index * half + part, part, 0)
            self.b1 = self.swap(self.second, 1)
            self.a2 = self.swap(self.first, 2)
            self.a1 = self.swap(self.first, 1)
            self.b2 = self.swap(self.second, 2)
            self.a3 = self.swap(self.a1, 2)
            self.b3 = self.swap(self.b2, 1)
            got = [(self.a1, 1, 0), (self.b2, 2, part), (self.b1, 1, part), (self.a2, 2, 0), (self.a3, 3, 0), (self.b3, 3, part)]
            for array, block, base in got:
                self.pieces.append((array, block, 0, base))
                self.pieces.append((dp_swap(array), block, 1, base))
        else:
            for block in range(1, self.count):
                self.pieces.append((mp_swap(layer, block), block, None, 0))

    def swap(self, array, flip):
        return mp_swap(array, flip)

    def assemble(self, ids, deps):
        early = len(self.pieces) - 4 if self.colored else len(self.pieces)
        layer = self.place(ids, None, self.pieces[:early], "assemble", deps)
        return layer if early == len(self.pieces) else self.place(ids, layer, self.pieces[early:], "complete", [])

    def place(self, ids, layer, pieces, name, deps):
        many = len(pieces)

        def body(ids_ref, *refs):
            out, sems = refs[-2:]
            copies = []
            for i, (array, block, which, base) in enumerate(pieces):
                row = pl.multiple_of(ids_ref[3 + block] * self.block_rows, self.block_rows) + base
                if which is not None:
                    row = row + pl.multiple_of(ids_ref[1 + which], self.block_rows // 2)
                copies.append(
                    pltpu.make_async_copy(refs[i], out.at[pl.ds(row, array.shape[0]), :], sems.at[i])
                )
            run_copies(copies)

        before = [] if layer is None else [layer]
        return call(
            body,
            [ids, *[piece[0] for piece in pieces], *before],
            [SMEM] + [ANY] * many + [VMEM] * len(before),
            deps,
            out_shape=jax.ShapeDtypeStruct((self.count * self.block_rows, self.width), BF16),
            out_specs=VMEM,
            input_output_aliases={1 + many: 0} if before else {},
            scratch_shapes=[pltpu.SemaphoreType.DMA((many,))],
            name=name,
        )


def fwd_stage(deps, level, ids, layer, rows, onehot, slope, kept):
    height, width = rows.shape
    prims = onehot.shape[1]
    leads = slope is None
    nb = width // BLOCKS

    def body(ids_ref, layer_ref, rows_ref, onehot_ref, *rest):
        if not leads:
            slope_ref, *rest = rest
        next_ref, pre_ref, kept_ref, *rest = rest[(kept is not None) :]
        if leads:
            tanh_ref, *rest = rest
        (kept_sem,) = rest

        @pl.when(ids_ref[0] == level)
        def _():
            keep = pltpu.make_async_copy(rows_ref, kept_ref, kept_sem)
            keep.start()

            def block(n, carry):
                cols = pl.ds(pl.multiple_of(n * nb, nb), nb)
                acc = jnp.dot(rows_ref[...], layer_ref[:, cols], preferred_element_type=F32)
                old = rows_ref[:, cols].astype(F32)
                pre_ref[:, cols] = acc.astype(BF16)
                if leads:
                    tanh_p = jnp.tanh(acc[:prims])
                    tanh_ref[:, cols] = tanh_p
                    factor = spread(onehot_ref[...], 1.0 - tanh_p * tanh_p)
                    new = jnp.concatenate(
                        [old[:prims] + tanh_p, old[prims:] + factor * acc[prims:]], axis=0
                    )
                else:
                    tanh_p = slope_ref[:, cols]
                    new = old + spread(onehot_ref[...], 1.0 - tanh_p * tanh_p) * acc
                next_ref[:, cols] = new.astype(BF16)
                return carry

            lax.fori_loop(0, BLOCKS, block, 0)
            keep.wait()

    outs = [jax.ShapeDtypeStruct((height, width), BF16)] * 3
    if leads:
        outs.append(jax.ShapeDtypeStruct((prims, width), F32))
    args = [ids, layer, rows, onehot] + ([] if leads else [slope])
    specs = [SMEM] + [VMEM] * (len(args) - 1)
    alias = {}
    if kept is not None:
        alias = {len(args): 2}
        args.append(kept)
        specs.append(ANY)
    return call(
        body,
        args,
        specs,
        deps,
        out_shape=outs,
        out_specs=[VMEM, VMEM, ANY] + [VMEM] * (len(outs) - 3),
        input_output_aliases=alias,
        scratch_shapes=[pltpu.SemaphoreType.DMA],
        cost_estimate=pl.CostEstimate(flops=2 * height * width * width * 4, bytes_accessed=2 * width * width, transcendentals=0),
        name=f"fwd{level}",
    )


def bwd_stage(deps, level, ids, layer, cot, pre, tanh_p, onehot, onehot_t, total, leads, kept):
    height, width = cot.shape
    prims = tanh_p.shape[0]
    deep = level > 0
    nb = width // BLOCKS

    def body(ids_ref, cot_ref, pre_ref, tanh_ref, onehot_ref, onehot_t_ref, *rest):
        if total is not None:
            total_ref, *rest = rest
        if deep:
            layer_ref, *rest = rest
        kept_ref, side_ref, *rest = rest[(kept is not None) :]
        if deep:
            new_ref, *rest = rest
        mix_ref, kept_sem = rest

        @pl.when(ids_ref[0] == level)
        def _():
            skip = prims if leads else 0

            def block(n, carry):
                cols = pl.ds(pl.multiple_of(n * nb, nb), nb)
                up = cot_ref[:, cols].astype(F32)
                tanh = tanh_ref[:, cols]
                slope = 1.0 - tanh * tanh
                up_t = up[skip:]
                mix_t = up_t * spread(onehot_ref[...], slope)
                total_here = spread(onehot_t_ref[...], up_t * pre_ref[:, cols].astype(F32)[skip:])
                if total is not None:
                    total_here = total_here + total_ref[:, cols]
                if leads:
                    mix_p = up[:prims] * slope - 2.0 * total_here * tanh * slope
                    mix_ref[:, cols] = jnp.concatenate([mix_p, mix_t], axis=0).astype(BF16)
                else:
                    mix_ref[:, cols] = mix_t.astype(BF16)
                side_ref[:, cols] = total_here
                return carry

            lax.fori_loop(0, BLOCKS, block, 0)
            keep = pltpu.make_async_copy(mix_ref, kept_ref, kept_sem)
            keep.start()
            if deep:

                def back_block(n, carry):
                    cols = pl.ds(pl.multiple_of(n * nb, nb), nb)
                    back = lax.dot_general(
                        mix_ref[...], layer_ref[cols, :], (((1,), (1,)), ((), ())), preferred_element_type=F32
                    )
                    new_ref[:, cols] = (cot_ref[:, cols].astype(F32) + back).astype(BF16)
                    return carry

                lax.fori_loop(0, BLOCKS, back_block, 0)
            keep.wait()

    rows_shape = jax.ShapeDtypeStruct((height, width), BF16)
    outs = [rows_shape, jax.ShapeDtypeStruct((prims, width), F32)] + ([rows_shape] if deep else [])
    args = [ids, cot, pre, tanh_p, onehot, onehot_t] + ([] if total is None else [total])
    args += [layer] if deep else []
    specs = [SMEM] + [VMEM] * (len(args) - 1)
    alias = {}
    if kept is not None:
        alias = {len(args): 0}
        args.append(kept)
        specs.append(ANY)
    return call(
        body,
        args,
        specs,
        deps,
        out_shape=outs,
        out_specs=[ANY] + [VMEM] * (len(outs) - 1),
        input_output_aliases=alias,
        scratch_shapes=[pltpu.VMEM((height, width), BF16), pltpu.SemaphoreType.DMA],
        cost_estimate=pl.CostEstimate(flops=2 * height * width * width * 4, bytes_accessed=2 * width * width, transcendentals=0),
        name=f"bwd{level}",
    )


def pick_rows(deps, ids, index, pieces, level):
    height = index.shape[0]
    piece_rows, width = pieces[0].shape

    def body(ids_ref, index_ref, *rest):
        out_ref = rest[-1]

        @pl.when(ids_ref[0] == level)
        def _():
            index_here = index_ref[...]
            acc = jnp.zeros((height, width), F32)
            for k, piece_ref in enumerate(rest[:-1]):
                place = lax.broadcasted_iota(jnp.int32, (height, piece_rows), 1) + k * piece_rows
                onehot = jnp.where(place == index_here, 1.0, 0.0).astype(BF16)
                acc = acc + jnp.dot(onehot, piece_ref[...], preferred_element_type=F32)
            out_ref[...] = acc.astype(BF16)

    return call(
        body,
        [ids, index, *pieces],
        [SMEM] + [VMEM] * (1 + len(pieces)),
        deps,
        out_shape=jax.ShapeDtypeStruct((height, width), BF16),
        out_specs=VMEM,
        name="pick",
    )


def lift_rows(ids, rows, encoder, chunks):
    height = rows.shape[0] // chunks
    width = encoder.shape[1]

    def body(ids_ref, rows_ref, encoder_ref, *outs):
        @pl.when(ids_ref[0] == 0)
        def _():
            for c, out in enumerate(outs):
                part = rows_ref[c * height : (c + 1) * height, :]
                out[...] = jnp.dot(part, encoder_ref[...], preferred_element_type=F32).astype(BF16)

    return pl.pallas_call(
        body,
        out_shape=[jax.ShapeDtypeStruct((height, width), BF16)] * chunks,
        in_specs=[SMEM, VMEM, VMEM],
        out_specs=[VMEM] * chunks,
        compiler_params=params(),
        name="lift",
    )(ids, rows, encoder)


def pack_columns(deps, ids, chunks, tails, level, n_dp, n_mp, blk):
    count = len(chunks)
    height, _ = chunks[0].shape
    tail_rows, tail_width = tails[0].shape if tails else (height, 0)
    core = n_dp * blk

    def body(ids_ref, *refs):
        chunk_refs, rest = refs[:count], refs[count:]
        tail_refs, outs = rest[: len(tails)], rest[len(tails) :]

        def fill():
            for k, out in enumerate(outs):
                for c, chunk_ref in enumerate(chunk_refs):
                    first = c * tail_rows
                    for d in range(n_dp):
                        col = pl.multiple_of((ids_ref[3 + k] + d * n_mp) * blk, blk)
                        out[first : first + height, d * blk : (d + 1) * blk] = chunk_ref[:, pl.ds(col, blk)]
                    if tails:
                        out[first + height : first + tail_rows, :core] = jnp.zeros((EXTRA, core), BF16)
                        out[first : first + tail_rows, core:] = tail_refs[c][...]

        if level is None:
            fill()
        else:
            pl.when(ids_ref[0] == level)(fill)

    shape = jax.ShapeDtypeStruct((count * tail_rows, core + tail_width), BF16)
    return call(
        body,
        [ids, *chunks, *tails],
        [SMEM] + [VMEM] * (count + len(tails)),
        deps,
        out_shape=[shape] * n_mp,
        out_specs=[VMEM] * n_mp,
        name="pack",
    )


def both_groups(pieces):
    return pieces + ([dp_swap(piece) for piece in pieces] if lax.axis_size("dp") > 1 else [])


def loss_rows(loss, cols):
    high = loss.astype(BF16).astype(F32)
    line = lax.broadcasted_iota(jnp.int32, (EXTRA, cols), 0)
    return jnp.where(line == 0, high, jnp.where(line == 1, loss - high, 0.0))


def head_partial(deps, ids, pieces, level, blk, height):
    rows_each, wide = pieces[0].shape
    core = 2 * blk
    out_width = wide - core
    many = len(pieces)

    def body(ids_ref, *refs):
        piece_refs, (mine_ref, send_ref, left, right, sems) = refs[:many], refs[many:]

        @pl.when(ids_ref[0] == level)
        def _():
            here = pl.multiple_of(ids_ref[1] // ids_ref[7] * blk, blk)
            there = pl.multiple_of(blk - here, blk)
            copies = []
            for i, ref in enumerate(piece_refs):
                rows = pl.ds(i * rows_each, rows_each)
                copies.append(pltpu.make_async_copy(ref.at[:, pl.ds(here, blk)], left.at[rows, :blk], sems.at[0, i]))
                copies.append(pltpu.make_async_copy(ref.at[:, pl.ds(there, blk)], left.at[rows, blk:], sems.at[1, i]))
                copies.append(pltpu.make_async_copy(ref.at[:, core:], right.at[rows], sems.at[2, i]))
            run_copies(copies)
            loss = jnp.zeros((1, 128), F32)
            for first in range(height, many * rows_each, height + EXTRA):
                loss = loss + right[first : first + 1, :128].astype(F32) + right[first + 1 : first + 2, :128].astype(F32)
            tail = loss_rows(loss[:, :1], out_width)
            part = lax.dot_general(left[...], right[...], (((0,), (0,)), ((), ())), preferred_element_type=F32)
            mine_ref[:blk, :] = part[:blk]
            mine_ref[blk:, :] = tail
            send_ref[:blk, :] = part[blk:].astype(BF16)
            send_ref[blk:, :] = tail.astype(BF16)

    shape = (blk + EXTRA, out_width)
    return call(
        body,
        [ids, *pieces],
        [SMEM] + [ANY] * many,
        deps,
        out_shape=[jax.ShapeDtypeStruct(shape, F32), jax.ShapeDtypeStruct(shape, BF16)],
        out_specs=[VMEM] * 2,
        scratch_shapes=[
            pltpu.VMEM((many * rows_each, core), BF16),
            pltpu.VMEM((many * rows_each, out_width), BF16),
            pltpu.SemaphoreType.DMA((3, many)),
        ],
        name="head_partial",
    )


def head_gradient(deps, ids, mine, other, level, blk, n_sec):
    cols = mine.shape[1] // n_sec

    def body(ids_ref, mine_ref, other_ref, *outs):
        @pl.when(ids_ref[0] == level)
        def _():
            tails = mine_ref[blk:, :1] + other_ref[blk:, :128].astype(F32)[:, :1]
            tail = loss_rows(tails[0:1] + tails[1:2], cols).astype(BF16)
            for j, out in enumerate(outs):
                span = slice(j * cols, (j + 1) * cols)
                out[:blk, :] = (mine_ref[:blk, span] + other_ref[:blk, span].astype(F32)).astype(BF16)
                out[blk:, :] = tail

    return call(
        body,
        [ids, mine, other],
        [SMEM, VMEM, VMEM],
        deps,
        out_shape=[jax.ShapeDtypeStruct((blk + EXTRA, cols), BF16)] * n_sec,
        out_specs=[VMEM] * n_sec,
        name="grad_head",
    )


def first_gradient(deps, ids, blocks, mixes, blk, height):
    many = len(mixes)
    every = len(blocks)
    width = mixes[0].shape[1]
    nb = width // BLOCKS

    def body(ids_ref, *refs):
        block_refs, mix_refs = refs[:every], refs[every : every + many]
        mine_ref, send_ref, later_ref, left, right, early, sems = refs[every + many :]
        here = pl.multiple_of(ids_ref[1] // ids_ref[7] * blk, blk)
        there = pl.multiple_of(blk - here, blk)
        copies = []
        for i in range(every):
            rows = pl.ds(i * height, height)
            if i < many:
                for j, col in enumerate([here, there]):
                    src = block_refs[i].at[height:, pl.ds(col, blk)]
                    copies.append(pltpu.make_async_copy(src, left.at[rows, j * blk : (j + 1) * blk], sems.at[j, i]))
                copies.append(pltpu.make_async_copy(mix_refs[i], right.at[rows], sems.at[2, i]))
            src = block_refs[i].at[:height, pl.ds(here, blk)]
            copies.append(pltpu.make_async_copy(src, early.at[rows], sems.at[3, i]))
        run_copies(copies)
        later_ref[...] = early[...].astype(F32).T.astype(BF16)
        turned = left[...].astype(F32).T.astype(BF16)
        for n in range(BLOCKS):
            cols = slice(n * nb, (n + 1) * nb)
            part = jnp.dot(turned, right[:, cols], preferred_element_type=F32)
            mine_ref[:, cols] = part[:blk]
            send_ref[:, cols] = part[blk:].astype(BF16)

    return call(
        body,
        [ids, *blocks, *mixes],
        [SMEM] + [ANY] * (every + many),
        deps,
        out_shape=[
            jax.ShapeDtypeStruct((blk, width), F32),
            jax.ShapeDtypeStruct((blk, width), BF16),
            jax.ShapeDtypeStruct((blk, every * height), BF16),
        ],
        out_specs=[VMEM] * 3,
        scratch_shapes=[
            pltpu.VMEM((many * height, 2 * blk), BF16),
            pltpu.VMEM((many * height, width), BF16),
            pltpu.VMEM((every * height, blk), BF16),
            pltpu.SemaphoreType.DMA((4, every)),
        ],
        name="first_gradient",
    )


def last_gradient(deps, turned, mixes, mine, other):
    blk, width = mine.shape
    nb = width // BLOCKS

    def body(turned_ref, *refs):
        mix_refs, (mine_ref, other_ref, out) = refs[:-3], refs[-3:]
        for n in range(BLOCKS):
            cols = slice(n * nb, (n + 1) * nb)
            right = jnp.concatenate([ref[:, cols] for ref in mix_refs], axis=0)
            part = jnp.dot(turned_ref[...], right, preferred_element_type=F32)
            out[:, cols] = part + mine_ref[:, cols] + other_ref[:, cols].astype(F32)

    return call(
        body,
        [turned, *mixes, mine, other],
        [VMEM] * (3 + len(mixes)),
        deps,
        out_shape=jax.ShapeDtypeStruct((blk, width), F32),
        out_specs=VMEM,
        name="last_gradient",
    )


def join_rows(deps, flat, deep, rows_out):
    count, rank, width = deep.shape

    def body(flat_ref, deep_ref, out, sem):
        copies = [
            pltpu.make_async_copy(deep_ref.at[i], out.at[i * rank : (i + 1) * rank], sem.at[i])
            for i in range(count)
        ]
        for copy in copies:
            copy.start()
        spare = jnp.zeros((rows_out - count * (rank + 1), width), F32)
        out[count * rank :, :] = jnp.concatenate([flat_ref[...].astype(F32), spare], axis=0).astype(BF16)
        for copy in copies:
            copy.wait()

    return call(
        body,
        [flat, deep],
        [VMEM, ANY],
        deps,
        out_shape=jax.ShapeDtypeStruct((rows_out, width), BF16),
        out_specs=VMEM,
        scratch_shapes=[pltpu.SemaphoreType.DMA((count,))],
        name="join",
    )


def head_stage(deps, level, ids, rows, wanted, share, head_weight):
    height, width = rows.shape
    out_width = head_weight.shape[1]

    def body(ids_ref, rows_ref, wanted_ref, share_ref, head_ref, cot_ref, new_ref):
        @pl.when(ids_ref[0] == level)
        def _():
            nb = out_width // BLOCKS

            def block(n, loss):
                cols = pl.ds(pl.multiple_of(n * nb, nb), nb)
                outputs = jnp.dot(rows_ref[...], head_ref[:, cols], preferred_element_type=F32)
                mismatch = outputs - wanted_ref[:, cols].astype(F32)
                scaled = share_ref[...] * mismatch
                cot_ref[:height, cols] = (2.0 * scaled).astype(BF16)
                return loss + jnp.sum(scaled * mismatch, axis=1, keepdims=True)

            loss = lax.fori_loop(0, BLOCKS, block, jnp.zeros((height, 1), F32))
            loss = jnp.sum(loss, axis=0, keepdims=True)
            line = lax.broadcasted_iota(jnp.int32, (EXTRA, out_width), 0)
            high = loss.astype(BF16).astype(F32)
            tail = jnp.where(line == 0, high, jnp.where(line == 1, loss - high, 0.0))
            cot_ref[height:, :] = tail.astype(BF16)
            kb = width // BLOCKS

            def back_block(k, carry):
                cols = pl.ds(pl.multiple_of(k * kb, kb), kb)
                new_ref[:, cols] = lax.dot_general(
                    cot_ref[:height, :], head_ref[cols, :], (((1,), (1,)), ((), ())), preferred_element_type=F32
                ).astype(BF16)
                return carry

            lax.fori_loop(0, BLOCKS, back_block, 0)

    return call(
        body,
        [ids, rows, wanted, share, head_weight],
        [SMEM] + [VMEM] * 4,
        deps,
        out_shape=[
            jax.ShapeDtypeStruct((height + EXTRA, out_width), BF16),
            jax.ShapeDtypeStruct((height, width), BF16),
        ],
        out_specs=[VMEM] * 2,
        cost_estimate=pl.CostEstimate(flops=2 * height * width * width * 4, bytes_accessed=2 * width * out_width, transcendentals=0),
        name="head",
    )


def local(
    inputs, tangents, targets, target_jac, rank_mask, batch_order, encoder, layers, head_weight
):
    samp_dev, rank = rank_mask.shape
    in_width = inputs.shape[1]
    width = layers.shape[2]
    out_width = head_weight.shape[1]
    n_dp = lax.axis_size("dp")
    n_mp = lax.axis_size("mp")
    n_sec = lax.axis_size("section")
    last = n_sec - 1
    dp_index = lax.axis_index("dp")
    sec = lax.axis_index("section")
    mp_index = lax.axis_index("mp")
    prims = n_mp * samp_dev
    blk = width // (n_dp * n_mp)

    weights = Weights(layers[0])
    helper = last

    piece_rows = round_up(samp_dev * (rank + 1), 16)
    joined_rows = join_rows([], inputs, tangents, piece_rows)
    row_pieces = plane_pieces(joined_rows, helper)

    own_rank = jnp.sum(rank_mask, axis=1)
    slot_line = jnp.arange(samp_dev, dtype=jnp.int32)
    own_slot = jnp.sum(
        jnp.where(batch_order[0][None, :] == slot_line[:, None], slot_line[None, :], 0), axis=1
    ) // (samp_dev // MB)
    own_meta = jnp.stack([own_rank, own_slot]).astype(jnp.int32)
    meta_pieces = jnp.stack(mp_pieces(own_meta))
    order_line = jnp.arange(n_mp, dtype=jnp.int32)
    swap = ((order_line[:, None] ^ mp_index) == order_line[None, :]).astype(jnp.int32)
    meta = jnp.sum(swap[:, :, None, None] * meta_pieces[None], axis=1)
    ranks = meta[:, 0].reshape(prims)
    slots = meta[:, 1].reshape(prims)
    sample_line = jnp.arange(prims, dtype=jnp.int32)
    ends = jnp.sum(jnp.where(sample_line[None, :] <= sample_line[:, None], ranks[None, :], 0), axis=1)
    active = jnp.sum(ranks)
    counts = jnp.sum(jnp.where(slots[None, :] == slots[:, None], ranks[None, :] + 1, 0), axis=1)
    inverse = 1.0 / counts.astype(F32)

    kb = width // n_mp
    ids = jnp.stack(
        [sec] + weights.offsets + [mp_index ^ k for k in range(n_mp)] + [jnp.int32(kb // 2)] * (n_mp == 4)
    ).astype(jnp.int32)
    chunks = 2
    usual = samp_dev * (rank // 2 + 1)
    height = max(round_up(-(-(prims + usual) // chunks), 16), round_up(prims + 8, 16))
    slots_here = chunks * height - prims

    place = mp_index * slots_here + jnp.arange(slots_here, dtype=jnp.int32)
    passed = ends[None, :] <= place[:, None]
    sample = jnp.sum(passed.astype(jnp.int32), axis=1)
    column = place - jnp.sum(jnp.where(passed, ranks[None, :], 0), axis=1)
    present = place < active
    belongs = (sample[:, None] == sample_line[None, :]) & present[:, None]
    source = ((sample // samp_dev) ^ mp_index) * piece_rows + (sample % samp_dev) * rank + column
    source = jnp.where(present, source, -1)
    source_p = ((sample_line // samp_dev) ^ mp_index) * piece_rows + samp_dev * rank + sample_line % samp_dev
    share = jnp.sum(jnp.where(belongs, inverse[None, :], 0.0), axis=1)
    share_p = jnp.where(sample_line // samp_dev == mp_index, inverse, 0.0)
    index = jnp.concatenate([source_p, source])[:, None]
    shares = jnp.concatenate([share_p, share])[:, None]
    onehot = belongs.astype(BF16)
    first = height - prims
    onehots = [onehot[:first], onehot[first:]]
    onehot_t = ((sample_line[:, None] == sample[None, :]) & present[None, :]).astype(BF16)
    onehots_t = [onehot_t[:, :first], onehot_t[:, first:]]
    share_of = [shares[:height], shares[height:]]

    packed = pick_rows([], ids, index, row_pieces, helper)
    if helper != 0:
        packed = hop(packed, helper, 0)
    rows = list(lift_rows(ids, packed, encoder, chunks))
    other_active = dp_swap(active.reshape(1, 1)).reshape(()) if n_dp > 1 else active
    most_active = jnp.maximum(active, other_active)

    small_arrays = [*onehots, *onehots_t, *share_of, index, most_active.reshape(1)]
    layer = weights.assemble(ids, small_arrays)
    token = []
    entered = [None] * chunks
    pres = [[None] * n_sec for _ in range(chunks)]
    tanhs = [None] * n_sec
    heads = [None] * chunks
    goal_pieces = None
    for level in range(n_sec):
        for c in range(chunks):
            got = fwd_stage(
                token, level, ids, layer, rows[c], onehots[c], None if c == 0 else tanhs[level], entered[c]
            )
            token = [got[0]]
            entered[c], pres[c][level] = got[2], got[1]
            if c == 0:
                tanhs[level] = got[3]
            rows[c] = got[0] if level == last else hop(got[0], level, level + 1)
            if level == last:
                heads[c] = head_stage(
                    token, last, ids, rows[c], wanted[c * height : (c + 1) * height], share_of[c], head_weight
                )
                token = [heads[c][1]]
        if goal_pieces is None:
            goal_pieces = plane_pieces(join_rows(token, targets, target_jac, piece_rows), last)
        if level == max(last - 1, 0):
            wanted = pick_rows(token, ids, index, goal_pieces, last)
            token = [wanted]

    small = n_dp * n_mp <= 8 and blk % 128 == 0
    cots = [heads[c][1] for c in range(chunks)]
    mixes = [None] * chunks
    backward_order = list(range(1, chunks)) + [0]
    hidden_pieces = head_pieces = None
    arrived = []
    for level in range(last, -1, -1):
        total = None
        for c in backward_order:
            got = bwd_stage(
                token, level, ids, layer, cots[c], pres[c][level], tanhs[level],
                onehots[c], onehots_t[c], total, c == 0, mixes[c],
            )
            mixes[c], total = got[0], got[1]
            token = [got[1]]
            if level > 0:
                cots[c] = hop(got[2], level, level - 1)
        if not small:
            continue
        if level == last:
            sends = pack_columns(token, ids, rows, [h[0] for h in heads], last, n_dp, n_mp, blk)
            token = [sends[0]]
            base = last * n_mp
            head_pieces = [sends[0]] + [
                lax.ppermute(sends[k], ("section", "mp"), [(base + m, base + (m ^ k)) for m in range(n_mp)])
                for k in range(1, n_mp)
            ]
        elif level == last - 1:
            sends = pack_columns(token, ids, entered, [], None, n_dp, n_mp, blk)
            token = [sends[0]]
            hidden_pieces = [sends[0]] + [mp_swap(sends[k], k) for k in range(1, n_mp)]
        elif level == last - 2:
            hidden_pieces = both_groups(hidden_pieces)
            token = [*token, *hidden_pieces]

    cols = out_width // n_sec
    if small:
        swapped = []
        for c in backward_order:
            swapped.append([mixes[c]] + [mp_swap(mixes[c], k) for k in range(1, n_mp)])
        first_mine, send, turned = first_gradient([], ids, hidden_pieces, swapped[0], blk, height)
        first_other = dp_swap(send)
        mine, send = head_partial([], ids, head_pieces, last, blk, height)
        other = dp_swap(send)
        blocks = head_gradient([], ids, mine, other, last, blk, n_sec)
        arrived = [hop(blocks[j], last, j) for j in range(last)]
        head_ext = blocks[last].astype(F32)
        for j in range(last):
            head_ext = jnp.where(sec == j, arrived[j].astype(F32), head_ext)
        head_mine = head_ext[:blk]
        loss_mine = (head_ext[blk, 0] + head_ext[blk + 1, 0]) / (n_dp * MB * out_width)
        grad = last_gradient([], turned, both_groups(swapped[1]), first_mine, first_other)
    else:
        contract = (((0,), (0,)), ((), ()))
        joined = jnp.concatenate(entered, axis=0)
        part = lax.dot_general(joined, jnp.concatenate(mixes, axis=0), contract, preferred_element_type=F32)
        grad = lax.psum_scatter(part.astype(BF16), ("dp", "mp"), scatter_dimension=0, tiled=True).astype(F32)
        cot_out = jnp.concatenate([h[0][:height] for h in heads], axis=0)
        part = lax.dot_general(jnp.concatenate(rows, axis=0), cot_out, contract, preferred_element_type=F32)
        head = lax.psum_scatter(part.astype(BF16), ("dp", "mp"), scatter_dimension=0, tiled=True)
        loss = sum(jnp.sum(h[0][height : height + 2, 0].astype(F32)) for h in heads)
        loss = jnp.where(sec == last, lax.psum(loss, ("dp", "mp")), 0.0).reshape(1, 1)
        head_mine = jnp.where(sec == last, head[:, last * cols :], jnp.zeros((blk, cols), BF16))
        loss_mine = loss
        for j in range(last):
            head_mine = head_mine + hop(head[:, j * cols : (j + 1) * cols], last, j)
            loss_mine = loss_mine + hop(loss, last, j)
        head_mine = head_mine.astype(F32)
        loss_mine = loss_mine.reshape(()) / (n_dp * MB * out_width)
    fast = (grad[None], head_mine, loss_mine)

    def plain():
        depth = rank + 1
        total_rows = samp_dev * depth
        layer_full = jnp.zeros((width, width), BF16)
        kb = weights.block_rows
        for array, block, which, base in weights.pieces:
            row = (mp_index ^ block) * kb + base
            row = row if which is None else row + weights.offsets[which]
            layer_full = lax.dynamic_update_slice_in_dim(layer_full, array, row, 0)
        rows_in = jnp.concatenate([inputs[:, None, :], tangents], axis=1).reshape(total_rows, in_width)
        start = jnp.dot(rows_in, encoder, preferred_element_type=F32).astype(BF16)
        chain = [(j, (j + 1) % n_sec) for j in range(n_sec)]

        def back_one(value):
            return lax.fori_loop(0, last, lambda _, v: lax.ppermute(v, "section", chain), value)

        def pre_of(rows):
            pre = jnp.dot(rows, layer_full, preferred_element_type=F32).reshape(samp_dev, depth, width)
            tanh_p = jnp.tanh(pre[:, 0])
            return pre, tanh_p, 1.0 - tanh_p * tanh_p

        def forward(level, state):
            rows, mine, _ = state
            mine = jnp.where(level == sec, rows, mine)
            pre, tanh_p, slope = pre_of(rows)
            change = jnp.concatenate([tanh_p[:, None], slope[:, None] * pre[:, 1:]], axis=1)
            new = (rows.astype(F32) + change.reshape(total_rows, width)).astype(BF16)
            return lax.ppermute(new, "section", chain), mine, new

        _, mine, final = lax.fori_loop(0, n_sec, forward, (start, start, start))
        own = lax.dynamic_slice_in_dim(inverse, mp_index * samp_dev, samp_dev, 0)
        row_weight = jnp.concatenate([jnp.ones((samp_dev, 1), F32), rank_mask.astype(F32)], axis=1)
        share = (row_weight * own[:, None]).reshape(total_rows, 1)
        outputs = jnp.dot(final, head_weight, preferred_element_type=F32)
        wanted = jnp.concatenate([targets[:, None, :], target_jac], axis=1).reshape(total_rows, out_width)
        mismatch = outputs - wanted.astype(F32)
        loss = jnp.sum(share * mismatch * mismatch)
        cot_out = (2.0 * share * mismatch).astype(BF16)
        cot = lax.dot_general(cot_out, head_weight, (((1,), (1,)), ((), ())), preferred_element_type=F32)
        pre, tanh_p, slope = pre_of(mine)

        def backward(step, state):
            cot, mix_mine = state
            up = cot.astype(F32).reshape(samp_dev, depth, width)
            side = jnp.sum(up[:, 1:] * pre[:, 1:], axis=1)
            lead = up[:, 0] * slope - 2.0 * side * tanh_p * slope
            mix = jnp.concatenate([lead[:, None], up[:, 1:] * slope[:, None]], axis=1)
            mix = mix.astype(BF16).reshape(total_rows, width)
            mix_mine = jnp.where(step == last - sec, mix, mix_mine)
            back = lax.dot_general(mix, layer_full, (((1,), (1,)), ((), ())), preferred_element_type=F32)
            new = (up.reshape(total_rows, width) + back).astype(BF16)
            return back_one(new), mix_mine

        _, mix = lax.fori_loop(0, n_sec, backward, (cot.astype(BF16), mine))

        def scatter(left, right):
            part = lax.dot_general(left, right, (((0,), (0,)), ((), ())), preferred_element_type=F32)
            part = part.astype(BF16).reshape(n_dp, n_mp, blk, right.shape[1])
            mine_part = jnp.zeros((n_dp, blk, right.shape[1]), F32)
            for k in range(n_mp):
                piece = lax.dynamic_index_in_dim(part, mp_index ^ k, 1, False)
                mine_part = mine_part + (piece if k == 0 else mp_swap(piece, k)).astype(F32)
            kept = lax.dynamic_index_in_dim(mine_part, dp_index, 0, False)
            if n_dp > 1:
                sent = lax.dynamic_index_in_dim(mine_part, 1 - dp_index, 0, False)
                kept = kept + dp_swap(sent.astype(BF16)).astype(F32)
            return kept

        grad = scatter(mine, mix)
        head = scatter(final, cot_out)
        cols = out_width // n_sec
        loss_group = sum(mp_pieces(loss.reshape(1, 1)))
        if n_dp > 1:
            loss_group = loss_group + dp_swap(loss_group)
        head_mine = jnp.where(sec == last, head[:, last * cols :], 0.0)
        loss_mine = jnp.where(sec == last, loss_group, 0.0)
        for j in range(last):
            block = jnp.concatenate([head[:, j * cols : (j + 1) * cols], jnp.broadcast_to(loss_group, (8, cols))])
            block = hop(block, last, j)
            head_mine = head_mine + block[:blk]
            loss_mine = loss_mine + block[blk:, :1][:1]
        return grad[None], head_mine, loss_mine.reshape(()) / (n_dp * MB * out_width)

    room = n_mp * slots_here
    if room >= n_mp * samp_dev * rank:
        return fast
    return lax.while_loop(
        lambda state: state[0] > room, lambda state: (jnp.int32(0), *plain()), (most_active, *fast)
    )[1:]


def solution(mesh):
    in_specs = (
        P(("dp", "mp"), None),
        P(("dp", "mp"), None, None),
        P(("dp", "mp"), None),
        P(("dp", "mp"), None, None),
        P(("dp", "mp"), None),
        P(("dp", "mp"), None),
        P(),
        P("section", "mp", None),
        P(),
    )
    out_specs = (P("section", ("dp", "mp"), None), P(("dp", "mp"), "section"), P())

    return jax.shard_map(local, mesh=mesh, in_specs=in_specs, out_specs=out_specs, check_vma=False)
```

```python
import jax
import jax.numpy as jnp
from jax import lax
from jax.experimental import pallas as pl
from jax.experimental.pallas import tpu as pltpu
from jax.sharding import PartitionSpec as P


F32 = jnp.float32
BF16 = jnp.bfloat16
MB = 6
EXTRA = 16
BLOCKS = 4

ANY = pl.BlockSpec(memory_space=pl.ANY)
SMEM = pl.BlockSpec(memory_space=pltpu.SMEM)
VMEM = pl.BlockSpec(memory_space=pltpu.VMEM)


def round_up(value, unit):
    return -(-value // unit) * unit


def mp_swap(value, flip):
    count = lax.axis_size("mp")
    return lax.ppermute(value, "mp", [(m, m ^ flip) for m in range(count)])


def dp_swap(value):
    count = lax.axis_size("dp")
    return lax.ppermute(value, "dp", [(d, d ^ 1) for d in range(count)])


def mp_pieces(value):
    return [value] + [mp_swap(value, k) for k in range(1, lax.axis_size("mp"))]


def hop(value, source, target):
    return lax.ppermute(value, "section", [(source, target)])


def plane_pieces(value, section):
    count = lax.axis_size("mp")
    base = section * count
    swaps = [[(base + m, base + (m ^ k)) for m in range(count)] for k in range(1, count)]
    return [value] + [lax.ppermute(value, ("section", "mp"), pairs) for pairs in swaps]


def params():
    return pltpu.CompilerParams(vmem_limit_bytes=16 * 2**20)


def call(body, args, specs, deps=(), **options):
    reads, waits = len(args), len(deps)

    def inner(*refs):
        body(*refs[:reads], *refs[reads + waits :])

    return pl.pallas_call(
        inner, in_specs=list(specs) + [ANY] * waits, compiler_params=params(), **options
    )(*args, *deps)


def run_copies(copies):
    for copy in copies:
        copy.start()
    for copy in copies:
        copy.wait()


def spread(onehot, value):
    high = value.astype(BF16)
    low = (value - high.astype(F32)).astype(BF16)
    return jnp.dot(onehot, high, preferred_element_type=F32) + jnp.dot(
        onehot, low, preferred_element_type=F32
    )


class Weights:
    def __init__(self, layer):
        self.count = lax.axis_size("mp")
        self.block_rows, self.width = layer.shape
        dp_index = lax.axis_index("dp")
        half = self.block_rows // 2
        self.offsets = [dp_index * half, (1 - dp_index) * half]
        self.pieces = [(layer, 0, None, 0)]
        self.colored = self.count == 4 and lax.axis_size("dp") == 2
        self.part = part = half // 2
        if self.colored:
            self.first = lax.dynamic_slice_in_dim(layer, dp_index * half, part, 0)
            self.second = lax.dynamic_slice_in_dim(layer, dp_index * half + part, part, 0)
            self.b1 = self.swap(self.second, 1)
            self.a2 = self.swap(self.first, 2)
            self.a1 = self.swap(self.first, 1)
            self.b2 = self.swap(self.second, 2)
            self.a3 = self.swap(self.a1, 2)
            self.b3 = self.swap(self.b2, 1)
            got = [(self.a1, 1, 0), (self.b2, 2, part), (self.b1, 1, part), (self.a2, 2, 0), (self.a3, 3, 0), (self.b3, 3, part)]
            for array, block, base in got:
                self.pieces.append((array, block, 0, base))
                self.pieces.append((dp_swap(array), block, 1, base))
        else:
            for block in range(1, self.count):
                self.pieces.append((mp_swap(layer, block), block, None, 0))

    def swap(self, array, flip):
        return mp_swap(array, flip)

    def assemble(self, ids, deps):
        early = len(self.pieces) - 4 if self.colored else len(self.pieces)
        layer = self.place(ids, None, self.pieces[:early], "assemble", deps)
        return layer if early == len(self.pieces) else self.place(ids, layer, self.pieces[early:], "complete", [])

    def place(self, ids, layer, pieces, name, deps):
        many = len(pieces)

        def body(ids_ref, *refs):
            out, sems = refs[-2:]
            copies = []
            for i, (array, block, which, base) in enumerate(pieces):
                row = pl.multiple_of(ids_ref[3 + block] * self.block_rows, self.block_rows) + base
                if which is not None:
                    row = row + pl.multiple_of(ids_ref[1 + which], self.block_rows // 2)
                copies.append(
                    pltpu.make_async_copy(refs[i], out.at[pl.ds(row, array.shape[0]), :], sems.at[i])
                )
            run_copies(copies)

        before = [] if layer is None else [layer]
        return call(
            body,
            [ids, *[piece[0] for piece in pieces], *before],
            [SMEM] + [ANY] * many + [VMEM] * len(before),
            deps,
            out_shape=jax.ShapeDtypeStruct((self.count * self.block_rows, self.width), BF16),
            out_specs=VMEM,
            input_output_aliases={1 + many: 0} if before else {},
            scratch_shapes=[pltpu.SemaphoreType.DMA((many,))],
            name=name,
        )


def fwd_stage(deps, level, ids, layer, rows, onehot, slope, kept):
    height, width = rows.shape
    prims = onehot.shape[1]
    leads = slope is None
    nb = width // BLOCKS

    def body(ids_ref, layer_ref, rows_ref, onehot_ref, *rest):
        if not leads:
            slope_ref, *rest = rest
        next_ref, pre_ref, kept_ref, *rest = rest[(kept is not None) :]
        if leads:
            tanh_ref, *rest = rest
        (kept_sem,) = rest

        @pl.when(ids_ref[0] == level)
        def _():
            keep = pltpu.make_async_copy(rows_ref, kept_ref, kept_sem)
            keep.start()

            def block(n, carry):
                cols = pl.ds(pl.multiple_of(n * nb, nb), nb)
                acc = jnp.dot(rows_ref[...], layer_ref[:, cols], preferred_element_type=F32)
                old = rows_ref[:, cols].astype(F32)
                pre_ref[:, cols] = acc.astype(BF16)
                if leads:
                    tanh_p = jnp.tanh(acc[:prims])
                    tanh_ref[:, cols] = tanh_p
                    factor = spread(onehot_ref[...], 1.0 - tanh_p * tanh_p)
                    new = jnp.concatenate(
                        [old[:prims] + tanh_p, old[prims:] + factor * acc[prims:]], axis=0
                    )
                else:
                    tanh_p = slope_ref[:, cols]
                    new = old + spread(onehot_ref[...], 1.0 - tanh_p * tanh_p) * acc
                next_ref[:, cols] = new.astype(BF16)
                return carry

            lax.fori_loop(0, BLOCKS, block, 0)
            keep.wait()

    outs = [jax.ShapeDtypeStruct((height, width), BF16)] * 3
    if leads:
        outs.append(jax.ShapeDtypeStruct((prims, width), F32))
    args = [ids, layer, rows, onehot] + ([] if leads else [slope])
    specs = [SMEM] + [VMEM] * (len(args) - 1)
    alias = {}
    if kept is not None:
        alias = {len(args): 2}
        args.append(kept)
        specs.append(ANY)
    return call(
        body,
        args,
        specs,
        deps,
        out_shape=outs,
        out_specs=[VMEM, VMEM, ANY] + [VMEM] * (len(outs) - 3),
        input_output_aliases=alias,
        scratch_shapes=[pltpu.SemaphoreType.DMA],
        cost_estimate=pl.CostEstimate(flops=2 * height * width * width * 4, bytes_accessed=2 * width * width, transcendentals=0),
        name=f"fwd{level}",
    )


def bwd_stage(deps, level, ids, layer, cot, pre, tanh_p, onehot, onehot_t, total, leads, kept):
    height, width = cot.shape
    prims = tanh_p.shape[0]
    deep = level > 0
    nb = width // BLOCKS

    def body(ids_ref, cot_ref, pre_ref, tanh_ref, onehot_ref, onehot_t_ref, *rest):
        if total is not None:
            total_ref, *rest = rest
        if deep:
            layer_ref, *rest = rest
        kept_ref, side_ref, *rest = rest[(kept is not None) :]
        if deep:
            new_ref, *rest = rest
        mix_ref, kept_sem = rest

        @pl.when(ids_ref[0] == level)
        def _():
            skip = prims if leads else 0

            def block(n, carry):
                cols = pl.ds(pl.multiple_of(n * nb, nb), nb)
                up = cot_ref[:, cols].astype(F32)
                tanh = tanh_ref[:, cols]
                slope = 1.0 - tanh * tanh
                up_t = up[skip:]
                mix_t = up_t * spread(onehot_ref[...], slope)
                total_here = spread(onehot_t_ref[...], up_t * pre_ref[:, cols].astype(F32)[skip:])
                if total is not None:
                    total_here = total_here + total_ref[:, cols]
                if leads:
                    mix_p = up[:prims] * slope - 2.0 * total_here * tanh * slope
                    mix_ref[:, cols] = jnp.concatenate([mix_p, mix_t], axis=0).astype(BF16)
                else:
                    mix_ref[:, cols] = mix_t.astype(BF16)
                side_ref[:, cols] = total_here
                return carry

            lax.fori_loop(0, BLOCKS, block, 0)
            keep = pltpu.make_async_copy(mix_ref, kept_ref, kept_sem)
            keep.start()
            if deep:

                def back_block(n, carry):
                    cols = pl.ds(pl.multiple_of(n * nb, nb), nb)
                    back = lax.dot_general(
                        mix_ref[...], layer_ref[cols, :], (((1,), (1,)), ((), ())), preferred_element_type=F32
                    )
                    new_ref[:, cols] = (cot_ref[:, cols].astype(F32) + back).astype(BF16)
                    return carry

                lax.fori_loop(0, BLOCKS, back_block, 0)
            keep.wait()

    rows_shape = jax.ShapeDtypeStruct((height, width), BF16)
    outs = [rows_shape, jax.ShapeDtypeStruct((prims, width), F32)] + ([rows_shape] if deep else [])
    args = [ids, cot, pre, tanh_p, onehot, onehot_t] + ([] if total is None else [total])
    args += [layer] if deep else []
    specs = [SMEM] + [VMEM] * (len(args) - 1)
    alias = {}
    if kept is not None:
        alias = {len(args): 0}
        args.append(kept)
        specs.append(ANY)
    return call(
        body,
        args,
        specs,
        deps,
        out_shape=outs,
        out_specs=[ANY] + [VMEM] * (len(outs) - 1),
        input_output_aliases=alias,
        scratch_shapes=[pltpu.VMEM((height, width), BF16), pltpu.SemaphoreType.DMA],
        cost_estimate=pl.CostEstimate(flops=2 * height * width * width * 4, bytes_accessed=2 * width * width, transcendentals=0),
        name=f"bwd{level}",
    )


def pick_rows(deps, ids, index, pieces, level):
    height = index.shape[0]
    piece_rows, width = pieces[0].shape

    def body(ids_ref, index_ref, *rest):
        out_ref = rest[-1]

        @pl.when(ids_ref[0] == level)
        def _():
            index_here = index_ref[...]
            acc = jnp.zeros((height, width), F32)
            for k, piece_ref in enumerate(rest[:-1]):
                place = lax.broadcasted_iota(jnp.int32, (height, piece_rows), 1) + k * piece_rows
                onehot = jnp.where(place == index_here, 1.0, 0.0).astype(BF16)
                acc = acc + jnp.dot(onehot, piece_ref[...], preferred_element_type=F32)
            out_ref[...] = acc.astype(BF16)

    return call(
        body,
        [ids, index, *pieces],
        [SMEM] + [VMEM] * (1 + len(pieces)),
        deps,
        out_shape=jax.ShapeDtypeStruct((height, width), BF16),
        out_specs=VMEM,
        name="pick",
    )


def lift_rows(ids, rows, encoder, chunks):
    height = rows.shape[0] // chunks
    width = encoder.shape[1]

    def body(ids_ref, rows_ref, encoder_ref, *outs):
        @pl.when(ids_ref[0] == 0)
        def _():
            for c, out in enumerate(outs):
                part = rows_ref[c * height : (c + 1) * height, :]
                out[...] = jnp.dot(part, encoder_ref[...], preferred_element_type=F32).astype(BF16)

    return pl.pallas_call(
        body,
        out_shape=[jax.ShapeDtypeStruct((height, width), BF16)] * chunks,
        in_specs=[SMEM, VMEM, VMEM],
        out_specs=[VMEM] * chunks,
        compiler_params=params(),
        name="lift",
    )(ids, rows, encoder)


def pack_columns(deps, ids, chunks, tails, level, n_dp, n_mp, blk):
    count = len(chunks)
    height, _ = chunks[0].shape
    tail_width = tails[0].shape[1] if tails else 0
    core = n_dp * blk
    end = count * height

    def body(ids_ref, *refs):
        chunk_refs, rest = refs[:count], refs[count:]
        tail_refs, outs = rest[: len(tails)], rest[len(tails) :]

        def fill():
            for k, out in enumerate(outs):
                for c, chunk_ref in enumerate(chunk_refs):
                    first = c * height
                    for d in range(n_dp):
                        col = pl.multiple_of((ids_ref[3 + k] + d * n_mp) * blk, blk)
                        out[first : first + height, d * blk : (d + 1) * blk] = chunk_ref[:, pl.ds(col, blk)]
                    if tails:
                        out[first : first + height, core:] = tail_refs[c][:height, :]
                if tails:
                    sums = [ref[height:, :].astype(F32)[: EXTRA // 2] for ref in tail_refs]
                    out[end:, :core] = jnp.zeros((EXTRA, core), BF16)
                    out[end:, core:] = jnp.concatenate(sums, axis=0).astype(BF16)

        if level is None:
            fill()
        else:
            pl.when(ids_ref[0] == level)(fill)

    shape = jax.ShapeDtypeStruct((end + (EXTRA if tails else 0), core + tail_width), BF16)
    return call(
        body,
        [ids, *chunks, *tails],
        [SMEM] + [VMEM] * (count + len(tails)),
        deps,
        out_shape=[shape] * n_mp,
        out_specs=[VMEM] * n_mp,
        name="pack",
    )


def both_groups(pieces):
    return pieces + ([dp_swap(piece) for piece in pieces] if lax.axis_size("dp") > 1 else [])


def loss_rows(loss, cols):
    high = loss.astype(BF16).astype(F32)
    line = lax.broadcasted_iota(jnp.int32, (EXTRA, cols), 0)
    return jnp.where(line == 0, high, jnp.where(line == 1, loss - high, 0.0))


def head_partial(deps, ids, pieces, level, blk):
    rows_each, wide = pieces[0].shape
    core = 2 * blk
    out_width = wide - core
    many = len(pieces)

    def body(ids_ref, *refs):
        piece_refs, (mine_ref, send_ref, left, right, sems) = refs[:many], refs[many:]

        @pl.when(ids_ref[0] == level)
        def _():
            here = pl.multiple_of(ids_ref[1] // ids_ref[7] * blk, blk)
            there = pl.multiple_of(blk - here, blk)
            copies = []
            for i, ref in enumerate(piece_refs):
                rows = pl.ds(i * rows_each, rows_each)
                copies.append(pltpu.make_async_copy(ref.at[:, pl.ds(here, blk)], left.at[rows, :blk], sems.at[0, i]))
                copies.append(pltpu.make_async_copy(ref.at[:, pl.ds(there, blk)], left.at[rows, blk:], sems.at[1, i]))
                copies.append(pltpu.make_async_copy(ref.at[:, core:], right.at[rows], sems.at[2, i]))
            run_copies(copies)
            loss = jnp.zeros((1, 128), F32)
            for piece in range(1, many + 1):
                tail = right[piece * rows_each - EXTRA : piece * rows_each, :128].astype(F32)
                loss = loss + tail[0:1] + tail[1:2] + tail[EXTRA // 2 : EXTRA // 2 + 1] + tail[EXTRA // 2 + 1 : EXTRA // 2 + 2]
            tail = loss_rows(loss[:, :1], out_width)
            part = lax.dot_general(left[...], right[...], (((0,), (0,)), ((), ())), preferred_element_type=F32)
            mine_ref[:blk, :] = part[:blk]
            mine_ref[blk:, :] = tail
            send_ref[:blk, :] = part[blk:].astype(BF16)
            send_ref[blk:, :] = tail.astype(BF16)

    shape = (blk + EXTRA, out_width)
    return call(
        body,
        [ids, *pieces],
        [SMEM] + [ANY] * many,
        deps,
        out_shape=[jax.ShapeDtypeStruct(shape, F32), jax.ShapeDtypeStruct(shape, BF16)],
        out_specs=[VMEM] * 2,
        scratch_shapes=[
            pltpu.VMEM((many * rows_each, core), BF16),
            pltpu.VMEM((many * rows_each, out_width), BF16),
            pltpu.SemaphoreType.DMA((3, many)),
        ],
        name="head_partial",
    )


def head_gradient(deps, ids, mine, other, level, blk, n_sec):
    cols = mine.shape[1] // n_sec

    def body(ids_ref, mine_ref, other_ref, *outs):
        @pl.when(ids_ref[0] == level)
        def _():
            tails = mine_ref[blk:, :1] + other_ref[blk:, :128].astype(F32)[:, :1]
            tail = loss_rows(tails[0:1] + tails[1:2], cols).astype(BF16)
            for j, out in enumerate(outs):
                span = slice(j * cols, (j + 1) * cols)
                out[:blk, :] = (mine_ref[:blk, span] + other_ref[:blk, span].astype(F32)).astype(BF16)
                out[blk:, :] = tail

    return call(
        body,
        [ids, mine, other],
        [SMEM, VMEM, VMEM],
        deps,
        out_shape=[jax.ShapeDtypeStruct((blk + EXTRA, cols), BF16)] * n_sec,
        out_specs=[VMEM] * n_sec,
        name="grad_head",
    )


def first_gradient(deps, ids, blocks, mixes, blk, height):
    many = len(mixes)
    every = len(blocks)
    width = mixes[0].shape[1]
    nb = width // BLOCKS

    def body(ids_ref, *refs):
        block_refs, mix_refs = refs[:every], refs[every : every + many]
        mine_ref, send_ref, later_ref, left, right, early, sems = refs[every + many :]
        here = pl.multiple_of(ids_ref[1] // ids_ref[7] * blk, blk)
        there = pl.multiple_of(blk - here, blk)
        copies = []
        for i in range(every):
            rows = pl.ds(i * height, height)
            if i < many:
                for j, col in enumerate([here, there]):
                    src = block_refs[i].at[height:, pl.ds(col, blk)]
                    copies.append(pltpu.make_async_copy(src, left.at[rows, j * blk : (j + 1) * blk], sems.at[j, i]))
                copies.append(pltpu.make_async_copy(mix_refs[i], right.at[rows], sems.at[2, i]))
            src = block_refs[i].at[:height, pl.ds(here, blk)]
            copies.append(pltpu.make_async_copy(src, early.at[rows], sems.at[3, i]))
        run_copies(copies)
        later_ref[...] = early[...].astype(F32).T.astype(BF16)
        turned = left[...].astype(F32).T.astype(BF16)
        for n in range(BLOCKS):
            cols = slice(n * nb, (n + 1) * nb)
            part = jnp.dot(turned, right[:, cols], preferred_element_type=F32)
            mine_ref[:, cols] = part[:blk]
            send_ref[:, cols] = part[blk:].astype(BF16)

    return call(
        body,
        [ids, *blocks, *mixes],
        [SMEM] + [ANY] * (every + many),
        deps,
        out_shape=[
            jax.ShapeDtypeStruct((blk, width), F32),
            jax.ShapeDtypeStruct((blk, width), BF16),
            jax.ShapeDtypeStruct((blk, every * height), BF16),
        ],
        out_specs=[VMEM] * 3,
        scratch_shapes=[
            pltpu.VMEM((many * height, 2 * blk), BF16),
            pltpu.VMEM((many * height, width), BF16),
            pltpu.VMEM((every * height, blk), BF16),
            pltpu.SemaphoreType.DMA((4, every)),
        ],
        name="first_gradient",
    )


def last_gradient(deps, turned, mixes, mine, other):
    blk, width = mine.shape
    nb = width // BLOCKS

    def body(turned_ref, *refs):
        mix_refs, (mine_ref, other_ref, out) = refs[:-3], refs[-3:]
        for n in range(BLOCKS):
            cols = slice(n * nb, (n + 1) * nb)
            right = jnp.concatenate([ref[:, cols] for ref in mix_refs], axis=0)
            part = jnp.dot(turned_ref[...], right, preferred_element_type=F32)
            out[:, cols] = part + mine_ref[:, cols] + other_ref[:, cols].astype(F32)

    return call(
        body,
        [turned, *mixes, mine, other],
        [VMEM] * (3 + len(mixes)),
        deps,
        out_shape=jax.ShapeDtypeStruct((blk, width), F32),
        out_specs=VMEM,
        name="last_gradient",
    )


def join_rows(deps, flat, deep, rows_out):
    count, rank, width = deep.shape

    def body(flat_ref, deep_ref, out, sem):
        copies = [
            pltpu.make_async_copy(deep_ref.at[i], out.at[i * rank : (i + 1) * rank], sem.at[i])
            for i in range(count)
        ]
        for copy in copies:
            copy.start()
        spare = jnp.zeros((rows_out - count * (rank + 1), width), F32)
        out[count * rank :, :] = jnp.concatenate([flat_ref[...].astype(F32), spare], axis=0).astype(BF16)
        for copy in copies:
            copy.wait()

    return call(
        body,
        [flat, deep],
        [VMEM, ANY],
        deps,
        out_shape=jax.ShapeDtypeStruct((rows_out, width), BF16),
        out_specs=VMEM,
        scratch_shapes=[pltpu.SemaphoreType.DMA((count,))],
        name="join",
    )


def head_stage(deps, level, ids, rows, wanted, share, head_weight):
    height, width = rows.shape
    out_width = head_weight.shape[1]

    def body(ids_ref, rows_ref, wanted_ref, share_ref, head_ref, cot_ref, new_ref):
        @pl.when(ids_ref[0] == level)
        def _():
            nb = out_width // BLOCKS

            def block(n, loss):
                cols = pl.ds(pl.multiple_of(n * nb, nb), nb)
                outputs = jnp.dot(rows_ref[...], head_ref[:, cols], preferred_element_type=F32)
                mismatch = outputs - wanted_ref[:, cols].astype(F32)
                scaled = share_ref[...] * mismatch
                cot_ref[:height, cols] = (2.0 * scaled).astype(BF16)
                return loss + jnp.sum(scaled * mismatch, axis=1, keepdims=True)

            loss = lax.fori_loop(0, BLOCKS, block, jnp.zeros((height, 1), F32))
            loss = jnp.sum(loss, axis=0, keepdims=True)
            line = lax.broadcasted_iota(jnp.int32, (EXTRA, out_width), 0)
            high = loss.astype(BF16).astype(F32)
            tail = jnp.where(line == 0, high, jnp.where(line == 1, loss - high, 0.0))
            cot_ref[height:, :] = tail.astype(BF16)
            kb = width // BLOCKS

            def back_block(k, carry):
                cols = pl.ds(pl.multiple_of(k * kb, kb), kb)
                new_ref[:, cols] = lax.dot_general(
                    cot_ref[:height, :], head_ref[cols, :], (((1,), (1,)), ((), ())), preferred_element_type=F32
                ).astype(BF16)
                return carry

            lax.fori_loop(0, BLOCKS, back_block, 0)

    return call(
        body,
        [ids, rows, wanted, share, head_weight],
        [SMEM] + [VMEM] * 4,
        deps,
        out_shape=[
            jax.ShapeDtypeStruct((height + EXTRA, out_width), BF16),
            jax.ShapeDtypeStruct((height, width), BF16),
        ],
        out_specs=[VMEM] * 2,
        cost_estimate=pl.CostEstimate(flops=2 * height * width * width * 4, bytes_accessed=2 * width * out_width, transcendentals=0),
        name="head",
    )


def local(
    inputs, tangents, targets, target_jac, rank_mask, batch_order, encoder, layers, head_weight
):
    samp_dev, rank = rank_mask.shape
    in_width = inputs.shape[1]
    width = layers.shape[2]
    out_width = head_weight.shape[1]
    n_dp = lax.axis_size("dp")
    n_mp = lax.axis_size("mp")
    n_sec = lax.axis_size("section")
    last = n_sec - 1
    dp_index = lax.axis_index("dp")
    sec = lax.axis_index("section")
    mp_index = lax.axis_index("mp")
    prims = n_mp * samp_dev
    blk = width // (n_dp * n_mp)

    weights = Weights(layers[0])
    helper = last

    piece_rows = round_up(samp_dev * (rank + 1), 16)
    joined_rows = join_rows([], inputs, tangents, piece_rows)
    row_pieces = plane_pieces(joined_rows, helper)

    own_rank = jnp.sum(rank_mask, axis=1)
    slot_line = jnp.arange(samp_dev, dtype=jnp.int32)
    own_slot = jnp.sum(
        jnp.where(batch_order[0][None, :] == slot_line[:, None], slot_line[None, :], 0), axis=1
    ) // (samp_dev // MB)
    own_meta = jnp.stack([own_rank, own_slot]).astype(jnp.int32)
    meta_pieces = jnp.stack(mp_pieces(own_meta))
    order_line = jnp.arange(n_mp, dtype=jnp.int32)
    swap = ((order_line[:, None] ^ mp_index) == order_line[None, :]).astype(jnp.int32)
    meta = jnp.sum(swap[:, :, None, None] * meta_pieces[None], axis=1)
    ranks = meta[:, 0].reshape(prims)
    slots = meta[:, 1].reshape(prims)
    sample_line = jnp.arange(prims, dtype=jnp.int32)
    ends = jnp.sum(jnp.where(sample_line[None, :] <= sample_line[:, None], ranks[None, :], 0), axis=1)
    active = jnp.sum(ranks)
    counts = jnp.sum(jnp.where(slots[None, :] == slots[:, None], ranks[None, :] + 1, 0), axis=1)
    inverse = 1.0 / counts.astype(F32)

    kb = width // n_mp
    ids = jnp.stack(
        [sec] + weights.offsets + [mp_index ^ k for k in range(n_mp)] + [jnp.int32(kb // 2)] * (n_mp == 4)
    ).astype(jnp.int32)
    chunks = 2
    usual = samp_dev * (rank // 2 + 1)
    height = max(round_up(-(-(prims + usual) // chunks), 16), round_up(prims + 8, 16))
    slots_here = chunks * height - prims

    place = mp_index * slots_here + jnp.arange(slots_here, dtype=jnp.int32)
    passed = ends[None, :] <= place[:, None]
    sample = jnp.sum(passed.astype(jnp.int32), axis=1)
    column = place - jnp.sum(jnp.where(passed, ranks[None, :], 0), axis=1)
    present = place < active
    belongs = (sample[:, None] == sample_line[None, :]) & present[:, None]
    source = ((sample // samp_dev) ^ mp_index) * piece_rows + (sample % samp_dev) * rank + column
    source = jnp.where(present, source, -1)
    source_p = ((sample_line // samp_dev) ^ mp_index) * piece_rows + samp_dev * rank + sample_line % samp_dev
    share = jnp.sum(jnp.where(belongs, inverse[None, :], 0.0), axis=1)
    share_p = jnp.where(sample_line // samp_dev == mp_index, inverse, 0.0)
    index = jnp.concatenate([source_p, source])[:, None]
    shares = jnp.concatenate([share_p, share])[:, None]
    onehot = belongs.astype(BF16)
    first = height - prims
    onehots = [onehot[:first], onehot[first:]]
    onehot_t = ((sample_line[:, None] == sample[None, :]) & present[None, :]).astype(BF16)
    onehots_t = [onehot_t[:, :first], onehot_t[:, first:]]
    share_of = [shares[:height], shares[height:]]

    packed = pick_rows([], ids, index, row_pieces, helper)
    if helper != 0:
        packed = hop(packed, helper, 0)
    rows = list(lift_rows(ids, packed, encoder, chunks))
    other_active = dp_swap(active.reshape(1, 1)).reshape(()) if n_dp > 1 else active
    most_active = jnp.maximum(active, other_active)

    small_arrays = [*onehots, *onehots_t, *share_of, index, most_active.reshape(1)]
    layer = weights.assemble(ids, small_arrays)
    token = []
    entered = [None] * chunks
    pres = [[None] * n_sec for _ in range(chunks)]
    tanhs = [None] * n_sec
    heads = [None] * chunks
    goal_pieces = None
    for level in range(n_sec):
        for c in range(chunks):
            got = fwd_stage(
                token, level, ids, layer, rows[c], onehots[c], None if c == 0 else tanhs[level], entered[c]
            )
            token = [got[0]]
            entered[c], pres[c][level] = got[2], got[1]
            if c == 0:
                tanhs[level] = got[3]
            rows[c] = got[0] if level == last else hop(got[0], level, level + 1)
            if level == last:
                heads[c] = head_stage(
                    token, last, ids, rows[c], wanted[c * height : (c + 1) * height], share_of[c], head_weight
                )
                token = [heads[c][1]]
        if goal_pieces is None:
            goal_pieces = plane_pieces(join_rows(token, targets, target_jac, piece_rows), last)
        if level == max(last - 1, 0):
            wanted = pick_rows(token, ids, index, goal_pieces, last)
            token = [wanted]

    small = n_dp * n_mp <= 8 and blk % 128 == 0
    cots = [heads[c][1] for c in range(chunks)]
    mixes = [None] * chunks
    backward_order = list(range(1, chunks)) + [0]
    hidden_pieces = head_pieces = None
    arrived = []
    for level in range(last, -1, -1):
        total = None
        for c in backward_order:
            got = bwd_stage(
                token, level, ids, layer, cots[c], pres[c][level], tanhs[level],
                onehots[c], onehots_t[c], total, c == 0, mixes[c],
            )
            mixes[c], total = got[0], got[1]
            token = [got[1]]
            if level > 0:
                cots[c] = hop(got[2], level, level - 1)
        if not small:
            continue
        if level == last:
            sends = pack_columns(token, ids, rows, [h[0] for h in heads], last, n_dp, n_mp, blk)
            token = [sends[0]]
            base = last * n_mp
            head_pieces = [sends[0]] + [
                lax.ppermute(sends[k], ("section", "mp"), [(base + m, base + (m ^ k)) for m in range(n_mp)])
                for k in range(1, n_mp)
            ]
        elif level == last - 1:
            sends = pack_columns(token, ids, entered, [], None, n_dp, n_mp, blk)
            token = [sends[0]]
            hidden_pieces = [sends[0]] + [mp_swap(sends[k], k) for k in range(1, n_mp)]

    cols = out_width // n_sec
    if small:
        swapped = []
        for c in backward_order:
            swapped.append([mixes[c]] + [mp_swap(mixes[c], k) for k in range(1, n_mp)])
        hidden_pieces = both_groups(hidden_pieces)
        first_mine, send, turned = first_gradient([], ids, hidden_pieces, swapped[0], blk, height)
        first_other = dp_swap(send)
        mine, send = head_partial([], ids, head_pieces, last, blk)
        other = dp_swap(send)
        blocks = head_gradient([], ids, mine, other, last, blk, n_sec)
        arrived = [hop(blocks[j], last, j) for j in range(last)]
        head_ext = blocks[last].astype(F32)
        for j in range(last):
            head_ext = jnp.where(sec == j, arrived[j].astype(F32), head_ext)
        head_mine = head_ext[:blk]
        loss_mine = (head_ext[blk, 0] + head_ext[blk + 1, 0]) / (n_dp * MB * out_width)
        grad = last_gradient([], turned, both_groups(swapped[1]), first_mine, first_other)
    else:
        contract = (((0,), (0,)), ((), ()))
        joined = jnp.concatenate(entered, axis=0)
        part = lax.dot_general(joined, jnp.concatenate(mixes, axis=0), contract, preferred_element_type=F32)
        grad = lax.psum_scatter(part.astype(BF16), ("dp", "mp"), scatter_dimension=0, tiled=True).astype(F32)
        cot_out = jnp.concatenate([h[0][:height] for h in heads], axis=0)
        part = lax.dot_general(jnp.concatenate(rows, axis=0), cot_out, contract, preferred_element_type=F32)
        head = lax.psum_scatter(part.astype(BF16), ("dp", "mp"), scatter_dimension=0, tiled=True)
        loss = sum(jnp.sum(h[0][height : height + 2, 0].astype(F32)) for h in heads)
        loss = jnp.where(sec == last, lax.psum(loss, ("dp", "mp")), 0.0).reshape(1, 1)
        head_mine = jnp.where(sec == last, head[:, last * cols :], jnp.zeros((blk, cols), BF16))
        loss_mine = loss
        for j in range(last):
            head_mine = head_mine + hop(head[:, j * cols : (j + 1) * cols], last, j)
            loss_mine = loss_mine + hop(loss, last, j)
        head_mine = head_mine.astype(F32)
        loss_mine = loss_mine.reshape(()) / (n_dp * MB * out_width)
    fast = (grad[None], head_mine, loss_mine)

    def plain():
        depth = rank + 1
        total_rows = samp_dev * depth
        layer_full = jnp.zeros((width, width), BF16)
        kb = weights.block_rows
        for array, block, which, base in weights.pieces:
            row = (mp_index ^ block) * kb + base
            row = row if which is None else row + weights.offsets[which]
            layer_full = lax.dynamic_update_slice_in_dim(layer_full, array, row, 0)
        rows_in = jnp.concatenate([inputs[:, None, :], tangents], axis=1).reshape(total_rows, in_width)
        start = jnp.dot(rows_in, encoder, preferred_element_type=F32).astype(BF16)
        chain = [(j, (j + 1) % n_sec) for j in range(n_sec)]

        def back_one(value):
            return lax.fori_loop(0, last, lambda _, v: lax.ppermute(v, "section", chain), value)

        def pre_of(rows):
            pre = jnp.dot(rows, layer_full, preferred_element_type=F32).reshape(samp_dev, depth, width)
            tanh_p = jnp.tanh(pre[:, 0])
            return pre, tanh_p, 1.0 - tanh_p * tanh_p

        def forward(level, state):
            rows, mine, _ = state
            mine = jnp.where(level == sec, rows, mine)
            pre, tanh_p, slope = pre_of(rows)
            change = jnp.concatenate([tanh_p[:, None], slope[:, None] * pre[:, 1:]], axis=1)
            new = (rows.astype(F32) + change.reshape(total_rows, width)).astype(BF16)
            return lax.ppermute(new, "section", chain), mine, new

        _, mine, final = lax.fori_loop(0, n_sec, forward, (start, start, start))
        own = lax.dynamic_slice_in_dim(inverse, mp_index * samp_dev, samp_dev, 0)
        row_weight = jnp.concatenate([jnp.ones((samp_dev, 1), F32), rank_mask.astype(F32)], axis=1)
        share = (row_weight * own[:, None]).reshape(total_rows, 1)
        outputs = jnp.dot(final, head_weight, preferred_element_type=F32)
        wanted = jnp.concatenate([targets[:, None, :], target_jac], axis=1).reshape(total_rows, out_width)
        mismatch = outputs - wanted.astype(F32)
        loss = jnp.sum(share * mismatch * mismatch)
        cot_out = (2.0 * share * mismatch).astype(BF16)
        cot = lax.dot_general(cot_out, head_weight, (((1,), (1,)), ((), ())), preferred_element_type=F32)
        pre, tanh_p, slope = pre_of(mine)

        def backward(step, state):
            cot, mix_mine = state
            up = cot.astype(F32).reshape(samp_dev, depth, width)
            side = jnp.sum(up[:, 1:] * pre[:, 1:], axis=1)
            lead = up[:, 0] * slope - 2.0 * side * tanh_p * slope
            mix = jnp.concatenate([lead[:, None], up[:, 1:] * slope[:, None]], axis=1)
            mix = mix.astype(BF16).reshape(total_rows, width)
            mix_mine = jnp.where(step == last - sec, mix, mix_mine)
            back = lax.dot_general(mix, layer_full, (((1,), (1,)), ((), ())), preferred_element_type=F32)
            new = (up.reshape(total_rows, width) + back).astype(BF16)
            return back_one(new), mix_mine

        _, mix = lax.fori_loop(0, n_sec, backward, (cot.astype(BF16), mine))

        def scatter(left, right):
            part = lax.dot_general(left, right, (((0,), (0,)), ((), ())), preferred_element_type=F32)
            part = part.astype(BF16).reshape(n_dp, n_mp, blk, right.shape[1])
            mine_part = jnp.zeros((n_dp, blk, right.shape[1]), F32)
            for k in range(n_mp):
                piece = lax.dynamic_index_in_dim(part, mp_index ^ k, 1, False)
                mine_part = mine_part + (piece if k == 0 else mp_swap(piece, k)).astype(F32)
            kept = lax.dynamic_index_in_dim(mine_part, dp_index, 0, False)
            if n_dp > 1:
                sent = lax.dynamic_index_in_dim(mine_part, 1 - dp_index, 0, False)
                kept = kept + dp_swap(sent.astype(BF16)).astype(F32)
            return kept

        grad = scatter(mine, mix)
        head = scatter(final, cot_out)
        cols = out_width // n_sec
        loss_group = sum(mp_pieces(loss.reshape(1, 1)))
        if n_dp > 1:
            loss_group = loss_group + dp_swap(loss_group)
        head_mine = jnp.where(sec == last, head[:, last * cols :], 0.0)
        loss_mine = jnp.where(sec == last, loss_group, 0.0)
        for j in range(last):
            block = jnp.concatenate([head[:, j * cols : (j + 1) * cols], jnp.broadcast_to(loss_group, (8, cols))])
            block = hop(block, last, j)
            head_mine = head_mine + block[:blk]
            loss_mine = loss_mine + block[blk:, :1][:1]
        return grad[None], head_mine, loss_mine.reshape(()) / (n_dp * MB * out_width)

    room = n_mp * slots_here
    if room >= n_mp * samp_dev * rank:
        return fast
    return lax.while_loop(
        lambda state: state[0] > room, lambda state: (jnp.int32(0), *plain()), (most_active, *fast)
    )[1:]


def solution(mesh):
    in_specs = (
        P(("dp", "mp"), None),
        P(("dp", "mp"), None, None),
        P(("dp", "mp"), None),
        P(("dp", "mp"), None, None),
        P(("dp", "mp"), None),
        P(("dp", "mp"), None),
        P(),
        P("section", "mp", None),
        P(),
    )
    out_specs = (P("section", ("dp", "mp"), None), P(("dp", "mp"), "section"), P())

    return jax.shard_map(local, mesh=mesh, in_specs=in_specs, out_specs=out_specs, check_vma=False)
```

```python
import jax
import jax.numpy as jnp
from jax import lax
from jax.experimental import pallas as pl
from jax.experimental.pallas import tpu as pltpu
from jax.sharding import PartitionSpec as P


F32 = jnp.float32
BF16 = jnp.bfloat16
MB = 6
EXTRA = 16
BLOCKS = 4

ANY = pl.BlockSpec(memory_space=pl.ANY)
SMEM = pl.BlockSpec(memory_space=pltpu.SMEM)
VMEM = pl.BlockSpec(memory_space=pltpu.VMEM)


def round_up(value, unit):
    return -(-value // unit) * unit


def mp_swap(value, flip):
    count = lax.axis_size("mp")
    return lax.ppermute(value, "mp", [(m, m ^ flip) for m in range(count)])


def dp_swap(value):
    count = lax.axis_size("dp")
    return lax.ppermute(value, "dp", [(d, d ^ 1) for d in range(count)])


def mp_pieces(value):
    return [value] + [mp_swap(value, k) for k in range(1, lax.axis_size("mp"))]


def hop(value, source, target):
    return lax.ppermute(value, "section", [(source, target)])


def plane_pieces(value, section):
    count = lax.axis_size("mp")
    base = section * count
    swaps = [[(base + m, base + (m ^ k)) for m in range(count)] for k in range(1, count)]
    return [value] + [lax.ppermute(value, ("section", "mp"), pairs) for pairs in swaps]


def params():
    return pltpu.CompilerParams(vmem_limit_bytes=16 * 2**20)


def call(body, args, specs, deps=(), **options):
    reads, waits = len(args), len(deps)

    def inner(*refs):
        body(*refs[:reads], *refs[reads + waits :])

    return pl.pallas_call(
        inner, in_specs=list(specs) + [ANY] * waits, compiler_params=params(), **options
    )(*args, *deps)


def run_copies(copies):
    for copy in copies:
        copy.start()
    for copy in copies:
        copy.wait()


def spread(onehot, value):
    high = value.astype(BF16)
    low = (value - high.astype(F32)).astype(BF16)
    return jnp.dot(onehot, high, preferred_element_type=F32) + jnp.dot(
        onehot, low, preferred_element_type=F32
    )


class Weights:
    def __init__(self, layer):
        self.count = lax.axis_size("mp")
        self.block_rows, self.width = layer.shape
        dp_index = lax.axis_index("dp")
        half = self.block_rows // 2
        self.offsets = [dp_index * half, (1 - dp_index) * half]
        self.pieces = [(layer, 0, None, 0)]
        self.colored = self.count == 4 and lax.axis_size("dp") == 2
        self.part = part = half // 2
        if self.colored:
            self.first = lax.dynamic_slice_in_dim(layer, dp_index * half, part, 0)
            self.second = lax.dynamic_slice_in_dim(layer, dp_index * half + part, part, 0)
            self.b1 = self.swap(self.second, 1)
            self.a2 = self.swap(self.first, 2)
            self.a1 = self.swap(self.first, 1)
            self.b2 = self.swap(self.second, 2)
            self.a3 = self.swap(self.a1, 2)
            self.b3 = self.swap(self.b2, 1)
            got = [(self.a1, 1, 0), (self.b2, 2, part), (self.b1, 1, part), (self.a2, 2, 0), (self.a3, 3, 0), (self.b3, 3, part)]
            for array, block, base in got:
                self.pieces.append((array, block, 0, base))
                self.pieces.append((dp_swap(array), block, 1, base))
        else:
            for block in range(1, self.count):
                self.pieces.append((mp_swap(layer, block), block, None, 0))

    def swap(self, array, flip):
        return mp_swap(array, flip)

    def assemble(self, ids, deps):
        early = len(self.pieces) - 4 if self.colored else len(self.pieces)
        layer = self.place(ids, None, self.pieces[:early], "assemble", deps)
        return layer if early == len(self.pieces) else self.place(ids, layer, self.pieces[early:], "complete", [])

    def place(self, ids, layer, pieces, name, deps):
        many = len(pieces)

        def body(ids_ref, *refs):
            out, sems = refs[-2:]
            copies = []
            for i, (array, block, which, base) in enumerate(pieces):
                row = pl.multiple_of(ids_ref[3 + block] * self.block_rows, self.block_rows) + base
                if which is not None:
                    row = row + pl.multiple_of(ids_ref[1 + which], self.block_rows // 2)
                copies.append(
                    pltpu.make_async_copy(refs[i], out.at[pl.ds(row, array.shape[0]), :], sems.at[i])
                )
            run_copies(copies)

        before = [] if layer is None else [layer]
        return call(
            body,
            [ids, *[piece[0] for piece in pieces], *before],
            [SMEM] + [ANY] * many + [VMEM] * len(before),
            deps,
            out_shape=jax.ShapeDtypeStruct((self.count * self.block_rows, self.width), BF16),
            out_specs=VMEM,
            input_output_aliases={1 + many: 0} if before else {},
            scratch_shapes=[pltpu.SemaphoreType.DMA((many,))],
            name=name,
        )


def fwd_stage(deps, level, ids, layer, rows, onehot, slope, kept):
    height, width = rows.shape
    prims = onehot.shape[1]
    leads = slope is None
    nb = width // BLOCKS

    def body(ids_ref, layer_ref, rows_ref, onehot_ref, *rest):
        if not leads:
            slope_ref, *rest = rest
        next_ref, pre_ref, kept_ref, *rest = rest[(kept is not None) :]
        if leads:
            tanh_ref, *rest = rest
        (kept_sem,) = rest

        @pl.when(ids_ref[0] == level)
        def _():
            keep = pltpu.make_async_copy(rows_ref, kept_ref, kept_sem)
            keep.start()

            def block(n, carry):
                cols = pl.ds(pl.multiple_of(n * nb, nb), nb)
                acc = jnp.dot(rows_ref[...], layer_ref[:, cols], preferred_element_type=F32)
                old = rows_ref[:, cols].astype(F32)
                pre_ref[:, cols] = acc.astype(BF16)
                if leads:
                    tanh_p = jnp.tanh(acc[:prims])
                    tanh_ref[:, cols] = tanh_p
                    factor = spread(onehot_ref[...], 1.0 - tanh_p * tanh_p)
                    new = jnp.concatenate(
                        [old[:prims] + tanh_p, old[prims:] + factor * acc[prims:]], axis=0
                    )
                else:
                    tanh_p = slope_ref[:, cols]
                    new = old + spread(onehot_ref[...], 1.0 - tanh_p * tanh_p) * acc
                next_ref[:, cols] = new.astype(BF16)
                return carry

            lax.fori_loop(0, BLOCKS, block, 0)
            keep.wait()

    outs = [jax.ShapeDtypeStruct((height, width), BF16)] * 3
    if leads:
        outs.append(jax.ShapeDtypeStruct((prims, width), F32))
    args = [ids, layer, rows, onehot] + ([] if leads else [slope])
    specs = [SMEM] + [VMEM] * (len(args) - 1)
    alias = {}
    if kept is not None:
        alias = {len(args): 2}
        args.append(kept)
        specs.append(ANY)
    return call(
        body,
        args,
        specs,
        deps,
        out_shape=outs,
        out_specs=[VMEM, VMEM, ANY] + [VMEM] * (len(outs) - 3),
        input_output_aliases=alias,
        scratch_shapes=[pltpu.SemaphoreType.DMA],
        cost_estimate=pl.CostEstimate(flops=2 * height * width * width * 4, bytes_accessed=2 * width * width, transcendentals=0),
        name=f"fwd{level}",
    )


def bwd_stage(deps, level, ids, layer, cot, pre, tanh_p, onehot, onehot_t, total, leads, kept):
    height, width = cot.shape
    prims = tanh_p.shape[0]
    deep = level > 0
    nb = width // BLOCKS

    def body(ids_ref, cot_ref, pre_ref, tanh_ref, onehot_ref, onehot_t_ref, *rest):
        if total is not None:
            total_ref, *rest = rest
        if deep:
            layer_ref, *rest = rest
        kept_ref, side_ref, *rest = rest[(kept is not None) :]
        if deep:
            new_ref, *rest = rest
        mix_ref, kept_sem = rest

        @pl.when(ids_ref[0] == level)
        def _():
            skip = prims if leads else 0

            def block(n, carry):
                cols = pl.ds(pl.multiple_of(n * nb, nb), nb)
                up = cot_ref[:, cols].astype(F32)
                tanh = tanh_ref[:, cols]
                slope = 1.0 - tanh * tanh
                up_t = up[skip:]
                mix_t = up_t * spread(onehot_ref[...], slope)
                total_here = spread(onehot_t_ref[...], up_t * pre_ref[:, cols].astype(F32)[skip:])
                if total is not None:
                    total_here = total_here + total_ref[:, cols]
                if leads:
                    mix_p = up[:prims] * slope - 2.0 * total_here * tanh * slope
                    mix_ref[:, cols] = jnp.concatenate([mix_p, mix_t], axis=0).astype(BF16)
                else:
                    mix_ref[:, cols] = mix_t.astype(BF16)
                side_ref[:, cols] = total_here
                return carry

            lax.fori_loop(0, BLOCKS, block, 0)
            keep = pltpu.make_async_copy(mix_ref, kept_ref, kept_sem)
            keep.start()
            if deep:

                def back_block(n, carry):
                    cols = pl.ds(pl.multiple_of(n * nb, nb), nb)
                    back = lax.dot_general(
                        mix_ref[...], layer_ref[cols, :], (((1,), (1,)), ((), ())), preferred_element_type=F32
                    )
                    new_ref[:, cols] = (cot_ref[:, cols].astype(F32) + back).astype(BF16)
                    return carry

                lax.fori_loop(0, BLOCKS, back_block, 0)
            keep.wait()

    rows_shape = jax.ShapeDtypeStruct((height, width), BF16)
    outs = [rows_shape, jax.ShapeDtypeStruct((prims, width), F32)] + ([rows_shape] if deep else [])
    args = [ids, cot, pre, tanh_p, onehot, onehot_t] + ([] if total is None else [total])
    args += [layer] if deep else []
    specs = [SMEM] + [VMEM] * (len(args) - 1)
    alias = {}
    if kept is not None:
        alias = {len(args): 0}
        args.append(kept)
        specs.append(ANY)
    return call(
        body,
        args,
        specs,
        deps,
        out_shape=outs,
        out_specs=[ANY] + [VMEM] * (len(outs) - 1),
        input_output_aliases=alias,
        scratch_shapes=[pltpu.VMEM((height, width), BF16), pltpu.SemaphoreType.DMA],
        cost_estimate=pl.CostEstimate(flops=2 * height * width * width * 4, bytes_accessed=2 * width * width, transcendentals=0),
        name=f"bwd{level}",
    )


def pick_rows(deps, ids, index, pieces, level):
    height = index.shape[0]
    piece_rows, width = pieces[0].shape

    def body(ids_ref, index_ref, *rest):
        out_ref = rest[-1]

        @pl.when(ids_ref[0] == level)
        def _():
            index_here = index_ref[...]
            acc = jnp.zeros((height, width), F32)
            for k, piece_ref in enumerate(rest[:-1]):
                place = lax.broadcasted_iota(jnp.int32, (height, piece_rows), 1) + k * piece_rows
                onehot = jnp.where(place == index_here, 1.0, 0.0).astype(BF16)
                acc = acc + jnp.dot(onehot, piece_ref[...], preferred_element_type=F32)
            out_ref[...] = acc.astype(BF16)

    return call(
        body,
        [ids, index, *pieces],
        [SMEM] + [VMEM] * (1 + len(pieces)),
        deps,
        out_shape=jax.ShapeDtypeStruct((height, width), BF16),
        out_specs=VMEM,
        name="pick",
    )


def lift_rows(ids, rows, encoder, chunks):
    height = rows.shape[0] // chunks
    width = encoder.shape[1]

    def body(ids_ref, rows_ref, encoder_ref, *outs):
        @pl.when(ids_ref[0] == 0)
        def _():
            for c, out in enumerate(outs):
                part = rows_ref[c * height : (c + 1) * height, :]
                out[...] = jnp.dot(part, encoder_ref[...], preferred_element_type=F32).astype(BF16)

    return pl.pallas_call(
        body,
        out_shape=[jax.ShapeDtypeStruct((height, width), BF16)] * chunks,
        in_specs=[SMEM, VMEM, VMEM],
        out_specs=[VMEM] * chunks,
        compiler_params=params(),
        name="lift",
    )(ids, rows, encoder)


def pack_columns(deps, ids, chunks, tails, level, n_dp, n_mp, blk):
    count = len(chunks)
    height, _ = chunks[0].shape
    tail_width = tails[0].shape[1] if tails else 0
    core = n_dp * blk
    end = count * height

    def body(ids_ref, *refs):
        chunk_refs, rest = refs[:count], refs[count:]
        tail_refs, outs = rest[: len(tails)], rest[len(tails) :]

        def fill():
            for k, out in enumerate(outs):
                for c, chunk_ref in enumerate(chunk_refs):
                    first = c * height
                    for d in range(n_dp):
                        col = pl.multiple_of((ids_ref[3 + k] + d * n_mp) * blk, blk)
                        out[first : first + height, d * blk : (d + 1) * blk] = chunk_ref[:, pl.ds(col, blk)]
                    if tails:
                        out[first : first + height, core:] = tail_refs[c][:height, :]
                if tails:
                    sums = [ref[height:, :].astype(F32)[: EXTRA // 2] for ref in tail_refs]
                    out[end:, :core] = jnp.zeros((EXTRA, core), BF16)
                    out[end:, core:] = jnp.concatenate(sums, axis=0).astype(BF16)

        if level is None:
            fill()
        else:
            pl.when(ids_ref[0] == level)(fill)

    shape = jax.ShapeDtypeStruct((end + (EXTRA if tails else 0), core + tail_width), BF16)
    return call(
        body,
        [ids, *chunks, *tails],
        [SMEM] + [VMEM] * (count + len(tails)),
        deps,
        out_shape=[shape] * n_mp,
        out_specs=[VMEM] * n_mp,
        name="pack",
    )


def both_groups(pieces):
    return pieces + ([dp_swap(piece) for piece in pieces] if lax.axis_size("dp") > 1 else [])


def loss_rows(loss, cols):
    high = loss.astype(BF16).astype(F32)
    line = lax.broadcasted_iota(jnp.int32, (EXTRA, cols), 0)
    return jnp.where(line == 0, high, jnp.where(line == 1, loss - high, 0.0))


def head_partial(deps, ids, pieces, level, blk):
    rows_each, wide = pieces[0].shape
    core = 2 * blk
    out_width = wide - core
    many = len(pieces)

    def body(ids_ref, *refs):
        piece_refs, (mine_ref, send_ref, left, right, sems) = refs[:many], refs[many:]

        @pl.when(ids_ref[0] == level)
        def _():
            here = pl.multiple_of(ids_ref[1] // ids_ref[7] * blk, blk)
            there = pl.multiple_of(blk - here, blk)
            copies = []
            for i, ref in enumerate(piece_refs):
                rows = pl.ds(i * rows_each, rows_each)
                copies.append(pltpu.make_async_copy(ref.at[:, pl.ds(here, blk)], left.at[rows, :blk], sems.at[0, i]))
                copies.append(pltpu.make_async_copy(ref.at[:, pl.ds(there, blk)], left.at[rows, blk:], sems.at[1, i]))
                copies.append(pltpu.make_async_copy(ref.at[:, core:], right.at[rows], sems.at[2, i]))
            run_copies(copies)
            loss = jnp.zeros((1, 128), F32)
            for piece in range(1, many + 1):
                tail = right[piece * rows_each - EXTRA : piece * rows_each, :128].astype(F32)
                loss = loss + tail[0:1] + tail[1:2] + tail[EXTRA // 2 : EXTRA // 2 + 1] + tail[EXTRA // 2 + 1 : EXTRA // 2 + 2]
            tail = loss_rows(loss[:, :1], out_width)
            part = lax.dot_general(left[...], right[...], (((0,), (0,)), ((), ())), preferred_element_type=F32)
            mine_ref[:blk, :] = part[:blk]
            mine_ref[blk:, :] = tail
            send_ref[:blk, :] = part[blk:].astype(BF16)
            send_ref[blk:, :] = tail.astype(BF16)

    shape = (blk + EXTRA, out_width)
    return call(
        body,
        [ids, *pieces],
        [SMEM] + [ANY] * many,
        deps,
        out_shape=[jax.ShapeDtypeStruct(shape, F32), jax.ShapeDtypeStruct(shape, BF16)],
        out_specs=[VMEM] * 2,
        scratch_shapes=[
            pltpu.VMEM((many * rows_each, core), BF16),
            pltpu.VMEM((many * rows_each, out_width), BF16),
            pltpu.SemaphoreType.DMA((3, many)),
        ],
        name="head_partial",
    )


def head_gradient(deps, ids, mine, other, level, blk, n_sec):
    cols = mine.shape[1] // n_sec

    def body(ids_ref, mine_ref, other_ref, *outs):
        @pl.when(ids_ref[0] == level)
        def _():
            tails = mine_ref[blk:, :1] + other_ref[blk:, :128].astype(F32)[:, :1]
            tail = loss_rows(tails[0:1] + tails[1:2], cols).astype(BF16)
            for j, out in enumerate(outs):
                span = slice(j * cols, (j + 1) * cols)
                out[:blk, :] = (mine_ref[:blk, span] + other_ref[:blk, span].astype(F32)).astype(BF16)
                out[blk:, :] = tail

    return call(
        body,
        [ids, mine, other],
        [SMEM, VMEM, VMEM],
        deps,
        out_shape=[jax.ShapeDtypeStruct((blk + EXTRA, cols), BF16)] * n_sec,
        out_specs=[VMEM] * n_sec,
        name="grad_head",
    )


def first_gradient(deps, ids, blocks, mixes, blk, height):
    many = len(mixes)
    every = len(blocks)
    width = mixes[0].shape[1]
    nb = width // BLOCKS

    def body(ids_ref, *refs):
        block_refs, mix_refs = refs[:every], refs[every : every + many]
        mine_ref, send_ref, later_ref, left, right, early, sems = refs[every + many :]
        here = pl.multiple_of(ids_ref[1] // ids_ref[7] * blk, blk)
        there = pl.multiple_of(blk - here, blk)
        copies = []
        for i in range(every):
            rows = pl.ds(i * height, height)
            if i < many:
                for j, col in enumerate([here, there]):
                    src = block_refs[i].at[height:, pl.ds(col, blk)]
                    copies.append(pltpu.make_async_copy(src, left.at[rows, j * blk : (j + 1) * blk], sems.at[j, i]))
                copies.append(pltpu.make_async_copy(mix_refs[i], right.at[rows], sems.at[2, i]))
            src = block_refs[i].at[:height, pl.ds(here, blk)]
            copies.append(pltpu.make_async_copy(src, early.at[rows], sems.at[3, i]))
        run_copies(copies)
        later_ref[...] = early[...].astype(F32).T.astype(BF16)
        turned = left[...].astype(F32).T.astype(BF16)
        for n in range(BLOCKS):
            cols = slice(n * nb, (n + 1) * nb)
            part = jnp.dot(turned, right[:, cols], preferred_element_type=F32)
            mine_ref[:, cols] = part[:blk]
            send_ref[:, cols] = part[blk:].astype(BF16)

    return call(
        body,
        [ids, *blocks, *mixes],
        [SMEM] + [ANY] * (every + many),
        deps,
        out_shape=[
            jax.ShapeDtypeStruct((blk, width), F32),
            jax.ShapeDtypeStruct((blk, width), BF16),
            jax.ShapeDtypeStruct((blk, every * height), BF16),
        ],
        out_specs=[VMEM] * 3,
        scratch_shapes=[
            pltpu.VMEM((many * height, 2 * blk), BF16),
            pltpu.VMEM((many * height, width), BF16),
            pltpu.VMEM((every * height, blk), BF16),
            pltpu.SemaphoreType.DMA((4, every)),
        ],
        name="first_gradient",
    )


def last_gradient(deps, ids, turned, mixes, mine, other, blocks, scale):
    blk, width = mine.shape
    nb = width // BLOCKS
    many = len(mixes)
    cols = blocks[0].shape[1]

    def body(ids_ref, turned_ref, *refs):
        mix_refs, (mine_ref, other_ref, *rest) = refs[:many], refs[many:]
        block_refs, (out, head_out, loss_out) = rest[:-3], rest[-3:]
        for j, ref in enumerate(block_refs):

            @pl.when(ids_ref[0] == j)
            def _():
                head_out[...] = ref[:blk, :].astype(F32)
                tail = ref[blk:, :].astype(F32)
                loss_out[...] = (tail[0:1, :128] + tail[1:2, :128]) * scale

        for n in range(BLOCKS):
            span = slice(n * nb, (n + 1) * nb)
            right = jnp.concatenate([ref[:, span] for ref in mix_refs], axis=0)
            part = jnp.dot(turned_ref[...], right, preferred_element_type=F32)
            out[:, span] = part + mine_ref[:, span] + other_ref[:, span].astype(F32)

    args = [ids, turned, *mixes, mine, other, *blocks]
    return call(
        body,
        args,
        [SMEM] + [VMEM] * (len(args) - 1),
        deps,
        out_shape=[
            jax.ShapeDtypeStruct((blk, width), F32),
            jax.ShapeDtypeStruct((blk, cols), F32),
            jax.ShapeDtypeStruct((1, 128), F32),
        ],
        out_specs=[VMEM] * 3,
        name="last_gradient",
    )


def join_rows(deps, flat, deep, rows_out):
    count, rank, width = deep.shape

    def body(flat_ref, deep_ref, out, sem):
        copies = [
            pltpu.make_async_copy(deep_ref.at[i], out.at[i * rank : (i + 1) * rank], sem.at[i])
            for i in range(count)
        ]
        for copy in copies:
            copy.start()
        spare = jnp.zeros((rows_out - count * (rank + 1), width), F32)
        out[count * rank :, :] = jnp.concatenate([flat_ref[...].astype(F32), spare], axis=0).astype(BF16)
        for copy in copies:
            copy.wait()

    return call(
        body,
        [flat, deep],
        [VMEM, ANY],
        deps,
        out_shape=jax.ShapeDtypeStruct((rows_out, width), BF16),
        out_specs=VMEM,
        scratch_shapes=[pltpu.SemaphoreType.DMA((count,))],
        name="join",
    )


def head_stage(deps, level, ids, rows, wanted, share, head_weight):
    height, width = rows.shape
    out_width = head_weight.shape[1]

    def body(ids_ref, rows_ref, wanted_ref, share_ref, head_ref, cot_ref, new_ref):
        @pl.when(ids_ref[0] == level)
        def _():
            nb = out_width // BLOCKS

            def block(n, loss):
                cols = pl.ds(pl.multiple_of(n * nb, nb), nb)
                outputs = jnp.dot(rows_ref[...], head_ref[:, cols], preferred_element_type=F32)
                mismatch = outputs - wanted_ref[:, cols].astype(F32)
                scaled = share_ref[...] * mismatch
                cot_ref[:height, cols] = (2.0 * scaled).astype(BF16)
                return loss + jnp.sum(scaled * mismatch, axis=1, keepdims=True)

            loss = lax.fori_loop(0, BLOCKS, block, jnp.zeros((height, 1), F32))
            loss = jnp.sum(loss, axis=0, keepdims=True)
            line = lax.broadcasted_iota(jnp.int32, (EXTRA, out_width), 0)
            high = loss.astype(BF16).astype(F32)
            tail = jnp.where(line == 0, high, jnp.where(line == 1, loss - high, 0.0))
            cot_ref[height:, :] = tail.astype(BF16)
            kb = width // BLOCKS

            def back_block(k, carry):
                cols = pl.ds(pl.multiple_of(k * kb, kb), kb)
                new_ref[:, cols] = lax.dot_general(
                    cot_ref[:height, :], head_ref[cols, :], (((1,), (1,)), ((), ())), preferred_element_type=F32
                ).astype(BF16)
                return carry

            lax.fori_loop(0, BLOCKS, back_block, 0)

    return call(
        body,
        [ids, rows, wanted, share, head_weight],
        [SMEM] + [VMEM] * 4,
        deps,
        out_shape=[
            jax.ShapeDtypeStruct((height + EXTRA, out_width), BF16),
            jax.ShapeDtypeStruct((height, width), BF16),
        ],
        out_specs=[VMEM] * 2,
        cost_estimate=pl.CostEstimate(flops=2 * height * width * width * 4, bytes_accessed=2 * width * out_width, transcendentals=0),
        name="head",
    )


def local(
    inputs, tangents, targets, target_jac, rank_mask, batch_order, encoder, layers, head_weight
):
    samp_dev, rank = rank_mask.shape
    in_width = inputs.shape[1]
    width = layers.shape[2]
    out_width = head_weight.shape[1]
    n_dp = lax.axis_size("dp")
    n_mp = lax.axis_size("mp")
    n_sec = lax.axis_size("section")
    last = n_sec - 1
    dp_index = lax.axis_index("dp")
    sec = lax.axis_index("section")
    mp_index = lax.axis_index("mp")
    prims = n_mp * samp_dev
    blk = width // (n_dp * n_mp)

    weights = Weights(layers[0])
    helper = last

    piece_rows = round_up(samp_dev * (rank + 1), 16)
    joined_rows = join_rows([], inputs, tangents, piece_rows)
    row_pieces = plane_pieces(joined_rows, helper)

    own_rank = jnp.sum(rank_mask, axis=1)
    slot_line = jnp.arange(samp_dev, dtype=jnp.int32)
    own_slot = jnp.sum(
        jnp.where(batch_order[0][None, :] == slot_line[:, None], slot_line[None, :], 0), axis=1
    ) // (samp_dev // MB)
    own_meta = jnp.stack([own_rank, own_slot]).astype(jnp.int32)
    meta_pieces = jnp.stack(mp_pieces(own_meta))
    order_line = jnp.arange(n_mp, dtype=jnp.int32)
    swap = ((order_line[:, None] ^ mp_index) == order_line[None, :]).astype(jnp.int32)
    meta = jnp.sum(swap[:, :, None, None] * meta_pieces[None], axis=1)
    ranks = meta[:, 0].reshape(prims)
    slots = meta[:, 1].reshape(prims)
    sample_line = jnp.arange(prims, dtype=jnp.int32)
    ends = jnp.sum(jnp.where(sample_line[None, :] <= sample_line[:, None], ranks[None, :], 0), axis=1)
    active = jnp.sum(ranks)
    counts = jnp.sum(jnp.where(slots[None, :] == slots[:, None], ranks[None, :] + 1, 0), axis=1)
    inverse = 1.0 / counts.astype(F32)

    kb = width // n_mp
    ids = jnp.stack(
        [sec] + weights.offsets + [mp_index ^ k for k in range(n_mp)] + [jnp.int32(kb // 2)] * (n_mp == 4)
    ).astype(jnp.int32)
    chunks = 2
    usual = samp_dev * (rank // 2 + 1)
    height = max(round_up(-(-(prims + usual) // chunks), 16), round_up(prims + 8, 16))
    slots_here = chunks * height - prims

    place = mp_index * slots_here + jnp.arange(slots_here, dtype=jnp.int32)
    passed = ends[None, :] <= place[:, None]
    sample = jnp.sum(passed.astype(jnp.int32), axis=1)
    column = place - jnp.sum(jnp.where(passed, ranks[None, :], 0), axis=1)
    present = place < active
    belongs = (sample[:, None] == sample_line[None, :]) & present[:, None]
    source = ((sample // samp_dev) ^ mp_index) * piece_rows + (sample % samp_dev) * rank + column
    source = jnp.where(present, source, -1)
    source_p = ((sample_line // samp_dev) ^ mp_index) * piece_rows + samp_dev * rank + sample_line % samp_dev
    share = jnp.sum(jnp.where(belongs, inverse[None, :], 0.0), axis=1)
    share_p = jnp.where(sample_line // samp_dev == mp_index, inverse, 0.0)
    index = jnp.concatenate([source_p, source])[:, None]
    shares = jnp.concatenate([share_p, share])[:, None]
    onehot = belongs.astype(BF16)
    first = height - prims
    onehots = [onehot[:first], onehot[first:]]
    onehot_t = ((sample_line[:, None] == sample[None, :]) & present[None, :]).astype(BF16)
    onehots_t = [onehot_t[:, :first], onehot_t[:, first:]]
    share_of = [shares[:height], shares[height:]]

    packed = pick_rows([], ids, index, row_pieces, helper)
    if helper != 0:
        packed = hop(packed, helper, 0)
    rows = list(lift_rows(ids, packed, encoder, chunks))
    other_active = dp_swap(active.reshape(1, 1)).reshape(()) if n_dp > 1 else active
    most_active = jnp.maximum(active, other_active)

    small_arrays = [*onehots, *onehots_t, *share_of, index, most_active.reshape(1)]
    layer = weights.assemble(ids, small_arrays)
    token = []
    entered = [None] * chunks
    pres = [[None] * n_sec for _ in range(chunks)]
    tanhs = [None] * n_sec
    heads = [None] * chunks
    goal_pieces = None
    for level in range(n_sec):
        for c in range(chunks):
            got = fwd_stage(
                token, level, ids, layer, rows[c], onehots[c], None if c == 0 else tanhs[level], entered[c]
            )
            token = [got[0]]
            entered[c], pres[c][level] = got[2], got[1]
            if c == 0:
                tanhs[level] = got[3]
            rows[c] = got[0] if level == last else hop(got[0], level, level + 1)
            if level == last:
                heads[c] = head_stage(
                    token, last, ids, rows[c], wanted[c * height : (c + 1) * height], share_of[c], head_weight
                )
                token = [heads[c][1]]
        if goal_pieces is None:
            goal_pieces = plane_pieces(join_rows(token, targets, target_jac, piece_rows), last)
        if level == max(last - 1, 0):
            wanted = pick_rows(token, ids, index, goal_pieces, last)
            token = [wanted]

    small = n_dp * n_mp <= 8 and blk % 128 == 0
    cots = [heads[c][1] for c in range(chunks)]
    mixes = [None] * chunks
    backward_order = list(range(1, chunks)) + [0]
    hidden_pieces = head_pieces = None
    arrived = []
    for level in range(last, -1, -1):
        total = None
        for c in backward_order:
            got = bwd_stage(
                token, level, ids, layer, cots[c], pres[c][level], tanhs[level],
                onehots[c], onehots_t[c], total, c == 0, mixes[c],
            )
            mixes[c], total = got[0], got[1]
            token = [got[1]]
            if level > 0:
                cots[c] = hop(got[2], level, level - 1)
        if not small:
            continue
        if level == last:
            sends = pack_columns(token, ids, rows, [h[0] for h in heads], last, n_dp, n_mp, blk)
            token = [sends[0]]
            base = last * n_mp
            head_pieces = [sends[0]] + [
                lax.ppermute(sends[k], ("section", "mp"), [(base + m, base + (m ^ k)) for m in range(n_mp)])
                for k in range(1, n_mp)
            ]
        elif level == last - 1:
            sends = pack_columns(token, ids, entered, [], None, n_dp, n_mp, blk)
            token = [sends[0]]
            hidden_pieces = [sends[0]] + [mp_swap(sends[k], k) for k in range(1, n_mp)]

    cols = out_width // n_sec
    if small:
        swapped = []
        for c in backward_order:
            swapped.append([mixes[c]] + [mp_swap(mixes[c], k) for k in range(1, n_mp)])
        hidden_pieces = both_groups(hidden_pieces)
        first_mine, send, turned = first_gradient([], ids, hidden_pieces, swapped[0], blk, height)
        first_other = dp_swap(send)
        mine, send = head_partial([], ids, head_pieces, last, blk)
        other = dp_swap(send)
        blocks = head_gradient([], ids, mine, other, last, blk, n_sec)
        arrived = [hop(blocks[j], last, j) for j in range(last)]
        grad, head_mine, loss_mine = last_gradient(
            [], ids, turned, both_groups(swapped[1]), first_mine, first_other, [*arrived, blocks[last]],
            1.0 / (n_dp * MB * out_width),
        )
        loss_mine = loss_mine[0, 0]
    else:
        contract = (((0,), (0,)), ((), ()))
        joined = jnp.concatenate(entered, axis=0)
        part = lax.dot_general(joined, jnp.concatenate(mixes, axis=0), contract, preferred_element_type=F32)
        grad = lax.psum_scatter(part.astype(BF16), ("dp", "mp"), scatter_dimension=0, tiled=True).astype(F32)
        cot_out = jnp.concatenate([h[0][:height] for h in heads], axis=0)
        part = lax.dot_general(jnp.concatenate(rows, axis=0), cot_out, contract, preferred_element_type=F32)
        head = lax.psum_scatter(part.astype(BF16), ("dp", "mp"), scatter_dimension=0, tiled=True)
        loss = sum(jnp.sum(h[0][height : height + 2, 0].astype(F32)) for h in heads)
        loss = jnp.where(sec == last, lax.psum(loss, ("dp", "mp")), 0.0).reshape(1, 1)
        head_mine = jnp.where(sec == last, head[:, last * cols :], jnp.zeros((blk, cols), BF16))
        loss_mine = loss
        for j in range(last):
            head_mine = head_mine + hop(head[:, j * cols : (j + 1) * cols], last, j)
            loss_mine = loss_mine + hop(loss, last, j)
        head_mine = head_mine.astype(F32)
        loss_mine = loss_mine.reshape(()) / (n_dp * MB * out_width)
    fast = (grad[None], head_mine, loss_mine)

    def plain():
        depth = rank + 1
        total_rows = samp_dev * depth
        layer_full = jnp.zeros((width, width), BF16)
        kb = weights.block_rows
        for array, block, which, base in weights.pieces:
            row = (mp_index ^ block) * kb + base
            row = row if which is None else row + weights.offsets[which]
            layer_full = lax.dynamic_update_slice_in_dim(layer_full, array, row, 0)
        rows_in = jnp.concatenate([inputs[:, None, :], tangents], axis=1).reshape(total_rows, in_width)
        start = jnp.dot(rows_in, encoder, preferred_element_type=F32).astype(BF16)
        chain = [(j, (j + 1) % n_sec) for j in range(n_sec)]

        def back_one(value):
            return lax.fori_loop(0, last, lambda _, v: lax.ppermute(v, "section", chain), value)

        def pre_of(rows):
            pre = jnp.dot(rows, layer_full, preferred_element_type=F32).reshape(samp_dev, depth, width)
            tanh_p = jnp.tanh(pre[:, 0])
            return pre, tanh_p, 1.0 - tanh_p * tanh_p

        def forward(level, state):
            rows, mine, _ = state
            mine = jnp.where(level == sec, rows, mine)
            pre, tanh_p, slope = pre_of(rows)
            change = jnp.concatenate([tanh_p[:, None], slope[:, None] * pre[:, 1:]], axis=1)
            new = (rows.astype(F32) + change.reshape(total_rows, width)).astype(BF16)
            return lax.ppermute(new, "section", chain), mine, new

        _, mine, final = lax.fori_loop(0, n_sec, forward, (start, start, start))
        own = lax.dynamic_slice_in_dim(inverse, mp_index * samp_dev, samp_dev, 0)
        row_weight = jnp.concatenate([jnp.ones((samp_dev, 1), F32), rank_mask.astype(F32)], axis=1)
        share = (row_weight * own[:, None]).reshape(total_rows, 1)
        outputs = jnp.dot(final, head_weight, preferred_element_type=F32)
        wanted = jnp.concatenate([targets[:, None, :], target_jac], axis=1).reshape(total_rows, out_width)
        mismatch = outputs - wanted.astype(F32)
        loss = jnp.sum(share * mismatch * mismatch)
        cot_out = (2.0 * share * mismatch).astype(BF16)
        cot = lax.dot_general(cot_out, head_weight, (((1,), (1,)), ((), ())), preferred_element_type=F32)
        pre, tanh_p, slope = pre_of(mine)

        def backward(step, state):
            cot, mix_mine = state
            up = cot.astype(F32).reshape(samp_dev, depth, width)
            side = jnp.sum(up[:, 1:] * pre[:, 1:], axis=1)
            lead = up[:, 0] * slope - 2.0 * side * tanh_p * slope
            mix = jnp.concatenate([lead[:, None], up[:, 1:] * slope[:, None]], axis=1)
            mix = mix.astype(BF16).reshape(total_rows, width)
            mix_mine = jnp.where(step == last - sec, mix, mix_mine)
            back = lax.dot_general(mix, layer_full, (((1,), (1,)), ((), ())), preferred_element_type=F32)
            new = (up.reshape(total_rows, width) + back).astype(BF16)
            return back_one(new), mix_mine

        _, mix = lax.fori_loop(0, n_sec, backward, (cot.astype(BF16), mine))

        def scatter(left, right):
            part = lax.dot_general(left, right, (((0,), (0,)), ((), ())), preferred_element_type=F32)
            part = part.astype(BF16).reshape(n_dp, n_mp, blk, right.shape[1])
            mine_part = jnp.zeros((n_dp, blk, right.shape[1]), F32)
            for k in range(n_mp):
                piece = lax.dynamic_index_in_dim(part, mp_index ^ k, 1, False)
                mine_part = mine_part + (piece if k == 0 else mp_swap(piece, k)).astype(F32)
            kept = lax.dynamic_index_in_dim(mine_part, dp_index, 0, False)
            if n_dp > 1:
                sent = lax.dynamic_index_in_dim(mine_part, 1 - dp_index, 0, False)
                kept = kept + dp_swap(sent.astype(BF16)).astype(F32)
            return kept

        grad = scatter(mine, mix)
        head = scatter(final, cot_out)
        cols = out_width // n_sec
        loss_group = sum(mp_pieces(loss.reshape(1, 1)))
        if n_dp > 1:
            loss_group = loss_group + dp_swap(loss_group)
        head_mine = jnp.where(sec == last, head[:, last * cols :], 0.0)
        loss_mine = jnp.where(sec == last, loss_group, 0.0)
        for j in range(last):
            block = jnp.concatenate([head[:, j * cols : (j + 1) * cols], jnp.broadcast_to(loss_group, (8, cols))])
            block = hop(block, last, j)
            head_mine = head_mine + block[:blk]
            loss_mine = loss_mine + block[blk:, :1][:1]
        return grad[None], head_mine, loss_mine.reshape(()) / (n_dp * MB * out_width)

    room = n_mp * slots_here
    if room >= n_mp * samp_dev * rank:
        return fast
    return lax.while_loop(
        lambda state: state[0] > room, lambda state: (jnp.int32(0), *plain()), (most_active, *fast)
    )[1:]


def solution(mesh):
    in_specs = (
        P(("dp", "mp"), None),
        P(("dp", "mp"), None, None),
        P(("dp", "mp"), None),
        P(("dp", "mp"), None, None),
        P(("dp", "mp"), None),
        P(("dp", "mp"), None),
        P(),
        P("section", "mp", None),
        P(),
    )
    out_specs = (P("section", ("dp", "mp"), None), P(("dp", "mp"), "section"), P())

    return jax.shard_map(local, mesh=mesh, in_specs=in_specs, out_specs=out_specs, check_vma=False)
```

```python
import jax
import jax.numpy as jnp
from jax import lax
from jax.experimental import pallas as pl
from jax.experimental.pallas import tpu as pltpu
from jax.sharding import PartitionSpec as P


F32 = jnp.float32
BF16 = jnp.bfloat16
MB = 6
EXTRA = 16
BLOCKS = 4

ANY = pl.BlockSpec(memory_space=pl.ANY)
SMEM = pl.BlockSpec(memory_space=pltpu.SMEM)
VMEM = pl.BlockSpec(memory_space=pltpu.VMEM)


def round_up(value, unit):
    return -(-value // unit) * unit


def mp_swap(value, flip):
    count = lax.axis_size("mp")
    return lax.ppermute(value, "mp", [(m, m ^ flip) for m in range(count)])


def dp_swap(value):
    count = lax.axis_size("dp")
    return lax.ppermute(value, "dp", [(d, d ^ 1) for d in range(count)])


def mp_pieces(value):
    return [value] + [mp_swap(value, k) for k in range(1, lax.axis_size("mp"))]


def hop(value, source, target):
    return lax.ppermute(value, "section", [(source, target)])


def plane_pieces(value, section):
    count = lax.axis_size("mp")
    base = section * count
    swaps = [[(base + m, base + (m ^ k)) for m in range(count)] for k in range(1, count)]
    return [value] + [lax.ppermute(value, ("section", "mp"), pairs) for pairs in swaps]


def params():
    return pltpu.CompilerParams(vmem_limit_bytes=20 * 2**20)


def call(body, args, specs, deps=(), **options):
    reads, waits = len(args), len(deps)

    def inner(*refs):
        body(*refs[:reads], *refs[reads + waits :])

    return pl.pallas_call(
        inner, in_specs=list(specs) + [ANY] * waits, compiler_params=params(), **options
    )(*args, *deps)


def each_block(width, body):
    nb = width // BLOCKS
    for n in range(BLOCKS):
        body(slice(n * nb, (n + 1) * nb))


def run_copies(copies):
    for copy in copies:
        copy.start()
    for copy in copies:
        copy.wait()


def spread(onehot, value):
    high = value.astype(BF16)
    low = (value - high.astype(F32)).astype(BF16)
    return jnp.dot(onehot, high, preferred_element_type=F32) + jnp.dot(
        onehot, low, preferred_element_type=F32
    )


class Weights:
    def __init__(self, layer):
        self.count = lax.axis_size("mp")
        self.block_rows, self.width = layer.shape
        dp_index = lax.axis_index("dp")
        half = self.block_rows // 2
        self.offsets = [dp_index * half, (1 - dp_index) * half]
        self.pieces = [(layer, 0, None, 0)]
        self.colored = self.count == 4 and lax.axis_size("dp") == 2
        self.part = part = half // 2
        if self.colored:
            self.first = lax.dynamic_slice_in_dim(layer, dp_index * half, part, 0)
            self.second = lax.dynamic_slice_in_dim(layer, dp_index * half + part, part, 0)
            self.b1 = self.swap(self.second, 1)
            self.a2 = self.swap(self.first, 2)
            self.a1 = self.swap(self.first, 1)
            self.b2 = self.swap(self.second, 2)
            self.a3 = self.swap(self.a1, 2)
            self.b3 = self.swap(self.b2, 1)
            got = [(self.a1, 1, 0), (self.b2, 2, part), (self.b1, 1, part), (self.a2, 2, 0), (self.a3, 3, 0), (self.b3, 3, part)]
            for array, block, base in got:
                self.pieces.append((array, block, 0, base))
                self.pieces.append((dp_swap(array), block, 1, base))
        else:
            for block in range(1, self.count):
                self.pieces.append((mp_swap(layer, block), block, None, 0))

    def swap(self, array, flip):
        return mp_swap(array, flip)

    def assemble(self, ids, deps):
        early = len(self.pieces) - 4 if self.colored else len(self.pieces)
        layer = self.place(ids, None, self.pieces[:early], "assemble", deps)
        return layer if early == len(self.pieces) else self.place(ids, layer, self.pieces[early:], "complete", [])

    def place(self, ids, layer, pieces, name, deps):
        many = len(pieces)

        def body(ids_ref, *refs):
            out, sems = refs[-2:]
            copies = []
            for i, (array, block, which, base) in enumerate(pieces):
                row = pl.multiple_of(ids_ref[3 + block] * self.block_rows, self.block_rows) + base
                if which is not None:
                    row = row + pl.multiple_of(ids_ref[1 + which], self.block_rows // 2)
                copies.append(
                    pltpu.make_async_copy(refs[i], out.at[pl.ds(row, array.shape[0]), :], sems.at[i])
                )
            run_copies(copies)

        before = [] if layer is None else [layer]
        return call(
            body,
            [ids, *[piece[0] for piece in pieces], *before],
            [SMEM] + [ANY] * many + [VMEM] * len(before),
            deps,
            out_shape=jax.ShapeDtypeStruct((self.count * self.block_rows, self.width), BF16),
            out_specs=VMEM,
            input_output_aliases={1 + many: 0} if before else {},
            scratch_shapes=[pltpu.SemaphoreType.DMA((many,))],
            name=name,
        )


def fwd_stage(deps, level, ids, layer, rows, onehot, slope, kept):
    height, width = rows.shape
    prims = onehot.shape[1]
    leads = slope is None

    def body(ids_ref, layer_ref, rows_ref, onehot_ref, *rest):
        if not leads:
            slope_ref, *rest = rest
        next_ref, pre_ref, kept_ref, *rest = rest[(kept is not None) :]
        if leads:
            tanh_ref, *rest = rest
        (kept_sem,) = rest

        @pl.when(ids_ref[0] == level)
        def _():
            keep = pltpu.make_async_copy(rows_ref, kept_ref, kept_sem)
            keep.start()

            def block(cols):
                acc = jnp.dot(rows_ref[...], layer_ref[:, cols], preferred_element_type=F32)
                old = rows_ref[:, cols].astype(F32)
                pre_ref[:, cols] = acc.astype(BF16)
                if leads:
                    tanh_p = jnp.tanh(acc[:prims])
                    tanh_ref[:, cols] = tanh_p
                    factor = spread(onehot_ref[...], 1.0 - tanh_p * tanh_p)
                    new = jnp.concatenate(
                        [old[:prims] + tanh_p, old[prims:] + factor * acc[prims:]], axis=0
                    )
                else:
                    tanh_p = slope_ref[:, cols]
                    new = old + spread(onehot_ref[...], 1.0 - tanh_p * tanh_p) * acc
                next_ref[:, cols] = new.astype(BF16)

            each_block(width, block)
            keep.wait()

    outs = [jax.ShapeDtypeStruct((height, width), BF16)] * 3
    if leads:
        outs.append(jax.ShapeDtypeStruct((prims, width), F32))
    args = [ids, layer, rows, onehot] + ([] if leads else [slope])
    specs = [SMEM] + [VMEM] * (len(args) - 1)
    alias = {}
    if kept is not None:
        alias = {len(args): 2}
        args.append(kept)
        specs.append(ANY)
    return call(
        body,
        args,
        specs,
        deps,
        out_shape=outs,
        out_specs=[VMEM, VMEM, ANY] + [VMEM] * (len(outs) - 3),
        input_output_aliases=alias,
        scratch_shapes=[pltpu.SemaphoreType.DMA],
        cost_estimate=pl.CostEstimate(flops=2 * height * width * width * 4, bytes_accessed=2 * width * width, transcendentals=0),
        name=f"fwd{level}",
    )


def bwd_stage(deps, level, ids, turned, cot, pre, tanh_p, onehot, onehot_t, total, leads, kept):
    height, width = cot.shape
    prims = tanh_p.shape[0]
    deep = level > 0

    def body(ids_ref, cot_ref, pre_ref, tanh_ref, onehot_ref, onehot_t_ref, *rest):
        if total is not None:
            total_ref, *rest = rest
        if deep:
            turned_ref, *rest = rest
        kept_ref, side_ref, *rest = rest[(kept is not None) :]
        if deep:
            new_ref, *rest = rest
        mix_ref, kept_sem = rest

        @pl.when(ids_ref[0] == level)
        def _():
            skip = prims if leads else 0

            def block(cols):
                up = cot_ref[:, cols].astype(F32)
                tanh = tanh_ref[:, cols]
                slope = 1.0 - tanh * tanh
                up_t = up[skip:]
                mix_t = up_t * spread(onehot_ref[...], slope)
                total_here = spread(onehot_t_ref[...], up_t * pre_ref[:, cols].astype(F32)[skip:])
                if total is not None:
                    total_here = total_here + total_ref[:, cols]
                if leads:
                    mix_p = up[:prims] * slope - 2.0 * total_here * tanh * slope
                    mix_ref[:, cols] = jnp.concatenate([mix_p, mix_t], axis=0).astype(BF16)
                else:
                    mix_ref[:, cols] = mix_t.astype(BF16)
                side_ref[:, cols] = total_here

            each_block(width, block)
            keep = pltpu.make_async_copy(mix_ref, kept_ref, kept_sem)
            keep.start()
            if deep:

                def back_block(cols):
                    back = jnp.dot(mix_ref[...], turned_ref[:, cols], preferred_element_type=F32)
                    new_ref[:, cols] = (cot_ref[:, cols].astype(F32) + back).astype(BF16)

                each_block(width, back_block)
            keep.wait()

    rows_shape = jax.ShapeDtypeStruct((height, width), BF16)
    outs = [rows_shape, jax.ShapeDtypeStruct((prims, width), F32)] + ([rows_shape] if deep else [])
    args = [ids, cot, pre, tanh_p, onehot, onehot_t] + ([] if total is None else [total])
    args += [turned] if deep else []
    specs = [SMEM] + [VMEM] * (len(args) - 1)
    alias = {}
    if kept is not None:
        alias = {len(args): 0}
        args.append(kept)
        specs.append(ANY)
    return call(
        body,
        args,
        specs,
        deps,
        out_shape=outs,
        out_specs=[ANY] + [VMEM] * (len(outs) - 1),
        input_output_aliases=alias,
        scratch_shapes=[pltpu.VMEM((height, width), BF16), pltpu.SemaphoreType.DMA],
        cost_estimate=pl.CostEstimate(flops=2 * height * width * width * 4, bytes_accessed=2 * width * width, transcendentals=0),
        name=f"bwd{level}",
    )


def turn(deps, ids, matrix, least):
    rows, cols = matrix.shape
    step = 256

    def body(ids_ref, matrix_ref, out_ref):
        @pl.when(ids_ref[0] >= least)
        def _():
            def strip(i, carry):
                top = pl.ds(pl.multiple_of(i * step, step), step)
                out_ref[:, top] = matrix_ref[top, :].T
                return carry

            lax.fori_loop(0, rows // step, strip, 0)

    return call(
        body,
        [ids, matrix],
        [SMEM, VMEM],
        deps,
        out_shape=jax.ShapeDtypeStruct((cols, rows), matrix.dtype),
        out_specs=VMEM,
        name="turn",
    )


def pick_rows(deps, ids, index, pieces, level):
    height = index.shape[0]
    piece_rows, width = pieces[0].shape

    def body(ids_ref, index_ref, *rest):
        out_ref = rest[-1]

        @pl.when(ids_ref[0] == level)
        def _():
            index_here = index_ref[...]
            acc = jnp.zeros((height, width), F32)
            for k, piece_ref in enumerate(rest[:-1]):
                place = lax.broadcasted_iota(jnp.int32, (height, piece_rows), 1) + k * piece_rows
                onehot = jnp.where(place == index_here, 1.0, 0.0).astype(BF16)
                acc = acc + jnp.dot(onehot, piece_ref[...], preferred_element_type=F32)
            out_ref[...] = acc.astype(BF16)

    return call(
        body,
        [ids, index, *pieces],
        [SMEM] + [VMEM] * (1 + len(pieces)),
        deps,
        out_shape=jax.ShapeDtypeStruct((height, width), BF16),
        out_specs=VMEM,
        name="pick",
    )


def lift_rows(ids, rows, encoder, chunks):
    height = rows.shape[0] // chunks
    width = encoder.shape[1]

    def body(ids_ref, rows_ref, encoder_ref, *outs):
        @pl.when(ids_ref[0] == 0)
        def _():
            for c, out in enumerate(outs):
                part = rows_ref[c * height : (c + 1) * height, :]
                out[...] = jnp.dot(part, encoder_ref[...], preferred_element_type=F32).astype(BF16)

    return pl.pallas_call(
        body,
        out_shape=[jax.ShapeDtypeStruct((height, width), BF16)] * chunks,
        in_specs=[SMEM, VMEM, VMEM],
        out_specs=[VMEM] * chunks,
        compiler_params=params(),
        name="lift",
    )(ids, rows, encoder)


def pack_columns(deps, ids, chunks, tails, level, n_dp, n_mp, blk):
    count = len(chunks)
    height, _ = chunks[0].shape
    tail_width = tails[0].shape[1] if tails else 0
    core = n_dp * blk
    end = count * height

    def body(ids_ref, *refs):
        chunk_refs, rest = refs[:count], refs[count:]
        tail_refs, outs = rest[: len(tails)], rest[len(tails) :]

        def fill():
            for k, out in enumerate(outs):
                for c, chunk_ref in enumerate(chunk_refs):
                    first = c * height
                    for d in range(n_dp):
                        col = pl.multiple_of((ids_ref[3 + k] + d * n_mp) * blk, blk)
                        out[first : first + height, d * blk : (d + 1) * blk] = chunk_ref[:, pl.ds(col, blk)]
                    if tails:
                        out[first : first + height, core:] = tail_refs[c][:height, :]
                if tails:
                    sums = [ref[height:, :].astype(F32)[: EXTRA // 2] for ref in tail_refs]
                    out[end:, :core] = jnp.zeros((EXTRA, core), BF16)
                    out[end:, core:] = jnp.concatenate(sums, axis=0).astype(BF16)

        if level is None:
            fill()
        else:
            pl.when(ids_ref[0] == level)(fill)

    shape = jax.ShapeDtypeStruct((end + (EXTRA if tails else 0), core + tail_width), BF16)
    return call(
        body,
        [ids, *chunks, *tails],
        [SMEM] + [VMEM] * (count + len(tails)),
        deps,
        out_shape=[shape] * n_mp,
        out_specs=[VMEM] * n_mp,
        name="pack",
    )


def both_groups(pieces):
    return pieces + ([dp_swap(piece) for piece in pieces] if lax.axis_size("dp") > 1 else [])


def loss_rows(loss, cols):
    high = loss.astype(BF16).astype(F32)
    line = lax.broadcasted_iota(jnp.int32, (EXTRA, cols), 0)
    return jnp.where(line == 0, high, jnp.where(line == 1, loss - high, 0.0))


def head_partial(deps, ids, pieces, level, blk):
    rows_each, wide = pieces[0].shape
    core = 2 * blk
    out_width = wide - core
    many = len(pieces)

    def body(ids_ref, *refs):
        piece_refs, (mine_ref, send_ref, left, right, sems) = refs[:many], refs[many:]

        @pl.when(ids_ref[0] == level)
        def _():
            here = pl.multiple_of(ids_ref[1] // ids_ref[7] * blk, blk)
            there = pl.multiple_of(blk - here, blk)
            copies = []
            for i, ref in enumerate(piece_refs):
                rows = pl.ds(i * rows_each, rows_each)
                copies.append(pltpu.make_async_copy(ref.at[:, pl.ds(here, blk)], left.at[rows, :blk], sems.at[0, i]))
                copies.append(pltpu.make_async_copy(ref.at[:, pl.ds(there, blk)], left.at[rows, blk:], sems.at[1, i]))
                copies.append(pltpu.make_async_copy(ref.at[:, core:], right.at[rows], sems.at[2, i]))
            run_copies(copies)
            loss = jnp.zeros((1, 128), F32)
            for piece in range(1, many + 1):
                tail = right[piece * rows_each - EXTRA : piece * rows_each, :128].astype(F32)
                loss = loss + tail[0:1] + tail[1:2] + tail[EXTRA // 2 : EXTRA // 2 + 1] + tail[EXTRA // 2 + 1 : EXTRA // 2 + 2]
            tail = loss_rows(loss[:, :1], out_width)
            part = lax.dot_general(left[...], right[...], (((0,), (0,)), ((), ())), preferred_element_type=F32)
            mine_ref[:blk, :] = part[:blk]
            mine_ref[blk:, :] = tail
            send_ref[:blk, :] = part[blk:].astype(BF16)
            send_ref[blk:, :] = tail.astype(BF16)

    shape = (blk + EXTRA, out_width)
    return call(
        body,
        [ids, *pieces],
        [SMEM] + [ANY] * many,
        deps,
        out_shape=[jax.ShapeDtypeStruct(shape, F32), jax.ShapeDtypeStruct(shape, BF16)],
        out_specs=[VMEM] * 2,
        scratch_shapes=[
            pltpu.VMEM((many * rows_each, core), BF16),
            pltpu.VMEM((many * rows_each, out_width), BF16),
            pltpu.SemaphoreType.DMA((3, many)),
        ],
        name="head_partial",
    )


def head_gradient(deps, ids, mine, other, level, blk, n_sec):
    cols = mine.shape[1] // n_sec

    def body(ids_ref, mine_ref, other_ref, *outs):
        @pl.when(ids_ref[0] == level)
        def _():
            tails = mine_ref[blk:, :1] + other_ref[blk:, :128].astype(F32)[:, :1]
            tail = loss_rows(tails[0:1] + tails[1:2], cols).astype(BF16)
            for j, out in enumerate(outs):
                span = slice(j * cols, (j + 1) * cols)
                out[:blk, :] = (mine_ref[:blk, span] + other_ref[:blk, span].astype(F32)).astype(BF16)
                out[blk:, :] = tail

    return call(
        body,
        [ids, mine, other],
        [SMEM, VMEM, VMEM],
        deps,
        out_shape=[jax.ShapeDtypeStruct((blk + EXTRA, cols), BF16)] * n_sec,
        out_specs=[VMEM] * n_sec,
        name="grad_head",
    )


def first_gradient(deps, ids, blocks, mixes, blk, height):
    many = len(mixes)
    every = len(blocks)
    width = mixes[0].shape[1]
    nb = width // BLOCKS

    def body(ids_ref, *refs):
        block_refs, mix_refs = refs[:every], refs[every : every + many]
        mine_ref, send_ref, later_ref, left, right, early, sems = refs[every + many :]
        here = pl.multiple_of(ids_ref[1] // ids_ref[7] * blk, blk)
        there = pl.multiple_of(blk - here, blk)
        copies = []
        for i in range(every):
            rows = pl.ds(i * height, height)
            if i < many:
                for j, col in enumerate([here, there]):
                    src = block_refs[i].at[height:, pl.ds(col, blk)]
                    copies.append(pltpu.make_async_copy(src, left.at[rows, j * blk : (j + 1) * blk], sems.at[j, i]))
                copies.append(pltpu.make_async_copy(mix_refs[i], right.at[rows], sems.at[2, i]))
            src = block_refs[i].at[:height, pl.ds(here, blk)]
            copies.append(pltpu.make_async_copy(src, early.at[rows], sems.at[3, i]))
        run_copies(copies)
        later_ref[...] = early[...].astype(F32).T.astype(BF16)
        turned = left[...].astype(F32).T.astype(BF16)
        for n in range(BLOCKS):
            cols = slice(n * nb, (n + 1) * nb)
            part = jnp.dot(turned, right[:, cols], preferred_element_type=F32)
            mine_ref[:, cols] = part[:blk]
            send_ref[:, cols] = part[blk:].astype(BF16)

    return call(
        body,
        [ids, *blocks, *mixes],
        [SMEM] + [ANY] * (every + many),
        deps,
        out_shape=[
            jax.ShapeDtypeStruct((blk, width), F32),
            jax.ShapeDtypeStruct((blk, width), BF16),
            jax.ShapeDtypeStruct((blk, every * height), BF16),
        ],
        out_specs=[VMEM] * 3,
        scratch_shapes=[
            pltpu.VMEM((many * height, 2 * blk), BF16),
            pltpu.VMEM((many * height, width), BF16),
            pltpu.VMEM((every * height, blk), BF16),
            pltpu.SemaphoreType.DMA((4, every)),
        ],
        name="first_gradient",
    )


def last_gradient(deps, ids, turned, mixes, mine, other, blocks, scale):
    blk, width = mine.shape
    nb = width // BLOCKS
    many = len(mixes)
    cols = blocks[0].shape[1]

    def body(ids_ref, turned_ref, *refs):
        mix_refs, (mine_ref, other_ref, *rest) = refs[:many], refs[many:]
        block_refs, (out, head_out, loss_out) = rest[:-3], rest[-3:]
        for j, ref in enumerate(block_refs):

            @pl.when(ids_ref[0] == j)
            def _():
                head_out[...] = ref[:blk, :].astype(F32)
                tail = ref[blk:, :].astype(F32)
                loss_out[...] = (tail[0:1, :128] + tail[1:2, :128]) * scale

        for n in range(BLOCKS):
            span = slice(n * nb, (n + 1) * nb)
            right = jnp.concatenate([ref[:, span] for ref in mix_refs], axis=0)
            part = jnp.dot(turned_ref[...], right, preferred_element_type=F32)
            out[:, span] = part + mine_ref[:, span] + other_ref[:, span].astype(F32)

    args = [ids, turned, *mixes, mine, other, *blocks]
    return call(
        body,
        args,
        [SMEM] + [VMEM] * (len(args) - 1),
        deps,
        out_shape=[
            jax.ShapeDtypeStruct((blk, width), F32),
            jax.ShapeDtypeStruct((blk, cols), F32),
            jax.ShapeDtypeStruct((1, 128), F32),
        ],
        out_specs=[VMEM] * 3,
        name="last_gradient",
    )


def join_rows(deps, flat, deep, rows_out):
    count, rank, width = deep.shape

    def body(flat_ref, deep_ref, out, sem):
        copies = [
            pltpu.make_async_copy(deep_ref.at[i], out.at[i * rank : (i + 1) * rank], sem.at[i])
            for i in range(count)
        ]
        for copy in copies:
            copy.start()
        spare = jnp.zeros((rows_out - count * (rank + 1), width), F32)
        out[count * rank :, :] = jnp.concatenate([flat_ref[...].astype(F32), spare], axis=0).astype(BF16)
        for copy in copies:
            copy.wait()

    return call(
        body,
        [flat, deep],
        [VMEM, ANY],
        deps,
        out_shape=jax.ShapeDtypeStruct((rows_out, width), BF16),
        out_specs=VMEM,
        scratch_shapes=[pltpu.SemaphoreType.DMA((count,))],
        name="join",
    )


def head_stage(deps, level, ids, rows, wanted, share, head_weight, turned):
    height, width = rows.shape
    out_width = head_weight.shape[1]

    def body(ids_ref, rows_ref, wanted_ref, share_ref, head_ref, turned_ref, cot_ref, new_ref):
        @pl.when(ids_ref[0] == level)
        def _():
            sums = []

            def block(cols):
                outputs = jnp.dot(rows_ref[...], head_ref[:, cols], preferred_element_type=F32)
                mismatch = outputs - wanted_ref[:, cols].astype(F32)
                scaled = share_ref[...] * mismatch
                cot_ref[:height, cols] = (2.0 * scaled).astype(BF16)
                sums.append(jnp.sum(scaled * mismatch, axis=1, keepdims=True))

            each_block(out_width, block)
            loss = sum(sums)
            loss = jnp.sum(loss, axis=0, keepdims=True)
            line = lax.broadcasted_iota(jnp.int32, (EXTRA, out_width), 0)
            high = loss.astype(BF16).astype(F32)
            tail = jnp.where(line == 0, high, jnp.where(line == 1, loss - high, 0.0))
            cot_ref[height:, :] = tail.astype(BF16)

            def back_block(cols):
                new_ref[:, cols] = jnp.dot(
                    cot_ref[:height, :], turned_ref[:, cols], preferred_element_type=F32
                ).astype(BF16)

            each_block(width, back_block)

    return call(
        body,
        [ids, rows, wanted, share, head_weight, turned],
        [SMEM] + [VMEM] * 5,
        deps,
        out_shape=[
            jax.ShapeDtypeStruct((height + EXTRA, out_width), BF16),
            jax.ShapeDtypeStruct((height, width), BF16),
        ],
        out_specs=[VMEM] * 2,
        cost_estimate=pl.CostEstimate(flops=2 * height * width * width * 4, bytes_accessed=2 * width * out_width, transcendentals=0),
        name="head",
    )


def local(
    inputs, tangents, targets, target_jac, rank_mask, batch_order, encoder, layers, head_weight
):
    samp_dev, rank = rank_mask.shape
    in_width = inputs.shape[1]
    width = layers.shape[2]
    out_width = head_weight.shape[1]
    n_dp = lax.axis_size("dp")
    n_mp = lax.axis_size("mp")
    n_sec = lax.axis_size("section")
    last = n_sec - 1
    dp_index = lax.axis_index("dp")
    sec = lax.axis_index("section")
    mp_index = lax.axis_index("mp")
    prims = n_mp * samp_dev
    blk = width // (n_dp * n_mp)

    weights = Weights(layers[0])
    helper = last

    piece_rows = round_up(samp_dev * (rank + 1), 16)
    joined_rows = join_rows([], inputs, tangents, piece_rows)
    row_pieces = plane_pieces(joined_rows, helper)

    own_rank = jnp.sum(rank_mask, axis=1)
    slot_line = jnp.arange(samp_dev, dtype=jnp.int32)
    own_slot = jnp.sum(
        jnp.where(batch_order[0][None, :] == slot_line[:, None], slot_line[None, :], 0), axis=1
    ) // (samp_dev // MB)
    own_meta = jnp.stack([own_rank, own_slot]).astype(jnp.int32)
    meta_pieces = jnp.stack(mp_pieces(own_meta))
    order_line = jnp.arange(n_mp, dtype=jnp.int32)
    swap = ((order_line[:, None] ^ mp_index) == order_line[None, :]).astype(jnp.int32)
    meta = jnp.sum(swap[:, :, None, None] * meta_pieces[None], axis=1)
    ranks = meta[:, 0].reshape(prims)
    slots = meta[:, 1].reshape(prims)
    sample_line = jnp.arange(prims, dtype=jnp.int32)
    ends = jnp.sum(jnp.where(sample_line[None, :] <= sample_line[:, None], ranks[None, :], 0), axis=1)
    active = jnp.sum(ranks)
    counts = jnp.sum(jnp.where(slots[None, :] == slots[:, None], ranks[None, :] + 1, 0), axis=1)
    inverse = 1.0 / counts.astype(F32)

    kb = width // n_mp
    ids = jnp.stack(
        [sec] + weights.offsets + [mp_index ^ k for k in range(n_mp)] + [jnp.int32(kb // 2)] * (n_mp == 4)
    ).astype(jnp.int32)
    chunks = 2
    usual = samp_dev * (rank // 2 + 1)
    height = max(round_up(-(-(prims + usual) // chunks), 16), round_up(prims + 8, 16))
    slots_here = chunks * height - prims

    place = mp_index * slots_here + jnp.arange(slots_here, dtype=jnp.int32)
    passed = ends[None, :] <= place[:, None]
    sample = jnp.sum(passed.astype(jnp.int32), axis=1)
    column = place - jnp.sum(jnp.where(passed, ranks[None, :], 0), axis=1)
    present = place < active
    belongs = (sample[:, None] == sample_line[None, :]) & present[:, None]
    source = ((sample // samp_dev) ^ mp_index) * piece_rows + (sample % samp_dev) * rank + column
    source = jnp.where(present, source, -1)
    source_p = ((sample_line // samp_dev) ^ mp_index) * piece_rows + samp_dev * rank + sample_line % samp_dev
    share = jnp.sum(jnp.where(belongs, inverse[None, :], 0.0), axis=1)
    share_p = jnp.where(sample_line // samp_dev == mp_index, inverse, 0.0)
    index = jnp.concatenate([source_p, source])[:, None]
    shares = jnp.concatenate([share_p, share])[:, None]
    onehot = belongs.astype(BF16)
    first = height - prims
    onehots = [onehot[:first], onehot[first:]]
    onehot_t = ((sample_line[:, None] == sample[None, :]) & present[None, :]).astype(BF16)
    onehots_t = [onehot_t[:, :first], onehot_t[:, first:]]
    share_of = [shares[:height], shares[height:]]

    packed = pick_rows([], ids, index, row_pieces, helper)
    if helper != 0:
        packed = hop(packed, helper, 0)
    rows = list(lift_rows(ids, packed, encoder, chunks))
    other_active = dp_swap(active.reshape(1, 1)).reshape(()) if n_dp > 1 else active
    most_active = jnp.maximum(active, other_active)

    small_arrays = [*onehots, *onehots_t, *share_of, index, most_active.reshape(1)]
    layer = weights.assemble(ids, small_arrays)
    token = []
    entered = [None] * chunks
    pres = [[None] * n_sec for _ in range(chunks)]
    tanhs = [None] * n_sec
    heads = [None] * chunks
    goal_pieces = None
    for level in range(n_sec):
        for c in range(chunks):
            got = fwd_stage(
                token, level, ids, layer, rows[c], onehots[c], None if c == 0 else tanhs[level], entered[c]
            )
            token = [got[0]]
            entered[c], pres[c][level] = got[2], got[1]
            if c == 0:
                tanhs[level] = got[3]
            rows[c] = got[0] if level == last else hop(got[0], level, level + 1)
            if level == last:
                heads[c] = head_stage(
                    token, last, ids, rows[c], wanted[c * height : (c + 1) * height], share_of[c], head_weight, turned_head
                )
                token = [heads[c][1]]
        if level == 0:
            turned_layer = turn(token, ids, layer, 1)
            token = [turned_layer]
        if level == min(1, last):
            turned_head = turn(token, ids, head_weight, last)
            token = [turned_head]
        if goal_pieces is None:
            goal_pieces = plane_pieces(join_rows(token, targets, target_jac, piece_rows), last)
        if level == max(last - 1, 0):
            wanted = pick_rows(token, ids, index, goal_pieces, last)
            token = [wanted]

    small = n_dp * n_mp <= 8 and blk % 128 == 0
    cots = [heads[c][1] for c in range(chunks)]
    mixes = [None] * chunks
    backward_order = list(range(1, chunks)) + [0]
    hidden_pieces = head_pieces = None
    arrived = []
    for level in range(last, -1, -1):
        total = None
        for c in backward_order:
            got = bwd_stage(
                token, level, ids, turned_layer, cots[c], pres[c][level], tanhs[level],
                onehots[c], onehots_t[c], total, c == 0, mixes[c],
            )
            mixes[c], total = got[0], got[1]
            token = [got[1]]
            if level > 0:
                cots[c] = hop(got[2], level, level - 1)
        if not small:
            continue
        if level == last:
            sends = pack_columns(token, ids, rows, [h[0] for h in heads], last, n_dp, n_mp, blk)
            token = [sends[0]]
            base = last * n_mp
            head_pieces = [sends[0]] + [
                lax.ppermute(sends[k], ("section", "mp"), [(base + m, base + (m ^ k)) for m in range(n_mp)])
                for k in range(1, n_mp)
            ]
        elif level == last - 1:
            sends = pack_columns(token, ids, entered, [], None, n_dp, n_mp, blk)
            token = [sends[0]]
            hidden_pieces = [sends[0]] + [mp_swap(sends[k], k) for k in range(1, n_mp)]

    cols = out_width // n_sec
    if small:
        swapped = []
        for c in backward_order:
            swapped.append([mixes[c]] + [mp_swap(mixes[c], k) for k in range(1, n_mp)])
        hidden_pieces = both_groups(hidden_pieces)
        first_mine, send, turned = first_gradient([], ids, hidden_pieces, swapped[0], blk, height)
        first_other = dp_swap(send)
        mine, send = head_partial([], ids, head_pieces, last, blk)
        other = dp_swap(send)
        blocks = head_gradient([], ids, mine, other, last, blk, n_sec)
        arrived = [hop(blocks[j], last, j) for j in range(last)]
        grad, head_mine, loss_mine = last_gradient(
            [], ids, turned, both_groups(swapped[1]), first_mine, first_other, [*arrived, blocks[last]],
            1.0 / (n_dp * MB * out_width),
        )
        loss_mine = loss_mine[0, 0]
    else:
        contract = (((0,), (0,)), ((), ()))
        joined = jnp.concatenate(entered, axis=0)
        part = lax.dot_general(joined, jnp.concatenate(mixes, axis=0), contract, preferred_element_type=F32)
        grad = lax.psum_scatter(part.astype(BF16), ("dp", "mp"), scatter_dimension=0, tiled=True).astype(F32)
        cot_out = jnp.concatenate([h[0][:height] for h in heads], axis=0)
        part = lax.dot_general(jnp.concatenate(rows, axis=0), cot_out, contract, preferred_element_type=F32)
        head = lax.psum_scatter(part.astype(BF16), ("dp", "mp"), scatter_dimension=0, tiled=True)
        loss = sum(jnp.sum(h[0][height : height + 2, 0].astype(F32)) for h in heads)
        loss = jnp.where(sec == last, lax.psum(loss, ("dp", "mp")), 0.0).reshape(1, 1)
        head_mine = jnp.where(sec == last, head[:, last * cols :], jnp.zeros((blk, cols), BF16))
        loss_mine = loss
        for j in range(last):
            head_mine = head_mine + hop(head[:, j * cols : (j + 1) * cols], last, j)
            loss_mine = loss_mine + hop(loss, last, j)
        head_mine = head_mine.astype(F32)
        loss_mine = loss_mine.reshape(()) / (n_dp * MB * out_width)
    fast = (grad[None], head_mine, loss_mine)

    def plain():
        depth = rank + 1
        total_rows = samp_dev * depth
        layer_full = jnp.zeros((width, width), BF16)
        kb = weights.block_rows
        for array, block, which, base in weights.pieces:
            row = (mp_index ^ block) * kb + base
            row = row if which is None else row + weights.offsets[which]
            layer_full = lax.dynamic_update_slice_in_dim(layer_full, array, row, 0)
        rows_in = jnp.concatenate([inputs[:, None, :], tangents], axis=1).reshape(total_rows, in_width)
        start = jnp.dot(rows_in, encoder, preferred_element_type=F32).astype(BF16)
        chain = [(j, (j + 1) % n_sec) for j in range(n_sec)]

        def back_one(value):
            return lax.fori_loop(0, last, lambda _, v: lax.ppermute(v, "section", chain), value)

        def pre_of(rows):
            pre = jnp.dot(rows, layer_full, preferred_element_type=F32).reshape(samp_dev, depth, width)
            tanh_p = jnp.tanh(pre[:, 0])
            return pre, tanh_p, 1.0 - tanh_p * tanh_p

        def forward(level, state):
            rows, mine, _ = state
            mine = jnp.where(level == sec, rows, mine)
            pre, tanh_p, slope = pre_of(rows)
            change = jnp.concatenate([tanh_p[:, None], slope[:, None] * pre[:, 1:]], axis=1)
            new = (rows.astype(F32) + change.reshape(total_rows, width)).astype(BF16)
            return lax.ppermute(new, "section", chain), mine, new

        _, mine, final = lax.fori_loop(0, n_sec, forward, (start, start, start))
        own = lax.dynamic_slice_in_dim(inverse, mp_index * samp_dev, samp_dev, 0)
        row_weight = jnp.concatenate([jnp.ones((samp_dev, 1), F32), rank_mask.astype(F32)], axis=1)
        share = (row_weight * own[:, None]).reshape(total_rows, 1)
        outputs = jnp.dot(final, head_weight, preferred_element_type=F32)
        wanted = jnp.concatenate([targets[:, None, :], target_jac], axis=1).reshape(total_rows, out_width)
        mismatch = outputs - wanted.astype(F32)
        loss = jnp.sum(share * mismatch * mismatch)
        cot_out = (2.0 * share * mismatch).astype(BF16)
        cot = lax.dot_general(cot_out, head_weight, (((1,), (1,)), ((), ())), preferred_element_type=F32)
        pre, tanh_p, slope = pre_of(mine)

        def backward(step, state):
            cot, mix_mine = state
            up = cot.astype(F32).reshape(samp_dev, depth, width)
            side = jnp.sum(up[:, 1:] * pre[:, 1:], axis=1)
            lead = up[:, 0] * slope - 2.0 * side * tanh_p * slope
            mix = jnp.concatenate([lead[:, None], up[:, 1:] * slope[:, None]], axis=1)
            mix = mix.astype(BF16).reshape(total_rows, width)
            mix_mine = jnp.where(step == last - sec, mix, mix_mine)
            back = lax.dot_general(mix, layer_full, (((1,), (1,)), ((), ())), preferred_element_type=F32)
            new = (up.reshape(total_rows, width) + back).astype(BF16)
            return back_one(new), mix_mine

        _, mix = lax.fori_loop(0, n_sec, backward, (cot.astype(BF16), mine))

        def scatter(left, right):
            part = lax.dot_general(left, right, (((0,), (0,)), ((), ())), preferred_element_type=F32)
            part = part.astype(BF16).reshape(n_dp, n_mp, blk, right.shape[1])
            mine_part = jnp.zeros((n_dp, blk, right.shape[1]), F32)
            for k in range(n_mp):
                piece = lax.dynamic_index_in_dim(part, mp_index ^ k, 1, False)
                mine_part = mine_part + (piece if k == 0 else mp_swap(piece, k)).astype(F32)
            kept = lax.dynamic_index_in_dim(mine_part, dp_index, 0, False)
            if n_dp > 1:
                sent = lax.dynamic_index_in_dim(mine_part, 1 - dp_index, 0, False)
                kept = kept + dp_swap(sent.astype(BF16)).astype(F32)
            return kept

        grad = scatter(mine, mix)
        head = scatter(final, cot_out)
        cols = out_width // n_sec
        loss_group = sum(mp_pieces(loss.reshape(1, 1)))
        if n_dp > 1:
            loss_group = loss_group + dp_swap(loss_group)
        head_mine = jnp.where(sec == last, head[:, last * cols :], 0.0)
        loss_mine = jnp.where(sec == last, loss_group, 0.0)
        for j in range(last):
            block = jnp.concatenate([head[:, j * cols : (j + 1) * cols], jnp.broadcast_to(loss_group, (8, cols))])
            block = hop(block, last, j)
            head_mine = head_mine + block[:blk]
            loss_mine = loss_mine + block[blk:, :1][:1]
        return grad[None], head_mine, loss_mine.reshape(()) / (n_dp * MB * out_width)

    room = n_mp * slots_here
    if room >= n_mp * samp_dev * rank:
        return fast
    return lax.while_loop(
        lambda state: state[0] > room, lambda state: (jnp.int32(0), *plain()), (most_active, *fast)
    )[1:]


def solution(mesh):
    in_specs = (
        P(("dp", "mp"), None),
        P(("dp", "mp"), None, None),
        P(("dp", "mp"), None),
        P(("dp", "mp"), None, None),
        P(("dp", "mp"), None),
        P(("dp", "mp"), None),
        P(),
        P("section", "mp", None),
        P(),
    )
    out_specs = (P("section", ("dp", "mp"), None), P(("dp", "mp"), "section"), P())

    return jax.shard_map(local, mesh=mesh, in_specs=in_specs, out_specs=out_specs, check_vma=False)
```

```python
import jax
import jax.numpy as jnp
from jax import lax
from jax.experimental import pallas as pl
from jax.experimental.pallas import tpu as pltpu
from jax.sharding import PartitionSpec as P


F32 = jnp.float32
BF16 = jnp.bfloat16
MB = 6
EXTRA = 16
BLOCKS = 4

ANY = pl.BlockSpec(memory_space=pl.ANY)
SMEM = pl.BlockSpec(memory_space=pltpu.SMEM)
VMEM = pl.BlockSpec(memory_space=pltpu.VMEM)


def round_up(value, unit):
    return -(-value // unit) * unit


def mp_swap(value, flip):
    count = lax.axis_size("mp")
    return lax.ppermute(value, "mp", [(m, m ^ flip) for m in range(count)])


def dp_swap(value):
    count = lax.axis_size("dp")
    return lax.ppermute(value, "dp", [(d, d ^ 1) for d in range(count)])


def mp_pieces(value):
    return [value] + [mp_swap(value, k) for k in range(1, lax.axis_size("mp"))]


def hop(value, source, target):
    return lax.ppermute(value, "section", [(source, target)])


def plane_pieces(value, section):
    count = lax.axis_size("mp")
    base = section * count
    swaps = [[(base + m, base + (m ^ k)) for m in range(count)] for k in range(1, count)]
    return [value] + [lax.ppermute(value, ("section", "mp"), pairs) for pairs in swaps]


def params():
    return pltpu.CompilerParams(vmem_limit_bytes=20 * 2**20)


def call(body, args, specs, deps=(), **options):
    reads, waits = len(args), len(deps)

    def inner(*refs):
        body(*refs[:reads], *refs[reads + waits :])

    return pl.pallas_call(
        inner, in_specs=list(specs) + [ANY] * waits, compiler_params=params(), **options
    )(*args, *deps)


def each_block(width, body):
    nb = width // BLOCKS

    def pair(i, carry):
        for j in range(2):
            body(pl.ds(pl.multiple_of((2 * i + j) * nb, nb), nb))
        return carry

    lax.fori_loop(0, BLOCKS // 2, pair, 0)


def small_dot(left, right, form):
    tile = 256
    if form == "tn":
        grid = (left.shape[1] // tile, right.shape[1] // tile)
        shape = (left.shape[1], right.shape[1])
        specs = [
            pl.BlockSpec((left.shape[0], tile), lambda i, j: (0, i)),
            pl.BlockSpec((right.shape[0], tile), lambda i, j: (0, j)),
        ]
        out_spec = pl.BlockSpec((tile, tile), lambda i, j: (i, j))
        contract = (((0,), (0,)), ((), ()))
    else:
        turned = form == "nt"
        width = right.shape[0] if turned else right.shape[1]
        grid = (width // tile, left.shape[1] // tile)
        shape = (left.shape[0], width)
        specs = [
            pl.BlockSpec((left.shape[0], tile), lambda i, j: (0, j)),
            pl.BlockSpec((tile, tile), (lambda i, j: (i, j)) if turned else (lambda i, j: (j, i))),
        ]
        out_spec = pl.BlockSpec((left.shape[0], tile), lambda i, j: (0, i))
        contract = (((1,), (1 if turned else 0,)), ((), ()))

    def body(left_ref, right_ref, out_ref):
        part = lax.dot_general(left_ref[...], right_ref[...], contract, preferred_element_type=F32)
        if form == "tn":
            out_ref[...] = part.astype(BF16)
        else:
            step = pl.program_id(1)

            @pl.when(step == 0)
            def _():
                out_ref[...] = part

            @pl.when(step > 0)
            def _():
                out_ref[...] = out_ref[...] + part

    return pl.pallas_call(
        body,
        out_shape=jax.ShapeDtypeStruct(shape, BF16 if form == "tn" else F32),
        grid=grid,
        in_specs=specs,
        out_specs=out_spec,
        compiler_params=params(),
        name="small_dot",
    )(left, right)


def run_copies(copies):
    for copy in copies:
        copy.start()
    for copy in copies:
        copy.wait()


def spread(onehot, value):
    high = value.astype(BF16)
    low = (value - high.astype(F32)).astype(BF16)
    return jnp.dot(onehot, high, preferred_element_type=F32) + jnp.dot(
        onehot, low, preferred_element_type=F32
    )


class Weights:
    def __init__(self, layer):
        self.count = lax.axis_size("mp")
        self.block_rows, self.width = layer.shape
        dp_index = lax.axis_index("dp")
        half = self.block_rows // 2
        self.offsets = [dp_index * half, (1 - dp_index) * half]
        self.pieces = [(layer, 0, None, 0)]
        self.colored = self.count == 4 and lax.axis_size("dp") == 2
        self.part = part = half // 2
        if self.colored:
            self.first = lax.dynamic_slice_in_dim(layer, dp_index * half, part, 0)
            self.second = lax.dynamic_slice_in_dim(layer, dp_index * half + part, part, 0)
            self.b1 = self.swap(self.second, 1)
            self.a2 = self.swap(self.first, 2)
            self.a1 = self.swap(self.first, 1)
            self.b2 = self.swap(self.second, 2)
            self.a3 = self.swap(self.a1, 2)
            self.b3 = self.swap(self.b2, 1)
            got = [(self.a1, 1, 0), (self.b2, 2, part), (self.b1, 1, part), (self.a2, 2, 0), (self.a3, 3, 0), (self.b3, 3, part)]
            for array, block, base in got:
                self.pieces.append((array, block, 0, base))
                self.pieces.append((dp_swap(array), block, 1, base))
        else:
            for block in range(1, self.count):
                self.pieces.append((mp_swap(layer, block), block, None, 0))

    def swap(self, array, flip):
        return mp_swap(array, flip)

    def assemble(self, ids, deps):
        early = len(self.pieces) - 4 if self.colored else len(self.pieces)
        layer = self.place(ids, None, self.pieces[:early], "assemble", deps)
        return layer if early == len(self.pieces) else self.place(ids, layer, self.pieces[early:], "complete", [])

    def place(self, ids, layer, pieces, name, deps):
        many = len(pieces)

        def body(ids_ref, *refs):
            out, sems = refs[-2:]
            copies = []
            for i, (array, block, which, base) in enumerate(pieces):
                row = pl.multiple_of(ids_ref[3 + block] * self.block_rows, self.block_rows) + base
                if which is not None:
                    row = row + pl.multiple_of(ids_ref[1 + which], self.block_rows // 2)
                copies.append(
                    pltpu.make_async_copy(refs[i], out.at[pl.ds(row, array.shape[0]), :], sems.at[i])
                )
            run_copies(copies)

        before = [] if layer is None else [layer]
        return call(
            body,
            [ids, *[piece[0] for piece in pieces], *before],
            [SMEM] + [ANY] * many + [VMEM] * len(before),
            deps,
            out_shape=jax.ShapeDtypeStruct((self.count * self.block_rows, self.width), BF16),
            out_specs=VMEM,
            input_output_aliases={1 + many: 0} if before else {},
            scratch_shapes=[pltpu.SemaphoreType.DMA((many,))],
            name=name,
        )


def fwd_stage(deps, level, ids, layer, rows, onehot, slope, kept):
    height, width = rows.shape
    prims = onehot.shape[1]
    leads = slope is None

    def body(ids_ref, layer_ref, rows_ref, onehot_ref, *rest):
        if not leads:
            slope_ref, *rest = rest
        next_ref, pre_ref, kept_ref, *rest = rest[(kept is not None) :]
        if leads:
            tanh_ref, *rest = rest
        (kept_sem,) = rest

        @pl.when(ids_ref[0] == level)
        def _():
            keep = pltpu.make_async_copy(rows_ref, kept_ref, kept_sem)
            keep.start()

            def block(cols):
                acc = jnp.dot(rows_ref[...], layer_ref[:, cols], preferred_element_type=F32)
                old = rows_ref[:, cols].astype(F32)
                pre_ref[:, cols] = acc.astype(BF16)
                if leads:
                    tanh_p = jnp.tanh(acc[:prims])
                    tanh_ref[:, cols] = tanh_p
                    factor = spread(onehot_ref[...], 1.0 - tanh_p * tanh_p)
                    new = jnp.concatenate(
                        [old[:prims] + tanh_p, old[prims:] + factor * acc[prims:]], axis=0
                    )
                else:
                    tanh_p = slope_ref[:, cols]
                    new = old + spread(onehot_ref[...], 1.0 - tanh_p * tanh_p) * acc
                next_ref[:, cols] = new.astype(BF16)

            each_block(width, block)
            keep.wait()

    outs = [jax.ShapeDtypeStruct((height, width), BF16)] * 3
    if leads:
        outs.append(jax.ShapeDtypeStruct((prims, width), F32))
    args = [ids, layer, rows, onehot] + ([] if leads else [slope])
    specs = [SMEM] + [VMEM] * (len(args) - 1)
    alias = {}
    if kept is not None:
        alias = {len(args): 2}
        args.append(kept)
        specs.append(ANY)
    return call(
        body,
        args,
        specs,
        deps,
        out_shape=outs,
        out_specs=[VMEM, VMEM, ANY] + [VMEM] * (len(outs) - 3),
        input_output_aliases=alias,
        scratch_shapes=[pltpu.SemaphoreType.DMA],
        cost_estimate=pl.CostEstimate(flops=2 * height * width * width * 4, bytes_accessed=2 * width * width, transcendentals=0),
        name=f"fwd{level}",
    )


def bwd_stage(deps, level, ids, turned, cot, pre, tanh_p, onehot, onehot_t, total, leads, kept):
    height, width = cot.shape
    prims = tanh_p.shape[0]
    deep = level > 0

    def body(ids_ref, cot_ref, pre_ref, tanh_ref, onehot_ref, onehot_t_ref, *rest):
        if total is not None:
            total_ref, *rest = rest
        if deep:
            turned_ref, *rest = rest
        kept_ref, side_ref, *rest = rest[(kept is not None) :]
        if deep:
            new_ref, *rest = rest
        mix_ref, kept_sem = rest

        @pl.when(ids_ref[0] == level)
        def _():
            skip = prims if leads else 0

            def block(cols):
                up = cot_ref[:, cols].astype(F32)
                tanh = tanh_ref[:, cols]
                slope = 1.0 - tanh * tanh
                up_t = up[skip:]
                mix_t = up_t * spread(onehot_ref[...], slope)
                total_here = spread(onehot_t_ref[...], up_t * pre_ref[:, cols].astype(F32)[skip:])
                if total is not None:
                    total_here = total_here + total_ref[:, cols]
                if leads:
                    mix_p = up[:prims] * slope - 2.0 * total_here * tanh * slope
                    mix_ref[:, cols] = jnp.concatenate([mix_p, mix_t], axis=0).astype(BF16)
                else:
                    mix_ref[:, cols] = mix_t.astype(BF16)
                side_ref[:, cols] = total_here

            each_block(width, block)
            keep = pltpu.make_async_copy(mix_ref, kept_ref, kept_sem)
            keep.start()
            if deep:

                def back_block(cols):
                    back = jnp.dot(mix_ref[...], turned_ref[:, cols], preferred_element_type=F32)
                    new_ref[:, cols] = (cot_ref[:, cols].astype(F32) + back).astype(BF16)

                each_block(width, back_block)
            keep.wait()

    rows_shape = jax.ShapeDtypeStruct((height, width), BF16)
    outs = [rows_shape, jax.ShapeDtypeStruct((prims, width), F32)] + ([rows_shape] if deep else [])
    args = [ids, cot, pre, tanh_p, onehot, onehot_t] + ([] if total is None else [total])
    args += [turned] if deep else []
    specs = [SMEM] + [VMEM] * (len(args) - 1)
    alias = {}
    if kept is not None:
        alias = {len(args): 0}
        args.append(kept)
        specs.append(ANY)
    return call(
        body,
        args,
        specs,
        deps,
        out_shape=outs,
        out_specs=[ANY] + [VMEM] * (len(outs) - 1),
        input_output_aliases=alias,
        scratch_shapes=[pltpu.VMEM((height, width), BF16), pltpu.SemaphoreType.DMA],
        cost_estimate=pl.CostEstimate(flops=2 * height * width * width * 4, bytes_accessed=2 * width * width, transcendentals=0),
        name=f"bwd{level}",
    )


def turn(deps, ids, matrix, least):
    rows, cols = matrix.shape
    step = 256

    def body(ids_ref, matrix_ref, out_ref):
        @pl.when(ids_ref[0] >= least)
        def _():
            def strip(i, carry):
                top = pl.ds(pl.multiple_of(i * step, step), step)
                out_ref[:, top] = matrix_ref[top, :].T
                return carry

            lax.fori_loop(0, rows // step, strip, 0)

    return call(
        body,
        [ids, matrix],
        [SMEM, VMEM],
        deps,
        out_shape=jax.ShapeDtypeStruct((cols, rows), matrix.dtype),
        out_specs=VMEM,
        name="turn",
    )


def pick_rows(deps, ids, index, pieces, level):
    height = index.shape[0]
    piece_rows, width = pieces[0].shape

    def body(ids_ref, index_ref, *rest):
        out_ref = rest[-1]

        @pl.when(ids_ref[0] == level)
        def _():
            index_here = index_ref[...]
            acc = jnp.zeros((height, width), F32)
            for k, piece_ref in enumerate(rest[:-1]):
                place = lax.broadcasted_iota(jnp.int32, (height, piece_rows), 1) + k * piece_rows
                onehot = jnp.where(place == index_here, 1.0, 0.0).astype(BF16)
                acc = acc + jnp.dot(onehot, piece_ref[...], preferred_element_type=F32)
            out_ref[...] = acc.astype(BF16)

    return call(
        body,
        [ids, index, *pieces],
        [SMEM] + [VMEM] * (1 + len(pieces)),
        deps,
        out_shape=jax.ShapeDtypeStruct((height, width), BF16),
        out_specs=VMEM,
        name="pick",
    )


def lift_rows(ids, rows, encoder, chunks):
    height = rows.shape[0] // chunks
    width = encoder.shape[1]

    def body(ids_ref, rows_ref, encoder_ref, *outs):
        @pl.when(ids_ref[0] == 0)
        def _():
            for c, out in enumerate(outs):
                part = rows_ref[c * height : (c + 1) * height, :]
                out[...] = jnp.dot(part, encoder_ref[...], preferred_element_type=F32).astype(BF16)

    return pl.pallas_call(
        body,
        out_shape=[jax.ShapeDtypeStruct((height, width), BF16)] * chunks,
        in_specs=[SMEM, VMEM, VMEM],
        out_specs=[VMEM] * chunks,
        compiler_params=params(),
        name="lift",
    )(ids, rows, encoder)


def pack_columns(deps, ids, chunks, tails, level, n_dp, n_mp, blk):
    count = len(chunks)
    height, _ = chunks[0].shape
    tail_width = tails[0].shape[1] if tails else 0
    core = n_dp * blk
    end = count * height

    def body(ids_ref, *refs):
        chunk_refs, rest = refs[:count], refs[count:]
        tail_refs, outs = rest[: len(tails)], rest[len(tails) :]

        def fill():
            for k, out in enumerate(outs):
                for c, chunk_ref in enumerate(chunk_refs):
                    first = c * height
                    for d in range(n_dp):
                        col = pl.multiple_of((ids_ref[3 + k] + d * n_mp) * blk, blk)
                        out[first : first + height, d * blk : (d + 1) * blk] = chunk_ref[:, pl.ds(col, blk)]
                    if tails:
                        out[first : first + height, core:] = tail_refs[c][:height, :]
                if tails:
                    sums = [ref[height:, :].astype(F32)[: EXTRA // 2] for ref in tail_refs]
                    out[end:, :core] = jnp.zeros((EXTRA, core), BF16)
                    out[end:, core:] = jnp.concatenate(sums, axis=0).astype(BF16)

        if level is None:
            fill()
        else:
            pl.when(ids_ref[0] == level)(fill)

    shape = jax.ShapeDtypeStruct((end + (EXTRA if tails else 0), core + tail_width), BF16)
    return call(
        body,
        [ids, *chunks, *tails],
        [SMEM] + [VMEM] * (count + len(tails)),
        deps,
        out_shape=[shape] * n_mp,
        out_specs=[VMEM] * n_mp,
        name="pack",
    )


def both_groups(pieces):
    return pieces + ([dp_swap(piece) for piece in pieces] if lax.axis_size("dp") > 1 else [])


def loss_rows(loss, cols):
    high = loss.astype(BF16).astype(F32)
    line = lax.broadcasted_iota(jnp.int32, (EXTRA, cols), 0)
    return jnp.where(line == 0, high, jnp.where(line == 1, loss - high, 0.0))


def head_partial(deps, ids, pieces, level, blk):
    rows_each, wide = pieces[0].shape
    core = 2 * blk
    out_width = wide - core
    many = len(pieces)

    def body(ids_ref, *refs):
        piece_refs, (mine_ref, send_ref, left, right, sems) = refs[:many], refs[many:]

        @pl.when(ids_ref[0] == level)
        def _():
            here = pl.multiple_of(ids_ref[1] // ids_ref[7] * blk, blk)
            there = pl.multiple_of(blk - here, blk)
            copies = []
            for i, ref in enumerate(piece_refs):
                rows = pl.ds(i * rows_each, rows_each)
                copies.append(pltpu.make_async_copy(ref.at[:, pl.ds(here, blk)], left.at[rows, :blk], sems.at[0, i]))
                copies.append(pltpu.make_async_copy(ref.at[:, pl.ds(there, blk)], left.at[rows, blk:], sems.at[1, i]))
                copies.append(pltpu.make_async_copy(ref.at[:, core:], right.at[rows], sems.at[2, i]))
            run_copies(copies)
            loss = jnp.zeros((1, 128), F32)
            for piece in range(1, many + 1):
                tail = right[piece * rows_each - EXTRA : piece * rows_each, :128].astype(F32)
                loss = loss + tail[0:1] + tail[1:2] + tail[EXTRA // 2 : EXTRA // 2 + 1] + tail[EXTRA // 2 + 1 : EXTRA // 2 + 2]
            tail = loss_rows(loss[:, :1], out_width)
            part = lax.dot_general(left[...], right[...], (((0,), (0,)), ((), ())), preferred_element_type=F32)
            mine_ref[:blk, :] = part[:blk]
            mine_ref[blk:, :] = tail
            send_ref[:blk, :] = part[blk:].astype(BF16)
            send_ref[blk:, :] = tail.astype(BF16)

    shape = (blk + EXTRA, out_width)
    return call(
        body,
        [ids, *pieces],
        [SMEM] + [ANY] * many,
        deps,
        out_shape=[jax.ShapeDtypeStruct(shape, F32), jax.ShapeDtypeStruct(shape, BF16)],
        out_specs=[VMEM] * 2,
        scratch_shapes=[
            pltpu.VMEM((many * rows_each, core), BF16),
            pltpu.VMEM((many * rows_each, out_width), BF16),
            pltpu.SemaphoreType.DMA((3, many)),
        ],
        name="head_partial",
    )


def head_gradient(deps, ids, mine, other, level, blk, n_sec):
    cols = mine.shape[1] // n_sec

    def body(ids_ref, mine_ref, other_ref, *outs):
        @pl.when(ids_ref[0] == level)
        def _():
            tails = mine_ref[blk:, :1] + other_ref[blk:, :128].astype(F32)[:, :1]
            tail = loss_rows(tails[0:1] + tails[1:2], cols).astype(BF16)
            for j, out in enumerate(outs):
                span = slice(j * cols, (j + 1) * cols)
                out[:blk, :] = (mine_ref[:blk, span] + other_ref[:blk, span].astype(F32)).astype(BF16)
                out[blk:, :] = tail

    return call(
        body,
        [ids, mine, other],
        [SMEM, VMEM, VMEM],
        deps,
        out_shape=[jax.ShapeDtypeStruct((blk + EXTRA, cols), BF16)] * n_sec,
        out_specs=[VMEM] * n_sec,
        name="grad_head",
    )


def first_gradient(deps, ids, blocks, mixes, blk, height):
    many = len(mixes)
    every = len(blocks)
    width = mixes[0].shape[1]
    nb = width // BLOCKS

    def body(ids_ref, *refs):
        block_refs, mix_refs = refs[:every], refs[every : every + many]
        mine_ref, send_ref, later_ref, left, right, early, sems = refs[every + many :]
        here = pl.multiple_of(ids_ref[1] // ids_ref[7] * blk, blk)
        there = pl.multiple_of(blk - here, blk)
        copies = []
        for i in range(every):
            rows = pl.ds(i * height, height)
            if i < many:
                for j, col in enumerate([here, there]):
                    src = block_refs[i].at[height:, pl.ds(col, blk)]
                    copies.append(pltpu.make_async_copy(src, left.at[rows, j * blk : (j + 1) * blk], sems.at[j, i]))
                copies.append(pltpu.make_async_copy(mix_refs[i], right.at[rows], sems.at[2, i]))
            src = block_refs[i].at[:height, pl.ds(here, blk)]
            copies.append(pltpu.make_async_copy(src, early.at[rows], sems.at[3, i]))
        run_copies(copies)
        later_ref[...] = early[...].astype(F32).T.astype(BF16)
        turned = left[...].astype(F32).T.astype(BF16)
        for n in range(BLOCKS):
            cols = slice(n * nb, (n + 1) * nb)
            part = jnp.dot(turned, right[:, cols], preferred_element_type=F32)
            mine_ref[:, cols] = part[:blk]
            send_ref[:, cols] = part[blk:].astype(BF16)

    return call(
        body,
        [ids, *blocks, *mixes],
        [SMEM] + [ANY] * (every + many),
        deps,
        out_shape=[
            jax.ShapeDtypeStruct((blk, width), F32),
            jax.ShapeDtypeStruct((blk, width), BF16),
            jax.ShapeDtypeStruct((blk, every * height), BF16),
        ],
        out_specs=[VMEM] * 3,
        scratch_shapes=[
            pltpu.VMEM((many * height, 2 * blk), BF16),
            pltpu.VMEM((many * height, width), BF16),
            pltpu.VMEM((every * height, blk), BF16),
            pltpu.SemaphoreType.DMA((4, every)),
        ],
        name="first_gradient",
    )


def last_gradient(deps, ids, turned, mixes, mine, other, blocks, scale):
    blk, width = mine.shape
    nb = width // BLOCKS
    many = len(mixes)
    cols = blocks[0].shape[1]

    def body(ids_ref, turned_ref, *refs):
        mix_refs, (mine_ref, other_ref, *rest) = refs[:many], refs[many:]
        block_refs, (out, head_out, loss_out) = rest[:-3], rest[-3:]
        for j, ref in enumerate(block_refs):

            @pl.when(ids_ref[0] == j)
            def _():
                head_out[...] = ref[:blk, :].astype(F32)
                tail = ref[blk:, :].astype(F32)
                loss_out[...] = (tail[0:1, :128] + tail[1:2, :128]) * scale

        for n in range(BLOCKS):
            span = slice(n * nb, (n + 1) * nb)
            right = jnp.concatenate([ref[:, span] for ref in mix_refs], axis=0)
            part = jnp.dot(turned_ref[...], right, preferred_element_type=F32)
            out[:, span] = part + mine_ref[:, span] + other_ref[:, span].astype(F32)

    args = [ids, turned, *mixes, mine, other, *blocks]
    return call(
        body,
        args,
        [SMEM] + [VMEM] * (len(args) - 1),
        deps,
        out_shape=[
            jax.ShapeDtypeStruct((blk, width), F32),
            jax.ShapeDtypeStruct((blk, cols), F32),
            jax.ShapeDtypeStruct((1, 128), F32),
        ],
        out_specs=[VMEM] * 3,
        name="last_gradient",
    )


def join_rows(deps, flat, deep, rows_out):
    count, rank, width = deep.shape

    def body(flat_ref, deep_ref, out, sem):
        copies = [
            pltpu.make_async_copy(deep_ref.at[i], out.at[i * rank : (i + 1) * rank], sem.at[i])
            for i in range(count)
        ]
        for copy in copies:
            copy.start()
        spare = jnp.zeros((rows_out - count * (rank + 1), width), F32)
        out[count * rank :, :] = jnp.concatenate([flat_ref[...].astype(F32), spare], axis=0).astype(BF16)
        for copy in copies:
            copy.wait()

    return call(
        body,
        [flat, deep],
        [VMEM, ANY],
        deps,
        out_shape=jax.ShapeDtypeStruct((rows_out, width), BF16),
        out_specs=VMEM,
        scratch_shapes=[pltpu.SemaphoreType.DMA((count,))],
        name="join",
    )


def head_stage(deps, level, ids, rows, wanted, share, head_weight, turned):
    height, width = rows.shape
    out_width = head_weight.shape[1]

    def body(ids_ref, rows_ref, wanted_ref, share_ref, head_ref, turned_ref, cot_ref, new_ref):
        @pl.when(ids_ref[0] == level)
        def _():
            sums = []

            def block(cols):
                outputs = jnp.dot(rows_ref[...], head_ref[:, cols], preferred_element_type=F32)
                mismatch = outputs - wanted_ref[:, cols].astype(F32)
                scaled = share_ref[...] * mismatch
                cot_ref[:height, cols] = (2.0 * scaled).astype(BF16)
                sums.append(jnp.sum(scaled * mismatch, axis=1, keepdims=True))

            for n in range(BLOCKS):
                block(slice(n * out_width // BLOCKS, (n + 1) * out_width // BLOCKS))
            loss = sum(sums)
            loss = jnp.sum(loss, axis=0, keepdims=True)
            line = lax.broadcasted_iota(jnp.int32, (EXTRA, out_width), 0)
            high = loss.astype(BF16).astype(F32)
            tail = jnp.where(line == 0, high, jnp.where(line == 1, loss - high, 0.0))
            cot_ref[height:, :] = tail.astype(BF16)

            def back_block(cols):
                new_ref[:, cols] = jnp.dot(
                    cot_ref[:height, :], turned_ref[:, cols], preferred_element_type=F32
                ).astype(BF16)

            each_block(width, back_block)

    return call(
        body,
        [ids, rows, wanted, share, head_weight, turned],
        [SMEM] + [VMEM] * 5,
        deps,
        out_shape=[
            jax.ShapeDtypeStruct((height + EXTRA, out_width), BF16),
            jax.ShapeDtypeStruct((height, width), BF16),
        ],
        out_specs=[VMEM] * 2,
        cost_estimate=pl.CostEstimate(flops=2 * height * width * width * 4, bytes_accessed=2 * width * out_width, transcendentals=0),
        name="head",
    )


def local(
    inputs, tangents, targets, target_jac, rank_mask, batch_order, encoder, layers, head_weight
):
    samp_dev, rank = rank_mask.shape
    width = layers.shape[2]
    out_width = head_weight.shape[1]
    n_dp = lax.axis_size("dp")
    n_mp = lax.axis_size("mp")
    n_sec = lax.axis_size("section")
    last = n_sec - 1
    dp_index = lax.axis_index("dp")
    sec = lax.axis_index("section")
    mp_index = lax.axis_index("mp")
    prims = n_mp * samp_dev
    blk = width // (n_dp * n_mp)

    weights = Weights(layers[0])
    helper = last

    piece_rows = round_up(samp_dev * (rank + 1), 16)
    joined_rows = join_rows([], inputs, tangents, piece_rows)
    row_pieces = plane_pieces(joined_rows, helper)

    own_rank = jnp.sum(rank_mask, axis=1)
    slot_line = jnp.arange(samp_dev, dtype=jnp.int32)
    own_slot = jnp.sum(
        jnp.where(batch_order[0][None, :] == slot_line[:, None], slot_line[None, :], 0), axis=1
    ) // (samp_dev // MB)
    own_meta = jnp.stack([own_rank, own_slot]).astype(jnp.int32)
    meta_pieces = jnp.stack(mp_pieces(own_meta))
    order_line = jnp.arange(n_mp, dtype=jnp.int32)
    swap = ((order_line[:, None] ^ mp_index) == order_line[None, :]).astype(jnp.int32)
    meta = jnp.sum(swap[:, :, None, None] * meta_pieces[None], axis=1)
    ranks = meta[:, 0].reshape(prims)
    slots = meta[:, 1].reshape(prims)
    sample_line = jnp.arange(prims, dtype=jnp.int32)
    ends = jnp.sum(jnp.where(sample_line[None, :] <= sample_line[:, None], ranks[None, :], 0), axis=1)
    active = jnp.sum(ranks)
    counts = jnp.sum(jnp.where(slots[None, :] == slots[:, None], ranks[None, :] + 1, 0), axis=1)
    inverse = 1.0 / counts.astype(F32)

    kb = width // n_mp
    ids = jnp.stack(
        [sec] + weights.offsets + [mp_index ^ k for k in range(n_mp)] + [jnp.int32(kb // 2)] * (n_mp == 4)
    ).astype(jnp.int32)
    chunks = 2
    usual = samp_dev * (rank // 2 + 1)
    height = max(round_up(-(-(prims + usual) // chunks), 16), round_up(prims + 8, 16))
    slots_here = chunks * height - prims

    place = mp_index * slots_here + jnp.arange(slots_here, dtype=jnp.int32)
    passed = ends[None, :] <= place[:, None]
    sample = jnp.sum(passed.astype(jnp.int32), axis=1)
    column = place - jnp.sum(jnp.where(passed, ranks[None, :], 0), axis=1)
    present = place < active
    belongs = (sample[:, None] == sample_line[None, :]) & present[:, None]
    source = ((sample // samp_dev) ^ mp_index) * piece_rows + (sample % samp_dev) * rank + column
    source = jnp.where(present, source, -1)
    source_p = ((sample_line // samp_dev) ^ mp_index) * piece_rows + samp_dev * rank + sample_line % samp_dev
    share = jnp.sum(jnp.where(belongs, inverse[None, :], 0.0), axis=1)
    share_p = jnp.where(sample_line // samp_dev == mp_index, inverse, 0.0)
    index = jnp.concatenate([source_p, source])[:, None]
    shares = jnp.concatenate([share_p, share])[:, None]
    onehot = belongs.astype(BF16)
    first = height - prims
    onehots = [onehot[:first], onehot[first:]]
    onehot_t = ((sample_line[:, None] == sample[None, :]) & present[None, :]).astype(BF16)
    onehots_t = [onehot_t[:, :first], onehot_t[:, first:]]
    share_of = [shares[:height], shares[height:]]

    packed = pick_rows([], ids, index, row_pieces, helper)
    if helper != 0:
        packed = hop(packed, helper, 0)
    rows = list(lift_rows(ids, packed, encoder, chunks))
    other_active = dp_swap(active.reshape(1, 1)).reshape(()) if n_dp > 1 else active
    most_active = jnp.maximum(active, other_active)

    small_arrays = [*onehots, *onehots_t, *share_of, index, most_active.reshape(1)]
    layer = weights.assemble(ids, small_arrays)
    token = []
    entered = [None] * chunks
    pres = [[None] * n_sec for _ in range(chunks)]
    tanhs = [None] * n_sec
    heads = [None] * chunks
    goal_pieces = plane_pieces(join_rows([], targets, target_jac, piece_rows), last)
    for level in range(n_sec):
        for c in range(chunks):
            got = fwd_stage(
                token, level, ids, layer, rows[c], onehots[c], None if c == 0 else tanhs[level], entered[c]
            )
            token = [got[0]]
            entered[c], pres[c][level] = got[2], got[1]
            if c == 0:
                tanhs[level] = got[3]
            rows[c] = got[0] if level == last else hop(got[0], level, level + 1)
            if level == last:
                heads[c] = head_stage(
                    token, last, ids, rows[c], wanted[c * height : (c + 1) * height], share_of[c], head_weight, turned_head
                )
                token = [heads[c][1]]
        if level == 0:
            turned_layer = turn(token, ids, layer, 1)
            token = [turned_layer]
        if level == min(1, last):
            turned_head = turn(token, ids, head_weight, last)
            token = [turned_head]
        if level == max(last - 1, 0):
            wanted = pick_rows(token, ids, index, goal_pieces, last)
            token = [wanted]

    small = n_dp * n_mp <= 8 and blk % 128 == 0
    cots = [heads[c][1] for c in range(chunks)]
    mixes = [None] * chunks
    backward_order = list(range(1, chunks)) + [0]
    hidden_pieces = head_pieces = None
    arrived = []
    for level in range(last, -1, -1):
        total = None
        for c in backward_order:
            got = bwd_stage(
                token, level, ids, turned_layer, cots[c], pres[c][level], tanhs[level],
                onehots[c], onehots_t[c], total, c == 0, mixes[c],
            )
            mixes[c], total = got[0], got[1]
            token = [got[1]]
            if level > 0:
                cots[c] = hop(got[2], level, level - 1)
        if not small:
            continue
        if level == last:
            sends = pack_columns(token, ids, rows, [h[0] for h in heads], last, n_dp, n_mp, blk)
            token = [sends[0]]
            base = last * n_mp
            head_pieces = [sends[0]] + [
                lax.ppermute(sends[k], ("section", "mp"), [(base + m, base + (m ^ k)) for m in range(n_mp)])
                for k in range(1, n_mp)
            ]
        elif level == last - 1:
            sends = pack_columns(token, ids, entered, [], None, n_dp, n_mp, blk)
            token = [sends[0]]
            hidden_pieces = [sends[0]] + [mp_swap(sends[k], k) for k in range(1, n_mp)]

    cols = out_width // n_sec
    if small:
        swapped = []
        for c in backward_order:
            swapped.append([mixes[c]] + [mp_swap(mixes[c], k) for k in range(1, n_mp)])
        hidden_pieces = both_groups(hidden_pieces)
        first_mine, send, turned = first_gradient([], ids, hidden_pieces, swapped[0], blk, height)
        first_other = dp_swap(send)
        mine, send = head_partial([], ids, head_pieces, last, blk)
        other = dp_swap(send)
        blocks = head_gradient([], ids, mine, other, last, blk, n_sec)
        arrived = [hop(blocks[j], last, j) for j in range(last)]
        grad, head_mine, loss_mine = last_gradient(
            [], ids, turned, both_groups(swapped[1]), first_mine, first_other, [*arrived, blocks[last]],
            1.0 / (n_dp * MB * out_width),
        )
        loss_mine = loss_mine[0, 0]
    else:
        contract = (((0,), (0,)), ((), ()))
        joined = jnp.concatenate(entered, axis=0)
        part = lax.dot_general(joined, jnp.concatenate(mixes, axis=0), contract, preferred_element_type=F32)
        grad = lax.psum_scatter(part.astype(BF16), ("dp", "mp"), scatter_dimension=0, tiled=True).astype(F32)
        cot_out = jnp.concatenate([h[0][:height] for h in heads], axis=0)
        part = lax.dot_general(jnp.concatenate(rows, axis=0), cot_out, contract, preferred_element_type=F32)
        head = lax.psum_scatter(part.astype(BF16), ("dp", "mp"), scatter_dimension=0, tiled=True)
        loss = sum(jnp.sum(h[0][height : height + 2, 0].astype(F32)) for h in heads)
        loss = jnp.where(sec == last, lax.psum(loss, ("dp", "mp")), 0.0).reshape(1, 1)
        head_mine = jnp.where(sec == last, head[:, last * cols :], jnp.zeros((blk, cols), BF16))
        loss_mine = loss
        for j in range(last):
            head_mine = head_mine + hop(head[:, j * cols : (j + 1) * cols], last, j)
            loss_mine = loss_mine + hop(loss, last, j)
        head_mine = head_mine.astype(F32)
        loss_mine = loss_mine.reshape(()) / (n_dp * MB * out_width)
    fast = (grad[None], head_mine, loss_mine)

    def plain():
        deep = samp_dev * rank
        layer_full = jnp.zeros((width, width), BF16)
        kb = weights.block_rows
        for array, block, which, base in weights.pieces:
            row = (mp_index ^ block) * kb + base
            row = row if which is None else row + weights.offsets[which]
            layer_full = lax.dynamic_update_slice_in_dim(layer_full, array, row, 0)

        def split(rows):
            return rows[:deep].reshape(samp_dev, rank, -1), rows[deep : deep + samp_dev]

        def merge(tangent, primal):
            wide = primal.shape[1]
            spare = jnp.zeros((piece_rows - deep - samp_dev, wide), primal.dtype)
            return jnp.concatenate([tangent.reshape(deep, wide), primal, spare], axis=0)

        start = small_dot(joined_rows, encoder, "nn").astype(BF16)
        chain = [(j, (j + 1) % n_sec) for j in range(n_sec)]

        def back_one(value):
            return lax.fori_loop(0, last, lambda _, v: lax.ppermute(v, "section", chain), value)

        def pre_of(rows):
            pre_t, pre_p = split(small_dot(rows, layer_full, "nn"))
            tanh_p = jnp.tanh(pre_p)
            return pre_t, tanh_p, 1.0 - tanh_p * tanh_p

        def forward(level, state):
            rows, mine, _ = state
            mine = jnp.where(level == sec, rows, mine)
            pre_t, tanh_p, slope = pre_of(rows)
            new = (rows.astype(F32) + merge(slope[:, None] * pre_t, tanh_p)).astype(BF16)
            return lax.ppermute(new, "section", chain), mine, new

        _, mine, final = lax.fori_loop(0, n_sec, forward, (start, start, start))
        own = lax.dynamic_slice_in_dim(inverse, mp_index * samp_dev, samp_dev, 0)
        share = merge((rank_mask.astype(F32) * own[:, None])[:, :, None], own[:, None])
        outputs = small_dot(final, head_weight, "nn")
        mismatch = outputs - join_rows([], targets, target_jac, piece_rows).astype(F32)
        loss = jnp.sum(share * mismatch * mismatch)
        cot_out = (2.0 * share * mismatch).astype(BF16)
        cot = small_dot(cot_out, head_weight, "nt").astype(BF16)
        pre_t, tanh_p, slope = pre_of(mine)

        def backward(step, state):
            cot, mix_mine = state
            up = cot.astype(F32)
            up_t, up_p = split(up)
            side = jnp.sum(up_t * pre_t, axis=1)
            mix = merge(up_t * slope[:, None], up_p * slope - 2.0 * side * tanh_p * slope).astype(BF16)
            mix_mine = jnp.where(step == last - sec, mix, mix_mine)
            return back_one((up + small_dot(mix, layer_full, "nt")).astype(BF16)), mix_mine

        _, mix = lax.fori_loop(0, n_sec, backward, (cot, mine))

        def scatter(part):
            wide = part.shape[1]
            part = part.reshape(n_dp, n_mp, blk, wide)
            mine_part = jnp.zeros((n_dp, blk, wide), F32)
            for k in range(n_mp):
                piece = lax.dynamic_index_in_dim(part, mp_index ^ k, 1, False)
                mine_part = mine_part + (piece if k == 0 else mp_swap(piece, k)).astype(F32)
            kept = lax.dynamic_index_in_dim(mine_part, dp_index, 0, False)
            if n_dp > 1:
                sent = lax.dynamic_index_in_dim(mine_part, 1 - dp_index, 0, False)
                kept = kept + dp_swap(sent.astype(BF16)).astype(F32)
            return kept

        both = scatter(
            jnp.concatenate([small_dot(mine, mix, "tn"), small_dot(final, cot_out, "tn")], axis=1)
        )
        grad, head = both[:, :width], both[:, width:]
        cols = out_width // n_sec
        loss_group = sum(mp_pieces(loss.reshape(1, 1)))
        if n_dp > 1:
            loss_group = loss_group + dp_swap(loss_group)
        head_mine = jnp.where(sec == last, head[:, last * cols :], 0.0)
        loss_mine = jnp.where(sec == last, loss_group, 0.0)
        for j in range(last):
            block = jnp.concatenate([head[:, j * cols : (j + 1) * cols], jnp.broadcast_to(loss_group, (8, cols))])
            block = hop(block, last, j)
            head_mine = head_mine + block[:blk]
            loss_mine = loss_mine + block[blk:, :1][:1]
        return grad[None], head_mine, loss_mine.reshape(()) / (n_dp * MB * out_width)

    room = n_mp * slots_here
    if room >= n_mp * samp_dev * rank:
        return fast
    return lax.while_loop(
        lambda state: state[0] > room, lambda state: (jnp.int32(0), *plain()), (most_active, *fast)
    )[1:]


def solution(mesh):
    in_specs = (
        P(("dp", "mp"), None),
        P(("dp", "mp"), None, None),
        P(("dp", "mp"), None),
        P(("dp", "mp"), None, None),
        P(("dp", "mp"), None),
        P(("dp", "mp"), None),
        P(),
        P("section", "mp", None),
        P(),
    )
    out_specs = (P("section", ("dp", "mp"), None), P(("dp", "mp"), "section"), P())

    return jax.shard_map(local, mesh=mesh, in_specs=in_specs, out_specs=out_specs, check_vma=False)
```
